32 devices in a mesh: dp: 2 (over x), tp: 16 (over y, z, core).
Axes of the slice: x: 2, y: 2, z: 4, core: 2. Of those that a mesh axis runs over, the one named last changes fastest.
Arguments:
- x: bfloat16 [4096, 12288], P('dp'), parts along dimension 0
- gain: bfloat16 [12288], replicated
- wq: bfloat16 [12288, 12288], P(None, 'tp')
- wk: bfloat16 [12288, 12288], P(None, 'tp')
- wv: bfloat16 [12288, 12288], P(None, 'tp')
- wo: bfloat16 [12288, 12288], P('tp')
Outputs:
- output: bfloat16 [4096, 12288], P('dp'), parts along dimension 0
There are 2 independent parts. The reference program is written for one: setup_inputs(seed, part) draws one part's arguments, and reference() takes and returns one part's arrays. A program takes and returns all parts, laid end to end along the dimension named above; an argument that names none is the same for every part.
All inputs are finite; a program needn't handle non-finite values.
Results may differ from the reference program's by a relative error of at most 0.012.
Values are sent between devices in bfloat16 or wider.
A program may use at most 2 GiB of HBM per device.

```python
import jax
import jax.numpy as jnp
from jax import lax

ROWS = 2048
D = 12288
HEADS = 96
KV_HEADS = 96
HEAD = 128
THETA = 10000


def setup_inputs(seed: int = 0, part: int = 0) -> dict:
    kx, kn, kq, kk, kv, ko = jax.random.split(jax.random.key(seed), 6)

    def weights(key, rows, columns):
        return jax.random.normal(key, (rows, columns), jnp.float32) * rows**-0.5

    drawn = {
        "x": jax.random.normal(jax.random.fold_in(kx, part), (ROWS, D), jnp.float32),
        "gain": 1 + 0.1 * jax.random.normal(kn, (D,), jnp.float32),
        "wq": 2 * weights(kq, D, HEADS * HEAD),
        "wk": 2 * weights(kk, D, KV_HEADS * HEAD),
        "wv": 4 * weights(kv, D, KV_HEADS * HEAD),
        "wo": weights(ko, HEADS * HEAD, D),
    }
    return {k: v.astype(jnp.bfloat16) for k, v in drawn.items()}


def normed(x, gain):
    wide = x.astype(jnp.float32)
    scale = lax.rsqrt(jnp.mean(wide * wide, -1, keepdims=True) + 1e-6)
    return (wide * scale * gain.astype(jnp.float32)).astype(jnp.bfloat16)


def turned(t, place, theta):
    half = t.shape[-1] // 2
    angle = place.astype(jnp.float32)[:, None] * theta ** (-jnp.arange(half, dtype=jnp.float32) / half)
    cos, sin = jnp.cos(angle)[:, None], jnp.sin(angle)[:, None]
    a, b = t[..., :half].astype(jnp.float32), t[..., half:].astype(jnp.float32)
    return jnp.concatenate([a * cos - b * sin, b * cos + a * sin], -1).astype(jnp.bfloat16)


def matmul(a, w):
    return jnp.dot(a, w, preferred_element_type=jnp.float32).astype(jnp.bfloat16)


def einsum(form, a, b):
    return jnp.einsum(form, a.astype(jnp.float32), b.astype(jnp.float32))


def attention(q, k, v):
    scores = einsum("tgsd,ugd->gstu", q, k) * q.shape[-1] ** -0.5
    token = jnp.arange(q.shape[0])
    scores = jnp.where(token[:, None] >= token, scores, -jnp.inf)
    weights = jax.nn.softmax(scores, -1).astype(jnp.bfloat16)
    return einsum("gstu,ugd->tgsd", weights, v).astype(jnp.bfloat16)


def reference(x, gain, wq, wk, wv, wo):
    a, place = normed(x, gain), jnp.arange(ROWS)
    q = turned(matmul(a, wq).reshape(ROWS, HEADS, HEAD), place, THETA).reshape(ROWS, KV_HEADS, -1, HEAD)
    k = turned(matmul(a, wk).reshape(ROWS, KV_HEADS, HEAD), place, THETA)
    v = matmul(a, wv).reshape(ROWS, KV_HEADS, HEAD)
    seen = attention(q, k, v).reshape(ROWS, HEADS * HEAD)
    return (x.astype(jnp.float32) + jnp.dot(seen, wo, preferred_element_type=jnp.float32)).astype(jnp.bfloat16)
```

```python
import functools

import jax
import jax.numpy as jnp
from jax import lax
from jax.experimental import pallas as pl
from jax.experimental.pallas import tpu as pltpu
from jax.sharding import PartitionSpec as P

HEAD = 128
THETA = 10000
LOG2E = 1.4426950408889634
NEG = -1e30
CHUNK = 256
SUB = 64
PER = CHUNK // SUB
TILE = 256
WO_TILE = 512
SLOTS = 6
MARKS = 8
LAST = 7
f32, bf16 = jnp.float32, jnp.bfloat16


def _dot(a, b, ca, cb):
    return lax.dot_general(a, b, (((ca,), (cb,)), ((), ())), preferred_element_type=f32)


def _kernel(x, gain, wq, wk, wv, wo, cos, sin, out, wo_ext, xb, wb, ob, kc, vt, qb, seen, pp, mix, top, cs, sn, xa_res, xb_res,
            ra0, ra1f, ra1n, ra2, rb0f, rb0n, rb1, rb2, sa0, sa1f, sa1n, sa2, sb0f, sb0n, sb1, sb2, fa, fb,
            s_x, s_w, s_o, s_cs, s_res, s_local, s_send, s_rs, s_ag, s_seen, s_ext, *, d, hl, nch):
    half, qa = d // 2, d // 4
    nt = hl * HEAD // TILE
    nsub = nch * PER
    pos = lax.axis_index("tp")
    y, z, core = lax.div(pos, 8), lax.rem(lax.div(pos, 2), 4), lax.rem(pos, 2)
    side = lax.div(z, 2)
    inner = (z == 1) | (z == 2)
    outer = (z == 0) | (z == 3)

    def at(y, z, core):
        return (y * 4 + z) * 2 + core

    partner = at(y, z, 1 - core)
    across = at(1 - y, z, core)
    middle = at(y, 3 - z, core)
    beside = at(y, 1 - z + 4 * side, core)
    col0 = core * half

    barrier = pltpu.get_barrier_semaphore()
    for dev in (partner, across, beside):
        pl.semaphore_signal(barrier, inc=1, device_id={"tp": dev})

    @pl.when(inner)
    def _():
        pl.semaphore_signal(barrier, inc=1, device_id={"tp": middle})

    def x_copy(c):
        return pltpu.make_async_copy(x.at[pl.ds(c * CHUNK, CHUNK), :], xb, s_x)

    def cs_copies(c):
        rows = pl.ds(c * CHUNK, CHUNK)
        return pltpu.make_async_copy(cos.at[rows, :], cs, s_cs.at[0]), pltpu.make_async_copy(sin.at[rows, :], sn, s_cs.at[1])

    parts = 4
    def w_start(g):
        i = lax.rem(g, 3 * nt)
        kind, tile, slot = lax.div(i, nt), lax.rem(i, nt), lax.rem(g, 2)
        for n, w in enumerate((wq, wk, wv)):
            @pl.when((kind == n) & (g < nch * 3 * nt))
            def _():
                for a in range(parts):
                    rows = pl.ds(a * (d // parts), d // parts)
                    pltpu.make_async_copy(w.at[rows, pl.ds(pl.multiple_of(tile * TILE, TILE), TILE)], wb.at[slot, rows, :], s_w.at[slot]).start()

    def w_wait(g):
        slot = lax.rem(g, 2)
        pltpu.make_async_copy(wq.at[:, pl.ds(0, TILE)], wb.at[slot], s_w.at[slot]).wait()

    def o_copies(n):
        slot, k = lax.rem(n, 2), hl * HEAD
        mine = pl.ds(pl.multiple_of(col0 + n * WO_TILE, WO_TILE), WO_TILE)
        theirs = pl.ds(pl.multiple_of(n * WO_TILE, WO_TILE), WO_TILE)
        return (pltpu.make_async_copy(wo.at[:, mine], ob.at[slot, pl.ds(0, k), :], s_o.at[slot, 0]),
                pltpu.make_async_copy(wo_ext.at[:, theirs], ob.at[slot, pl.ds(k, k), :], s_o.at[slot, 1]))

    def ext_copy():
        return pltpu.make_async_remote_copy(wo.at[:, pl.ds(pl.multiple_of((1 - core) * half, half), half)], wo_ext, s_ext.at[0], s_ext.at[1],
                                            device_id={"tp": partner})

    def seen_copy(c):
        k, b = hl * HEAD, lax.rem(c, 2)
        return pltpu.make_async_remote_copy(seen.at[b, :, pl.ds(0, k)], seen.at[b, :, pl.ds(k, k)], s_seen.at[0, b], s_seen.at[1, b],
                                            device_id={"tp": partner})

    def rs(n, src, dst, dev):
        def make(u):
            b = lax.rem(u, 2)
            return pltpu.make_async_remote_copy(src.at[b], dst.at[lax.rem(u, SLOTS)], s_send.at[n, b], s_rs.at[n, lax.rem(u, SLOTS)],
                                                device_id={"tp": dev})
        return make

    def ag(n, src, rows, height, cols, width, dev):
        def make(u):
            b = lax.rem(u, 2)
            there = out.at[pl.ds(pl.multiple_of(rows(u), 16), height), pl.ds(pl.multiple_of(cols, 128), width)]
            return pltpu.make_async_remote_copy(there if src is None else src.at[b], there, s_send.at[8 + n, b],
                                                s_ag.at[n, lax.rem(u, MARKS)], device_id={"tp": dev})
        return make

    a0 = rs(0, sa0, ra0, across)
    a1f = rs(1, sa1f, ra1f, beside)
    a1n = rs(2, sa1n, ra1n, beside)
    a2 = rs(3, sa2, ra2, middle)
    b0f = rs(4, sb0f, rb0f, beside)
    b0n = rs(5, sb0n, rb0n, beside)
    b1 = rs(6, sb1, rb1, middle)
    b2 = rs(7, sb2, rb2, across)
    ca, cb = col0, col0 + qa
    a_near = lambda u: u * SUB + y * 32 + side * 16
    a_far = lambda u: u * SUB + y * 32 + (1 - side) * 16
    b_own = lambda u: u * SUB + side * 32 + y * 16
    b_near = lambda u: u * SUB + side * 32
    b_far = lambda u: u * SUB + (1 - side) * 32
    a3o = ag(0, fa, a_near, 16, ca, qa, beside)
    a3m = ag(1, fa, a_near, 16, ca, qa, middle)
    a4o = ag(2, None, a_far, 16, ca, qa, beside)
    ayn_i = ag(3, fa, a_near, 16, ca, qa, across)
    ayn_o = ag(3, None, a_near, 16, ca, qa, across)
    ayf = ag(4, None, a_far, 16, ca, qa, across)
    b3y = ag(5, fb, b_own, 16, cb, qa, across)
    b4o = ag(6, None, b_near, 32, cb, qa, beside)
    b4m = ag(7, None, b_near, 32, cb, qa, middle)
    b5o = ag(8, None, b_far, 32, cb, qa, beside)
    d6 = ag(9, None, lambda u: u * SUB, SUB, col0, half, partner)

    def local(n, src, rows, cols):
        def make(u):
            b = lax.rem(u, 2)
            there = out.at[pl.ds(pl.multiple_of(rows(u), 16), 16), pl.ds(pl.multiple_of(cols, 128), qa)]
            return pltpu.make_async_copy(src.at[b], there, s_local.at[n, b])
        return make

    la, lb = local(0, fa, a_near, ca), local(1, fb, b_own, cb)

    def residual(n, dst, rows, cols):
        def make(u):
            b = lax.rem(u, 2)
            return pltpu.make_async_copy(x.at[pl.ds(pl.multiple_of(rows(u), 16), 16), pl.ds(pl.multiple_of(cols, 128), qa)], dst.at[b],
                                         s_res.at[n, b])
        return make

    xa, xbr = residual(0, xa_res, a_near, ca), residual(1, xb_res, b_own, cb)
    A, B = pl.ds(0, qa), pl.ds(qa, qa)

    def mine(u, row, height, cols):
        return pp.at[lax.rem(lax.div(u, PER), 2), pl.ds(pl.multiple_of(lax.rem(u, PER) * SUB + row, 16), height), cols]

    def stage(t, k, sends_i, sends_o, both, on_inner, on_outer):
        u = t - PER - k

        @pl.when((u >= 2) & (u < nsub + 2))
        def _():
            if sends_i is sends_o:
                for m in sends_i:
                    m(u - 2).wait_send()
            else:
                if sends_i:
                    @pl.when(inner)
                    def _():
                        for m in sends_i:
                            m(u - 2).wait_send()
                if sends_o:
                    @pl.when(outer)
                    def _():
                        for m in sends_o:
                            m(u - 2).wait_send()

        @pl.when((u >= 0) & (u < nsub))
        def _():
            s = lax.rem(u, SLOTS)
            if both is not None:
                both(u, lax.rem(u, 2), s)
            if on_inner is not None:
                @pl.when(inner)
                def _():
                    on_inner(u, lax.rem(u, 2), s)
            if on_outer is not None:
                @pl.when(outer)
                def _():
                    on_outer(u, lax.rem(u, 2), s)

    def stage_a0(u, b, s):
        sa0[b] = mine(u, (1 - y) * 32, 32, A)[...].astype(bf16)
        a0(u).start()

    def stage_b0(u, b, s):
        sb0f[b] = mine(u, (1 - side) * 32, 32, B)[...].astype(bf16)
        b0f(u).start()
        sb0n[b] = mine(u, side * 32, 32, B)[...].astype(bf16)
        b0n(u).start()

    def stage_a1(u, b, s):
        a0(u).wait_recv()

    def stage_a1_i(u, b, s):
        own = mine(u, y * 32, 32, A)
        own[...] = own[...] + ra0[s].astype(f32)

    def stage_a1_o(u, b, s):
        sa1f[b] = (mine(u, y * 32 + (1 - side) * 16, 16, A)[...] + ra0[s, pl.ds(pl.multiple_of((1 - side) * 16, 16), 16), :].astype(f32)).astype(bf16)
        a1f(u).start()
        sa1n[b] = (mine(u, y * 32 + side * 16, 16, A)[...] + ra0[s, pl.ds(pl.multiple_of(side * 16, 16), 16), :].astype(f32)).astype(bf16)
        a1n(u).start()

    def stage_b1_i(u, b, s):
        b0f(u).wait_recv()
        sb1[b] = (mine(u, (1 - side) * 32, 32, B)[...] + rb0f[s].astype(f32)).astype(bf16)
        b1(u).start()

    def stage_a2_i(u, b, s):
        xa(u).start()
        a1f(u).wait_recv()
        sa2[b] = (mine(u, y * 32 + (1 - side) * 16, 16, A)[...] + ra1f[s].astype(f32)).astype(bf16)
        a2(u).start()

    def stage_b2_i(u, b, s):
        xbr(u).start()
        b0n(u).wait_recv()
        b1(u).wait_recv()
        theirs = pl.ds(pl.multiple_of((1 - y) * 16, 16), 16)
        sb2[b] = (mine(u, side * 32 + (1 - y) * 16, 16, B)[...] + rb0n[s, theirs, :].astype(f32) + rb1[s, theirs, :].astype(f32)).astype(bf16)
        b2(u).start()
        ours = pl.ds(pl.multiple_of(y * 16, 16), 16)
        own = mine(u, side * 32 + y * 16, 16, B)
        own[...] = own[...] + rb0n[s, ours, :].astype(f32) + rb1[s, ours, :].astype(f32)

    def stage_a3_i(u, b, s):
        @pl.when(u >= 2)
        def _():
            la(u - 2).wait()
        a1n(u).wait_recv()
        a2(u).wait_recv()
        xa(u).wait()
        total = mine(u, y * 32 + side * 16, 16, A)[...] + ra1n[s].astype(f32) + ra2[s].astype(f32)
        fa[b] = (xa_res[b].astype(f32) + total).astype(bf16)
        ayn_i(u).start()
        a3o(u).start()
        a3m(u).start()
        la(u).start()

    def stage_b3_i(u, b, s):
        b2(u).wait_recv()
        xbr(u).wait()
        total = mine(u, side * 32 + y * 16, 16, B)[...] + rb2[s].astype(f32)
        fb[b] = (xb_res[b].astype(f32) + total).astype(bf16)
        b3y(u).start()
        lb(u).start()

    def stage_a4_o(u, b, s):
        a3o(u).wait_recv()
        ayn_o(u).start()

    def stage_a4_i(u, b, s):
        a3m(u).wait_recv()
        ayf(u).start()
        a4o(u).start()

    def stage_b4_i(u, b, s):
        b3y(u).wait_recv()
        lb(u).wait()
        b4o(u).start()
        b4m(u).start()

    def stage_a5_o(u, b, s):
        a4o(u).wait_recv()
        ayf(u).start()

    def stage_b5_i(u, b, s):
        b4m(u).wait_recv()
        b5o(u).start()

    def stage_b5_o(u, b, s):
        b4o(u).wait_recv()

    def stage_6_o(u, b, s):
        b5o(u).wait_recv()

    def stage_6(u, b, s):
        ayn_i(u).wait_recv()
        ayf(u).wait_recv()

    def stage_6_i(u, b, s):
        @pl.when(u >= nsub - 2)
        def _():
            la(u).wait()

    def send_6(u, b, s):
        d6(u).start()

    def stage_7(u, b, s):
        d6(u).wait_recv()

    def exchange(t):
        st = functools.partial(stage, t)
        st(0, [a0], None, stage_a0, None, None) if False else None
        both = [a0]
        st(0, both, both, stage_a0, None, None)
        st(0, [], [b0f, b0n], None, None, stage_b0)
        st(1, [], [a1f, a1n], stage_a1, stage_a1_i, stage_a1_o)
        st(1, [b1], [], None, stage_b1_i, None)
        st(2, [a2], [], None, stage_a2_i, None)
        st(2, [b2], [], None, stage_b2_i, None)
        st(3, [ayn_i, a3o, a3m], [], None, stage_a3_i, None)
        st(3, [b3y], [], None, stage_b3_i, None)
        st(4, [ayf, a4o], [ayn_o], None, stage_a4_i, stage_a4_o)
        st(4, [b4o, b4m], [], None, stage_b4_i, None)
        st(5, [], [ayf], None, None, stage_a5_o)
        st(5, [b5o], [], None, stage_b5_i, stage_b5_o)
        st(6, [], [], None, stage_6_i, stage_6_o)
        st(6, [], [], stage_6, None, None)
        both = [d6]
        st(6, both, both, send_6, None, None)
        st(7, [], [], stage_7, None, None)

    wide = 1024

    def norm():
        def rows(i, _):
            r = pl.ds(pl.multiple_of(i * 16, 16), 16)
            acc = jnp.zeros((16, wide), f32)
            for j in range(0, d, wide):
                v = xb[r, j : j + wide].astype(f32)
                acc = acc + v * v
            scale = lax.rsqrt(jnp.sum(acc, axis=-1, keepdims=True) * (1.0 / d) + 1e-6)
            for j in range(0, d, wide):
                v = xb[r, j : j + wide].astype(f32)
                xb[r, j : j + wide] = (v * scale * gain[:, j : j + wide].astype(f32)).astype(bf16)

        lax.fori_loop(0, CHUNK // 16, rows, None)

    def project(c, s):
        def tile(j, _):
            g = (c * 3 + s) * nt + j
            w_wait(g)
            r = jnp.dot(xb[...], wb[lax.rem(g, 2)], preferred_element_type=f32).astype(bf16)
            w_start(g + 2)
            tokens = pl.ds(pl.multiple_of(c * CHUNK, CHUNK), CHUNK)
            for n in range(TILE // HEAD):
                h = j * (TILE // HEAD) + n
                one = r[:, n * HEAD : (n + 1) * HEAD]

                @pl.when(s < 2)
                def _():
                    w = one.astype(f32)
                    w = (w * cs[...] + pltpu.roll(w, HEAD // 2, 1) * sn[...]).astype(bf16)

                    @pl.when(s == 0)
                    def _():
                        qb[h] = w

                    @pl.when(s == 1)
                    def _():
                        kc[h, tokens, :] = w

                @pl.when(s == 2)
                def _():
                    vt[h, pl.ds(0, HEAD), tokens] = one.T

        lax.fori_loop(0, nt, tile, None)

    e = HEAD**-0.5 * LOG2E

    def attention(c):
        top[...] = jnp.full(top.shape, NEG, f32)
        mix[...] = jnp.zeros(mix.shape, f32)

        def block(j, masked):
            here = pl.ds(pl.multiple_of(j * CHUNK, CHUNK), CHUNK)
            scores = [_dot(kc[h, here, :], qb[h], 1, 1) for h in range(hl)]
            if masked:
                ok = lax.broadcasted_iota(jnp.int32, (CHUNK, CHUNK), 1) >= lax.broadcasted_iota(jnp.int32, (CHUNK, CHUNK), 0)
            weights, keeps = [], []
            for h, s in enumerate(scores):
                if masked:
                    s = jnp.where(ok, s, 2 * NEG)
                old = top[h : h + 1, :]
                new = jnp.maximum(old, s.max(axis=0, keepdims=True))
                top[h : h + 1, :] = new
                weights.append(jnp.exp2((s - new) * e).astype(bf16))
                keeps.append(jnp.exp2((old - new) * e))
            for h in range(hl):
                mix[h] = mix[h] * keeps[h] + _dot(vt[h, :, here], weights[h], 1, 0)

        lax.fori_loop(0, c, lambda j, _: block(j, False), None)
        block(c, True)
        b = lax.rem(c, 2)
        for h in range(hl):
            total = mix[h, HEAD : HEAD + 1, :]
            seen[b, :, h * HEAD : (h + 1) * HEAD] = (mix[h, :HEAD, :] * (1 / total)).T.astype(bf16)

    def output(c):
        b = lax.rem(c, 2)

        def tile(n, _):
            for copy in o_copies(n):
                copy.wait()
            pp[b, :, pl.ds(pl.multiple_of(n * WO_TILE, WO_TILE), WO_TILE)] = jnp.dot(seen[b], ob[lax.rem(n, 2)], preferred_element_type=f32)

            @pl.when(n + 2 < half // WO_TILE)
            def _():
                for copy in o_copies(n + 2):
                    copy.start()

        lax.fori_loop(0, half // WO_TILE, tile, None)

    def compute(t):
        c, s = lax.div(t, PER), lax.rem(t, PER)

        @pl.when(s == 0)
        def _():
            x_copy(c).wait()
            for copy in cs_copies(c):
                copy.wait()
            norm()

        @pl.when(s < 3)
        def _():
            project(c, s)

        @pl.when(s == 2)
        def _():
            @pl.when(c + 1 < nch)
            def _():
                x_copy(c + 1).start()
                for copy in cs_copies(c + 1):
                    copy.start()

            @pl.when(c == 0)
            def _():
                ext_copy().wait_recv()

            for n in range(2):
                for copy in o_copies(n):
                    copy.start()

            @pl.when(c >= 2)
            def _():
                seen_copy(c - 2).wait_send()
            attention(c)
            seen_copy(c).start()

        @pl.when(s == 3)
        def _():
            seen_copy(c).wait_recv()
            output(c)

    x_copy(0).start()
    for copy in cs_copies(0):
        copy.start()
    w_start(0)
    w_start(1)
    for h in range(hl):
        vt[h, HEAD:, :] = jnp.ones((8, vt.shape[2]), bf16)

    @pl.when(inner)
    def _():
        pl.semaphore_wait(barrier, 4)

    @pl.when(outer)
    def _():
        pl.semaphore_wait(barrier, 3)

    ext_copy().start()

    def tick(t, _):
        exchange(t)

        @pl.when(t < nsub)
        def _():
            compute(t)

    lax.fori_loop(0, PER + nsub + LAST + 1, tick, None)
    for c in range(max(nch - 2, 0), nch):
        seen_copy(c).wait_send()
    ext_copy().wait_send()


def layer(x, gain, wq, wk, wv, wo, cos, sin):
    rows, d = x.shape
    hl = wq.shape[1] // HEAD
    half, qa = d // 2, d // 4
    nch = rows // CHUNK
    v, dma = pltpu.VMEM, pltpu.SemaphoreType.DMA
    hbm = pl.BlockSpec(memory_space=pl.ANY)
    r32, r16 = (SLOTS, 32, qa), (SLOTS, 16, qa)
    t32, t16 = (2, 32, qa), (2, 16, qa)
    scratch = [
        v((CHUNK, d), bf16), v((2, d, TILE), bf16), v((2, 2 * hl * HEAD, WO_TILE), bf16), v((hl, rows, HEAD), bf16),
        v((hl, HEAD + 8, rows), bf16), v((hl, CHUNK, HEAD), bf16), v((2, CHUNK, 2 * hl * HEAD), bf16), v((2, CHUNK, half), f32),
        v((hl, HEAD + 8, CHUNK), f32), v((hl, CHUNK), f32), v((CHUNK, HEAD), f32), v((CHUNK, HEAD), f32), v(t16, bf16), v(t16, bf16),
        v(r32, bf16), v(r16, bf16), v(r16, bf16), v(r16, bf16), v(r32, bf16), v(r32, bf16), v(r32, bf16), v(r16, bf16),
        v(t32, bf16), v(t16, bf16), v(t16, bf16), v(t16, bf16), v(t32, bf16), v(t32, bf16), v(t32, bf16), v(t16, bf16),
        v(t16, bf16), v(t16, bf16),
        dma, dma((2,)), dma((2, 2)), dma((2,)), dma((2, 2)), dma((2, 2)), dma((18, 2)), dma((8, SLOTS)), dma((10, MARKS)), dma((2, 2)), dma((2,)),
    ]
    out, _ = pl.pallas_call(
        functools.partial(_kernel, d=d, hl=hl, nch=nch),
        name="layer",
        in_specs=[hbm, pl.BlockSpec(memory_space=pltpu.VMEM), hbm, hbm, hbm, hbm, hbm, hbm],
        out_specs=[hbm, hbm],
        out_shape=[jax.ShapeDtypeStruct((rows, d), bf16), jax.ShapeDtypeStruct((hl * HEAD, half), bf16)],
        scratch_shapes=scratch,
        compiler_params=pltpu.CompilerParams(collective_id=0, has_side_effects=True, vmem_limit_bytes=63 * 2**20),
    )(x, gain, wq, wk, wv, wo, cos, sin)
    return out


def solution(mesh):
    def step(x, gain, wq, wk, wv, wo):
        half = HEAD // 2
        angle = jnp.arange(x.shape[0]).astype(f32)[:, None] * THETA ** (-jnp.arange(half, dtype=f32) / half)
        cos, sin = jnp.cos(angle), jnp.sin(angle)
        return layer(x, gain[None], wq, wk, wv, wo, jnp.concatenate([cos, cos], -1), jnp.concatenate([-sin, sin], -1))

    tokens, columns = P("dp", None), P(None, "tp")
    return jax.shard_map(
        step,
        mesh=mesh,
        in_specs=(tokens, P(None), columns, columns, columns, P("tp", None)),
        out_specs=tokens,
        check_vma=False,
    )
```

```python
import functools

import jax
import jax.numpy as jnp
import numpy as np
from jax import lax
from jax.experimental import pallas as pl
from jax.experimental.pallas import tpu as pltpu
from jax.sharding import PartitionSpec as P

HEAD = 128
THETA = 10000
LOG2E = 1.4426950408889634
NEG = -1e30
CHUNK = 256
SUB = 64
PER = CHUNK // SUB
ROWS = SUB // 2
TILE = 256
WO_TILE = 512
SLOTS = 6
MARKS = 16
SENDS = 3
RS_KINDS, AG_KINDS = 10, 12
A_SHARE = 2 / 3
f32, bf16 = jnp.float32, jnp.bfloat16

STEPS = (
    ("b_i1", 1), ("b_i2", 2), ("b_i3", 4), ("b_o3", 3), ("a_o4", 4), ("b_o4", 4), ("b_o5", 5), ("a_i6", 6), ("b_en", 8),
    ("b_o0", 0), ("a_s0", 0), ("a_o7", 7), ("a_i5", 5), ("a_i3", 3), ("a_o5", 6), ("a_en", 8), ("a_i1", 2), ("a_o1", 1),
    ("d_w", 11), ("a_i2", 2), ("b_ef", 8), ("a_ox", 3), ("a_ef", 8), ("d_s", 8), ("b_i6", 6), ("b_i7", 7), ("b_i4", 5),
)
AFTER = dict(STEPS)


def _dot(a, b, ca, cb):
    return lax.dot_general(a, b, (((ca,), (cb,)), ((), ())), preferred_element_type=f32)


def _split(half):
    return min(max(round(half * A_SHARE / 512), 1), half // 512 - 1) * 512


def _kernel(x, gain, wq, wk, wv, wo, cos, sin, out, wo_ext, xb, wb, ob, kc, vt, qb, seen, pp, mix, top, cs, sn, xa_res, xb_res,
            ra0, rafar, rani, ramid, rbfar, rbni, rbmid, rbgy, sa0, safar, sani, sbfar, sbni, sbgy, fa, fb,
            s_x, s_w, s_o, s_cs, s_res, s_local, s_send, s_rs, s_ag, s_seen, s_ext, *, d, hl, nch):
    half = d // 2
    wa = _split(half)
    qa, qb_ = wa // 4, (half - wa) // 4
    nt = hl * HEAD // TILE
    nsub = nch * PER
    pos = lax.axis_index("tp")
    y, z, core = lax.div(pos, 8), lax.rem(lax.div(pos, 2), 4), lax.rem(pos, 2)
    side = lax.div(z, 2)
    inner = (z == 1) | (z == 2)
    outer = (z == 0) | (z == 3)

    def at(y, z, core):
        return (y * 4 + z) * 2 + core

    partner = at(y, z, 1 - core)
    across = at(1 - y, z, core)
    middle = at(y, 3 - z, core)
    beside = at(y, 1 - z + 4 * side, core)
    col0 = core * half

    barrier = pltpu.get_barrier_semaphore()
    for dev in (partner, across, beside):
        pl.semaphore_signal(barrier, inc=1, device_id={"tp": dev})

    @pl.when(inner)
    def _():
        pl.semaphore_signal(barrier, inc=1, device_id={"tp": middle})

    def x_copy(c):
        return pltpu.make_async_copy(x.at[pl.ds(c * CHUNK, CHUNK), :], xb, s_x)

    def cs_copies(c):
        rows = pl.ds(c * CHUNK, CHUNK)
        return pltpu.make_async_copy(cos.at[rows, :], cs, s_cs.at[0]), pltpu.make_async_copy(sin.at[rows, :], sn, s_cs.at[1])

    parts = 4
    def w_start(g):
        i = lax.rem(g, 3 * nt)
        kind, tile, slot = lax.div(i, nt), lax.rem(i, nt), lax.rem(g, 2)
        for n, w in enumerate((wq, wk, wv)):
            @pl.when((kind == n) & (g < nch * 3 * nt))
            def _():
                for a in range(parts):
                    rows = pl.ds(a * (d // parts), d // parts)
                    pltpu.make_async_copy(w.at[rows, pl.ds(pl.multiple_of(tile * TILE, TILE), TILE)], wb.at[slot, rows, :], s_w.at[slot]).start()

    def w_wait(g):
        slot = lax.rem(g, 2)
        pltpu.make_async_copy(wq.at[:, pl.ds(0, TILE)], wb.at[slot], s_w.at[slot]).wait()

    def o_copies(n):
        slot, k = lax.rem(n, 2), hl * HEAD
        mine = pl.ds(pl.multiple_of(col0 + n * WO_TILE, WO_TILE), WO_TILE)
        theirs = pl.ds(pl.multiple_of(n * WO_TILE, WO_TILE), WO_TILE)
        return (pltpu.make_async_copy(wo.at[:, mine], ob.at[slot, pl.ds(0, k), :], s_o.at[slot, 0]),
                pltpu.make_async_copy(wo_ext.at[:, theirs], ob.at[slot, pl.ds(k, k), :], s_o.at[slot, 1]))

    def ext_copy():
        return pltpu.make_async_remote_copy(wo.at[:, pl.ds(pl.multiple_of((1 - core) * half, half), half)], wo_ext, s_ext.at[0], s_ext.at[1],
                                            device_id={"tp": partner})

    def seen_copy(c):
        k, b = hl * HEAD, lax.rem(c, 2)
        return pltpu.make_async_remote_copy(seen.at[b, :, pl.ds(0, k)], seen.at[b, :, pl.ds(k, k)], s_seen.at[0, b], s_seen.at[1, b],
                                            device_id={"tp": partner})

    kinds = {}

    def number(table, name):
        return kinds.setdefault((table, name), sum(t == table for t, _ in kinds))

    def rs(name, src, dst, dev):
        n = number("rs", name)

        def make(u):
            b = lax.rem(u, SENDS)
            return pltpu.make_async_remote_copy(src.at[b], dst.at[lax.rem(u, SLOTS)], s_send.at[n, b], s_rs.at[n, lax.rem(u, SLOTS)],
                                                device_id={"tp": dev})
        return make

    def place(row, height, col, width):
        return lambda u: (pl.ds(pl.multiple_of(u * SUB + row, 16), height), pl.ds(pl.multiple_of(col0 + col, 128), width))

    def ag(name, src, where, dev):
        n = number("ag", name)

        def make(u):
            b = lax.rem(u, SENDS)
            there = out.at[where(u)]
            return pltpu.make_async_remote_copy(there if src is None else src.at[b], there, s_send.at[RS_KINDS + n, b],
                                                s_ag.at[n, lax.rem(u, MARKS)], device_id={"tp": dev})
        return make

    def local(n, src, where):
        def make(u):
            b = lax.rem(u, SENDS)
            return pltpu.make_async_copy(src.at[b], out.at[where(u)], s_local.at[n, b])
        return make

    def residual(n, dst, where):
        def make(u):
            b = lax.rem(u, 4)
            return pltpu.make_async_copy(x.at[where(u)], dst.at[b], s_res.at[n, b])
        return make

    mine = y * ROWS
    a_near, a_far = side * 2 * qa, (1 - side) * 2 * qa
    b_near, b_far = wa + side * 2 * qb_, wa + (1 - side) * 2 * qb_
    a_in, a_out = a_near + (1 - side) * qa, a_near + side * qa
    b_in, b_out = b_near + (1 - side) * qb_, b_near + side * qb_
    a_i, a_o, b_i, b_o = (pl.ds(pl.multiple_of(n * q, 128), q) for n, q in ((1 - side, qa), (side, qa), (1 - side, qb_), (side, qb_)))

    a0 = rs("a0", sa0, ra0, across)
    afar = rs("afar", safar, rafar, beside)
    ani = rs("ani", sani, rani, beside)
    amid = rs("amid", safar, ramid, middle)
    arno = rs("arno", sani, rani, beside)
    bfar = rs("bfar", sbfar, rbfar, beside)
    bni = rs("bni", sbni, rbni, beside)
    bmid = rs("bmid", sbfar, rbmid, middle)
    brno = rs("brno", sbni, rbni, beside)
    bgy = rs("bgy", sbgy, rbgy, across)

    afo = ag("afo", fa, place(mine, ROWS, a_in, qa), beside)
    aof = ag("aof", fa, place(mine, ROWS, a_out, qa), beside)
    ayn = ag("ayn", None, place(mine, ROWS, a_near, 2 * qa), across)
    ayf = ag("ayf", None, place(mine, ROWS, a_far, 2 * qa), across)
    agm = ag("agm", None, place(mine, ROWS, a_near, 2 * qa), middle)
    afm = ag("afm", None, place(mine, ROWS, a_far, 2 * qa), beside)
    bfy_i = ag("bfy", fb, place(mine, ROWS, b_in, qb_), across)
    bfy_o = ag("bfy", fb, place(mine, ROWS, b_out, qb_), across)
    bfo = ag("bfo", None, place(0, SUB, b_in, qb_), beside)
    bof = ag("bof", None, place(0, SUB, b_out, qb_), beside)
    bgm = ag("bgm", None, place(0, SUB, b_near, 2 * qb_), middle)
    bfm = ag("bfm", None, place(0, SUB, b_far, 2 * qb_), beside)
    share = ag("share", None, place(0, SUB, 0, half), partner)
    la_i, la_o = (local(0, fa, place(mine, ROWS, c, qa)) for c in (a_in, a_out))
    lb_i, lb_o = (local(1, fb, place(mine, ROWS, c, qb_)) for c in (b_in, b_out))
    xa_i, xa_o = (residual(0, xa_res, place(mine, ROWS, c, qa)) for c in (a_in, a_out))
    xb_i, xb_o = (residual(1, xb_res, place(mine, ROWS, c, qb_)) for c in (b_in, b_out))

    def term(u, row, height, col, width):
        rows = pl.ds(pl.multiple_of(lax.rem(u, PER) * SUB + row, 16), height)
        return pp.at[lax.rem(lax.div(u, PER), 2), rows, pl.ds(pl.multiple_of(col, 128), width)]

    def wide(ref):
        return ref[...].astype(f32)

    def put(ref, value):
        ref[...] = value.astype(bf16)

    ours, theirs = pl.ds(pl.multiple_of(y * ROWS, 16), ROWS), pl.ds(pl.multiple_of((1 - y) * ROWS, 16), ROWS)

    def a_s0(u, b, s, r):
        put(sa0.at[b], term(u, (1 - y) * ROWS, ROWS, 0, wa)[...])
        a0(u).start()

    def a_o1(u, b, s, r):
        a0(u).wait_recv()

        def part(col, width):
            return term(u, mine, ROWS, col, width)[...] + wide(ra0.at[s, :, pl.ds(pl.multiple_of(col, 128), width)])

        put(safar.at[b], part(a_far, 2 * qa))
        afar(u).start()
        put(sani.at[b], part(a_in, qa))
        ani(u).start()
        term(u, mine, ROWS, a_out, qa)[...] = part(a_out, qa)

    def a_i1(u, b, s, r):
        a0(u).wait_recv()
        own = term(u, mine, ROWS, 0, wa)
        own[...] = own[...] + wide(ra0.at[s])

    def a_i2(u, b, s, r):
        xa_i(u).start()
        afar(u).wait_recv()
        put(safar.at[b], term(u, mine, ROWS, a_far, 2 * qa)[...] + wide(rafar.at[s]))
        amid(u).start()

    def a_i3(u, b, s, r):
        amid(u).wait_recv()
        put(sani.at[b], term(u, mine, ROWS, a_out, qa)[...] + wide(ramid.at[s, :, a_o]))
        arno(u).start()
        ani(u).wait_recv()
        xa_i(u).wait()
        put(fa.at[b], wide(xa_res.at[r]) + (term(u, mine, ROWS, a_in, qa)[...] + wide(ramid.at[s, :, a_i]) + wide(rani.at[s])))
        afo(u).start()
        la_i(u).start()

    def a_ox(u, b, s, r):
        xa_o(u).start()

    def a_o4(u, b, s, r):
        arno(u).wait_recv()
        xa_o(u).wait()
        put(fa.at[b], wide(xa_res.at[r]) + (term(u, mine, ROWS, a_out, qa)[...] + wide(rani.at[s])))
        aof(u).start()
        la_o(u).start()

    def a_o5(u, b, s, r):
        la_o(u).wait()
        afo(u).wait_recv()
        ayn(u).start()

    def a_i5(u, b, s, r):
        la_i(u).wait()
        aof(u).wait_recv()
        agm(u).start()
        ayn(u).start()

    def a_i6(u, b, s, r):
        agm(u).wait_recv()
        afm(u).start()
        ayf(u).start()

    def a_o7(u, b, s, r):
        afm(u).wait_recv()
        ayf(u).start()

    def a_en(u, b, s, r):
        ayn(u).wait_recv()

    def a_ef(u, b, s, r):
        ayf(u).wait_recv()

    def b_o0(u, b, s, r):
        put(sbfar.at[b], term(u, 0, SUB, b_far, 2 * qb_)[...])
        bfar(u).start()
        put(sbni.at[b], term(u, 0, SUB, b_in, qb_)[...])
        bni(u).start()

    def b_i1(u, b, s, r):
        bfar(u).wait_recv()
        put(sbfar.at[b], term(u, 0, SUB, b_far, 2 * qb_)[...] + wide(rbfar.at[s]))
        bmid(u).start()

    def b_i2(u, b, s, r):
        xb_i(u).start()
        bmid(u).wait_recv()
        put(sbni.at[b], term(u, 0, SUB, b_out, qb_)[...] + wide(rbmid.at[s, :, b_o]))
        brno(u).start()
        bni(u).wait_recv()
        put(sbgy.at[b], term(u, (1 - y) * ROWS, ROWS, b_in, qb_)[...] + wide(rbmid.at[s, theirs, b_i]) + wide(rbni.at[s, theirs, :]))
        bgy(u).start()
        own = term(u, mine, ROWS, b_in, qb_)
        own[...] = own[...] + wide(rbmid.at[s, ours, b_i]) + wide(rbni.at[s, ours, :])

    def b_o3(u, b, s, r):
        xb_o(u).start()
        brno(u).wait_recv()
        put(sbgy.at[b], term(u, (1 - y) * ROWS, ROWS, b_out, qb_)[...] + wide(rbni.at[s, theirs, :]))
        bgy(u).start()
        own = term(u, mine, ROWS, b_out, qb_)
        own[...] = own[...] + wide(rbni.at[s, ours, :])

    def finish_b(u, b, s, r, col, res, send, keep):
        bgy(u).wait_recv()
        res(u).wait()
        put(fb.at[b], wide(xb_res.at[r]) + (term(u, mine, ROWS, col, qb_)[...] + wide(rbgy.at[s])))
        send(u).start()
        keep(u).start()

    def b_i3(u, b, s, r):
        finish_b(u, b, s, r, b_in, xb_i, bfy_i, lb_i)

    def b_o4(u, b, s, r):
        finish_b(u, b, s, r, b_out, xb_o, bfy_o, lb_o)

    def b_i4(u, b, s, r):
        lb_i(u).wait()
        bfy_i(u).wait_recv()
        bfo(u).start()

    def b_o5(u, b, s, r):
        lb_o(u).wait()
        bfy_o(u).wait_recv()
        bof(u).start()

    def b_i6(u, b, s, r):
        bof(u).wait_recv()
        bgm(u).start()

    def b_i7(u, b, s, r):
        bgm(u).wait_recv()
        bfm(u).start()

    def b_en(u, b, s, r):
        bfo(u).wait_recv()

    def b_ef(u, b, s, r):
        bfm(u).wait_recv()

    def d_s(u, b, s, r):
        share(u).start()

    def d_w(u, b, s, r):
        share(u).wait_recv()

    steps = {
        "a_s0": (a_s0, [a0]), "a_o1": (a_o1, [afar, ani]), "a_i1": (a_i1, []), "a_i2": (a_i2, [amid]), "a_i3": (a_i3, [arno, afo]),
        "a_ox": (a_ox, []), "a_o4": (a_o4, [aof]), "a_o5": (a_o5, [ayn]), "a_i5": (a_i5, [agm, ayn]), "a_i6": (a_i6, [afm, ayf]),
        "a_o7": (a_o7, [ayf]), "a_en": (a_en, []), "a_ef": (a_ef, []), "b_o0": (b_o0, [bfar, bni]), "b_i1": (b_i1, [bmid]),
        "b_i2": (b_i2, [brno, bgy]), "b_o3": (b_o3, [bgy]), "b_i3": (b_i3, [bfy_i]), "b_o4": (b_o4, [bfy_o]), "b_i4": (b_i4, [bfo]),
        "b_o5": (b_o5, [bof]), "b_i6": (b_i6, [bgm]), "b_i7": (b_i7, [bfm]), "b_en": (b_en, []), "b_ef": (b_ef, []),
        "d_s": (d_s, [share]), "d_w": (d_w, []),
    }

    def role(name):
        return {"i": inner, "o": outer}.get(name[2]) if name not in ("b_en", "b_ef") else outer

    def exchange(t):
        for name, after in STEPS:
            do, sends = steps[name]
            u = t - PER - after
            go = (u >= 0) & (u < nsub)
            if role(name) is not None:
                go = go & role(name)

            @pl.when(go)
            def _():
                if sends:
                    @pl.when(u >= SENDS)
                    def _():
                        for m in sends:
                            m(u - SENDS).wait_send()
                do(u, lax.rem(u, SENDS), lax.rem(u, SLOTS), lax.rem(u, 4))

    def drain():
        for name, _ in STEPS:
            def leave(sends=steps[name][1]):
                for m in sends:
                    for u in range(max(nsub - SENDS, 0), nsub):
                        m(u).wait_send()
            if role(name) is None:
                leave()
            elif steps[name][1]:
                pl.when(role(name))(leave)

    lanes = 1024

    def norm():
        def rows(i, _):
            r = pl.ds(pl.multiple_of(i * 16, 16), 16)
            acc = jnp.zeros((16, lanes), f32)
            for j in range(0, d, lanes):
                v = xb[r, j : j + lanes].astype(f32)
                acc = acc + v * v
            scale = lax.rsqrt(jnp.sum(acc, axis=-1, keepdims=True) * (1.0 / d) + 1e-6)
            for j in range(0, d, lanes):
                v = xb[r, j : j + lanes].astype(f32)
                xb[r, j : j + lanes] = (v * scale * gain[pl.ds(j, lanes)].astype(f32)[None]).astype(bf16)

        lax.fori_loop(0, CHUNK // 16, rows, None)

    def project(c, s):
        def first(s):
            return jnp.minimum(s * nt + lax.div(s, 2) * (nt // 3), 3 * nt)

        def tile(i, _):
            g, kind, j = c * 3 * nt + i, lax.div(i, nt), lax.rem(i, nt)
            w_wait(g)
            r = jnp.dot(xb[...], wb[lax.rem(g, 2)], preferred_element_type=f32).astype(bf16)
            w_start(g + 2)
            tokens = pl.ds(pl.multiple_of(c * CHUNK, CHUNK), CHUNK)
            for n in range(TILE // HEAD):
                h = j * (TILE // HEAD) + n
                one = r[:, n * HEAD : (n + 1) * HEAD]

                @pl.when(kind < 2)
                def _():
                    w = one.astype(f32)
                    w = (w * cs[...] + pltpu.roll(w, HEAD // 2, 1) * sn[...]).astype(bf16)

                    @pl.when(kind == 0)
                    def _():
                        qb[h] = w

                    @pl.when(kind == 1)
                    def _():
                        kc[h, tokens, :] = w

                @pl.when(kind == 2)
                def _():
                    vt[h, pl.ds(0, HEAD), tokens] = one.T

        lax.fori_loop(first(s), first(s + 1), tile, None)

    e = HEAD**-0.5 * LOG2E

    def attention(c):
        top[...] = jnp.full(top.shape, NEG, f32)
        mix[...] = jnp.zeros(mix.shape, f32)

        def block(j, masked):
            here = pl.ds(pl.multiple_of(j * CHUNK, CHUNK), CHUNK)
            scores = [_dot(kc[h, here, :], qb[h], 1, 1) for h in range(hl)]
            if masked:
                ok = lax.broadcasted_iota(jnp.int32, (CHUNK, CHUNK), 1) >= lax.broadcasted_iota(jnp.int32, (CHUNK, CHUNK), 0)
            weights, keeps = [], []
            for h, s in enumerate(scores):
                if masked:
                    s = jnp.where(ok, s, 2 * NEG)
                old = top[h : h + 1, :]
                new = jnp.maximum(old, s.max(axis=0, keepdims=True))
                top[h : h + 1, :] = new
                weights.append(jnp.exp2((s - new) * e).astype(bf16))
                keeps.append(jnp.exp2((old - new) * e))
            for h in range(hl):
                mix[h] = mix[h] * keeps[h] + _dot(vt[h, :, here], weights[h], 1, 0)

        lax.fori_loop(0, c, lambda j, _: block(j, False), None)
        block(c, True)
        b = lax.rem(c, 2)
        for h in range(hl):
            total = mix[h, HEAD : HEAD + 1, :]
            seen[b, :, h * HEAD : (h + 1) * HEAD] = (mix[h, :HEAD, :] * (1 / total)).T.astype(bf16)

    def output(c):
        b = lax.rem(c, 2)

        def tile(n, _):
            for copy in o_copies(n):
                copy.wait()
            pp[b, :, pl.ds(pl.multiple_of(n * WO_TILE, WO_TILE), WO_TILE)] = jnp.dot(seen[b], ob[lax.rem(n, 2)], preferred_element_type=f32)

            @pl.when(n + 2 < half // WO_TILE)
            def _():
                for copy in o_copies(n + 2):
                    copy.start()

        lax.fori_loop(0, half // WO_TILE, tile, None)

    def compute(t):
        c, s = lax.div(t, PER), lax.rem(t, PER)

        @pl.when(s == 0)
        def _():
            x_copy(c).wait()
            for copy in cs_copies(c):
                copy.wait()
            norm()

        @pl.when(s < 3)
        def _():
            project(c, s)

        @pl.when(s == 2)
        def _():
            @pl.when(c + 1 < nch)
            def _():
                x_copy(c + 1).start()
                for copy in cs_copies(c + 1):
                    copy.start()

            @pl.when(c == 0)
            def _():
                ext_copy().wait_recv()

            for n in range(2):
                for copy in o_copies(n):
                    copy.start()

            @pl.when(c >= 2)
            def _():
                seen_copy(c - 2).wait_send()
            attention(c)
            seen_copy(c).start()

        @pl.when(s == 3)
        def _():
            seen_copy(c).wait_recv()
            output(c)

    x_copy(0).start()
    for copy in cs_copies(0):
        copy.start()
    w_start(0)
    w_start(1)
    for h in range(hl):
        vt[h, HEAD:, :] = jnp.ones((8, vt.shape[2]), bf16)

    @pl.when(inner)
    def _():
        pl.semaphore_wait(barrier, 4)

    @pl.when(outer)
    def _():
        pl.semaphore_wait(barrier, 3)

    ext_copy().start()


    def tick(t, _):
        exchange(t)

        @pl.when(t < nsub)
        def _():
            compute(t)

    lax.fori_loop(0, PER + nsub + max(AFTER.values()), tick, None)
    drain()
    for c in range(max(nch - 2, 0), nch):
        seen_copy(c).wait_send()
    ext_copy().wait_send()


def layer(x, gain, wq, wk, wv, wo, cos, sin):
    rows, d = x.shape
    hl = wq.shape[1] // HEAD
    half, qa = d // 2, d // 4
    nch = rows // CHUNK
    v, dma = pltpu.VMEM, pltpu.SemaphoreType.DMA
    hbm = pl.BlockSpec(memory_space=pl.ANY)
    wa = _split(half)
    qa, qb = wa // 4, (half - wa) // 4

    def buffers(n, *shapes):
        return [v((n, *s), bf16) for s in shapes]

    scratch = [
        v((CHUNK, d), bf16), v((2, d, TILE), bf16), v((2, 2 * hl * HEAD, WO_TILE), bf16), v((hl, rows, HEAD), bf16),
        v((hl, HEAD + 8, rows), bf16), v((hl, CHUNK, HEAD), bf16), v((2, CHUNK, 2 * hl * HEAD), bf16), v((2, CHUNK, half), f32),
        v((hl, HEAD + 8, CHUNK), f32), v((hl, CHUNK), f32), v((CHUNK, HEAD), f32), v((CHUNK, HEAD), f32),
        *buffers(4, (ROWS, qa), (ROWS, qb)),
        *buffers(SLOTS, (ROWS, wa), (ROWS, 2 * qa), (ROWS, qa), (ROWS, 2 * qa), (SUB, 2 * qb), (SUB, qb), (SUB, 2 * qb), (ROWS, qb)),
        *buffers(SENDS, (ROWS, wa), (ROWS, 2 * qa), (ROWS, qa), (SUB, 2 * qb), (SUB, qb), (ROWS, qb), (ROWS, qa), (ROWS, qb)),
        dma, dma((2,)), dma((2, 2)), dma((2,)), dma((2, 4)), dma((2, SENDS)), dma((RS_KINDS + AG_KINDS, SENDS)), dma((RS_KINDS, SLOTS)),
        dma((AG_KINDS, MARKS)), dma((2, 2)), dma((2,)),
    ]
    out, _ = pl.pallas_call(
        functools.partial(_kernel, d=d, hl=hl, nch=nch),
        name="layer",
        in_specs=[hbm, pl.BlockSpec(memory_space=pltpu.VMEM), hbm, hbm, hbm, hbm, hbm, hbm],
        out_specs=[hbm, hbm],
        out_shape=[jax.ShapeDtypeStruct((rows, d), bf16), jax.ShapeDtypeStruct((hl * HEAD, half), bf16)],
        scratch_shapes=scratch,
        compiler_params=pltpu.CompilerParams(collective_id=0, has_side_effects=True, vmem_limit_bytes=63 * 2**20),
    )(x, gain, wq, wk, wv, wo, cos, sin)
    return out


def solution(mesh):
    def step(x, gain, wq, wk, wv, wo):
        half = HEAD // 2
        angle = np.arange(x.shape[0], dtype=np.float32)[:, None] * np.float32(THETA) ** (-np.arange(half, dtype=np.float32) / half)
        cos, sin = np.cos(angle), np.sin(angle)
        cos, sin = (jnp.asarray(np.concatenate(t, -1), f32) for t in ([cos, cos], [-sin, sin]))
        return layer(x, gain, wq, wk, wv, wo, cos, sin)

    tokens, columns = P("dp", None), P(None, "tp")
    return jax.shard_map(
        step,
        mesh=mesh,
        in_specs=(tokens, P(None), columns, columns, columns, P("tp", None)),
        out_specs=tokens,
        check_vma=False,
    )
```

```python
import functools

import jax
import jax.numpy as jnp
import numpy as np
from jax import lax
from jax.experimental import pallas as pl
from jax.experimental.pallas import tpu as pltpu
from jax.sharding import PartitionSpec as P

HEAD = 128
THETA = 10000
LOG2E = 1.4426950408889634
NEG = -1e30
CHUNK = 256
SUB = 32
PER = CHUNK // SUB
ROWS = SUB // 2
PARTS = 16
TILE = 256
HELD = 5
WO_TILE = 512
WO_HELD = 3
SLOTS = 6
IMAGES = 14
MARKS = 16
SENDS = 3
RS_KINDS, AG_KINDS = 10, 12
A_SHARE = 7 / 12
f32, bf16 = jnp.float32, jnp.bfloat16

STEPS = (
    ("a_en", 8), ("d_w", 13), ("b_i1", 1), ("b_o5", 6), ("b_i4", 4), ("b_ef", 11), ("b_i3", 3), ("a_o5", 5), ("a_ef", 11),
    ("b_i2", 2), ("a_i3", 3), ("a_i2", 2), ("b_o0", 0), ("a_s0", 0), ("a_o7", 8), ("a_ox", 2), ("a_o1", 1), ("a_i5", 5),
    ("H1", 0), ("a_i6", 6), ("a_o4", 4), ("b_o4", 4), ("b_i6", 6), ("b_o3", 3), ("a_i1", 1), ("b_i7", 7), ("d_s", 11),
    ("b_en", 8), ("H2", 0),
)
AFTER = dict(STEPS)


def _dot(a, b, ca, cb):
    return lax.dot_general(a, b, (((ca,), (cb,)), ((), ())), preferred_element_type=f32)


def _split(half):
    return min(max(round(half * A_SHARE / 512), 1), half // 512 - 1) * 512


def _kernel(x, gain, wq, wk, wv, wo, cos, sin, out, wo_ext, xb, wb, ob, kc, vt, qb, seen, pp, mix, top, cs, sn, xa_res, xb_res,
            ra0, rafar, rani, ramid, rbfar, rbni, rbmid, rbgy, sa0, safar, sani, sbfar, sbni, sbgy, img,
            s_x, s_w, s_o, s_cs, s_res, s_local, s_send, s_rs, s_ag, s_seen, s_ext, *, d, hl, nch):
    half = d // 2
    wa = _split(half)
    qa, qb_ = wa // 4, (half - wa) // 4
    nt = hl * HEAD // TILE
    nsub = nch * PER
    pos = lax.axis_index("tp")
    y, z, core = lax.div(pos, 8), lax.rem(lax.div(pos, 2), 4), lax.rem(pos, 2)
    side = lax.div(z, 2)
    inner = (z == 1) | (z == 2)
    outer = (z == 0) | (z == 3)

    def at(y, z, core):
        return (y * 4 + z) * 2 + core

    partner = at(y, z, 1 - core)
    across = at(1 - y, z, core)
    middle = at(y, 3 - z, core)
    beside = at(y, 1 - z + 4 * side, core)
    col0 = core * half

    barrier = pltpu.get_barrier_semaphore()
    for dev in (partner, across, beside):
        pl.semaphore_signal(barrier, inc=1, device_id={"tp": dev})

    @pl.when(inner)
    def _():
        pl.semaphore_signal(barrier, inc=1, device_id={"tp": middle})

    def x_copy(c):
        return pltpu.make_async_copy(x.at[pl.ds(c * CHUNK, CHUNK), :], xb, s_x)

    def cs_copies(c):
        rows = pl.ds(c * CHUNK, CHUNK)
        return pltpu.make_async_copy(cos.at[rows, :], cs, s_cs.at[0]), pltpu.make_async_copy(sin.at[rows, :], sn, s_cs.at[1])

    k2, cuts = d // 2, 2

    def w_start(h):
        i, part, slot = lax.rem(lax.div(h, 2), 3 * nt), lax.rem(h, 2), lax.rem(h, HELD)
        kind, tile = lax.div(i, nt), lax.rem(i, nt)
        for n, w in enumerate((wq, wk, wv)):
            @pl.when((kind == n) & (h < nch * 3 * nt * 2))
            def _():
                for a in range(cuts):
                    rows = pl.ds(pl.multiple_of(part * k2 + a * (k2 // cuts), k2 // cuts), k2 // cuts)
                    pltpu.make_async_copy(w.at[rows, pl.ds(pl.multiple_of(tile * TILE, TILE), TILE)],
                                          wb.at[slot, pl.ds(a * (k2 // cuts), k2 // cuts), :], s_w.at[slot]).start()

    def w_wait(h):
        slot = lax.rem(h, HELD)
        pltpu.make_async_copy(wq.at[pl.ds(0, k2), pl.ds(0, TILE)], wb.at[slot], s_w.at[slot]).wait()

    def o_copies(n):
        slot, k = lax.rem(n, WO_HELD), hl * HEAD
        mine = pl.ds(pl.multiple_of(col0 + n * WO_TILE, WO_TILE), WO_TILE)
        theirs = pl.ds(pl.multiple_of(n * WO_TILE, WO_TILE), WO_TILE)
        return (pltpu.make_async_copy(wo.at[:, mine], ob.at[slot, pl.ds(0, k), :], s_o.at[slot, 0]),
                pltpu.make_async_copy(wo_ext.at[:, theirs], ob.at[slot, pl.ds(k, k), :], s_o.at[slot, 1]))

    def ext_copy():
        return pltpu.make_async_remote_copy(wo.at[:, pl.ds(pl.multiple_of((1 - core) * half, half), half)], wo_ext, s_ext.at[0], s_ext.at[1],
                                            device_id={"tp": partner})

    def seen_copy(c):
        k, b = hl * HEAD, lax.rem(c, 2)
        return pltpu.make_async_remote_copy(seen.at[b, :, pl.ds(0, k)], seen.at[b, :, pl.ds(k, k)], s_seen.at[0, b], s_seen.at[1, b],
                                            device_id={"tp": partner})

    kinds = {}

    def number(table, name):
        return kinds.setdefault((table, name), sum(t == table for t, _ in kinds))

    def rs(name, src, dst, dev):
        n = number("rs", name)

        def make(u):
            b = lax.rem(u, SENDS)
            return pltpu.make_async_remote_copy(src.at[b], dst.at[lax.rem(u, SLOTS)], s_send.at[n, b], s_rs.at[n, lax.rem(u, SLOTS)],
                                                device_id={"tp": dev})
        return make

    def place(row, height, col, width):
        return lambda u: (pl.ds(pl.multiple_of(u * SUB + row, 16), height), pl.ds(pl.multiple_of(col0 + col, 128), width))

    def ag(name, where, dev):
        n = number("ag", name)

        def make(u):
            there = img.at[(lax.rem(u, IMAGES), *where)]
            return pltpu.make_async_remote_copy(there, there, s_send.at[RS_KINDS + n, lax.rem(u, SENDS)], s_ag.at[n, lax.rem(u, MARKS)],
                                                device_id={"tp": dev})
        return make

    def part(row, height, col, width):
        return pl.ds(pl.multiple_of(row, 16), height), pl.ds(pl.multiple_of(col, 128), width)

    def rows_of(u):
        return out.at[pl.ds(pl.multiple_of(u * SUB, 16), SUB), pl.ds(pl.multiple_of(col0, 128), half)]

    def share(u):
        n = number("ag", "share")
        return pltpu.make_async_remote_copy(img.at[lax.rem(u, IMAGES)], rows_of(u), s_send.at[RS_KINDS + n, lax.rem(u, SENDS)],
                                            s_ag.at[n, lax.rem(u, MARKS)], device_id={"tp": partner})

    def keep(u):
        return pltpu.make_async_copy(img.at[lax.rem(u, IMAGES)], rows_of(u), s_local.at[lax.rem(u, SENDS)])

    def residual(n, dst, where):
        def make(u):
            b = lax.rem(u, 4)
            return pltpu.make_async_copy(x.at[where(u)], dst.at[b], s_res.at[n, b])
        return make

    mine = y * ROWS
    a_near, a_far = side * 2 * qa, (1 - side) * 2 * qa
    b_near, b_far = wa + side * 2 * qb_, wa + (1 - side) * 2 * qb_
    a_in, a_out = a_near + (1 - side) * qa, a_near + side * qa
    b_in, b_out = b_near + (1 - side) * qb_, b_near + side * qb_
    a_i, a_o, b_i, b_o = (pl.ds(pl.multiple_of(n * q, 128), q) for n, q in ((1 - side, qa), (side, qa), (1 - side, qb_), (side, qb_)))

    a0 = rs("a0", sa0, ra0, across)
    afar = rs("afar", safar, rafar, beside)
    ani = rs("ani", sani, rani, beside)
    amid = rs("amid", safar, ramid, middle)
    arno = rs("arno", sani, rani, beside)
    bfar = rs("bfar", sbfar, rbfar, beside)
    bni = rs("bni", sbni, rbni, beside)
    bmid = rs("bmid", sbfar, rbmid, middle)
    brno = rs("brno", sbni, rbni, beside)
    bgy = rs("bgy", sbgy, rbgy, across)

    afo = ag("afo", part(mine, ROWS, a_in, qa), beside)
    aof = ag("aof", part(mine, ROWS, a_out, qa), beside)
    ayn = ag("ayn", part(mine, ROWS, a_near, 2 * qa), across)
    ayf = ag("ayf", part(mine, ROWS, a_far, 2 * qa), across)
    agm = ag("agm", part(mine, ROWS, a_near, 2 * qa), middle)
    afm = ag("afm", part(mine, ROWS, a_far, 2 * qa), beside)
    bfy_i = ag("bfy", part(mine, ROWS, b_in, qb_), across)
    bfy_o = ag("bfy", part(mine, ROWS, b_out, qb_), across)
    bfo = ag("bfo", part(0, SUB, b_in, qb_), beside)
    bof = ag("bof", part(0, SUB, b_out, qb_), beside)
    bgm = ag("bgm", part(0, SUB, b_near, 2 * qb_), middle)
    bfm = ag("bfm", part(0, SUB, b_far, 2 * qb_), beside)
    xa_i, xa_o = (residual(0, xa_res, place(mine, ROWS, c, qa)) for c in (a_in, a_out))
    xb_i, xb_o = (residual(1, xb_res, place(mine, ROWS, c, qb_)) for c in (b_in, b_out))

    def term(u, row, height, col, width):
        rows = pl.ds(pl.multiple_of(lax.rem(u, PER) * SUB + row, 16), height)
        return pp.at[lax.rem(lax.div(u, PER), 2), rows, pl.ds(pl.multiple_of(col, 128), width)]

    def final(u, col, width):
        return img.at[(lax.rem(u, IMAGES), *part(mine, ROWS, col, width))]

    def wide(ref):
        return ref[...].astype(f32)

    def put(ref, value):
        ref[...] = value.astype(bf16)

    ours, theirs = pl.ds(pl.multiple_of(y * ROWS, 16), ROWS), pl.ds(pl.multiple_of((1 - y) * ROWS, 16), ROWS)

    def a_s0(u, b, s, r):
        put(sa0.at[b], term(u, (1 - y) * ROWS, ROWS, 0, wa)[...])
        a0(u).start()

    def a_o1(u, b, s, r):
        a0(u).wait_recv()

        def part(col, width):
            return term(u, mine, ROWS, col, width)[...] + wide(ra0.at[s, :, pl.ds(pl.multiple_of(col, 128), width)])

        put(safar.at[b], part(a_far, 2 * qa))
        afar(u).start()
        put(sani.at[b], part(a_in, qa))
        ani(u).start()
        term(u, mine, ROWS, a_out, qa)[...] = part(a_out, qa)

    def a_i1(u, b, s, r):
        a0(u).wait_recv()
        own = term(u, mine, ROWS, 0, wa)
        own[...] = own[...] + wide(ra0.at[s])

    def a_i2(u, b, s, r):
        xa_i(u).start()
        afar(u).wait_recv()
        put(safar.at[b], term(u, mine, ROWS, a_far, 2 * qa)[...] + wide(rafar.at[s]))
        amid(u).start()

    def a_i3(u, b, s, r):
        amid(u).wait_recv()
        put(sani.at[b], term(u, mine, ROWS, a_out, qa)[...] + wide(ramid.at[s, :, a_o]))
        arno(u).start()
        ani(u).wait_recv()
        xa_i(u).wait()
        total = term(u, mine, ROWS, a_in, qa)[...] + wide(ramid.at[s, :, a_i]) + wide(rani.at[s])
        put(final(u, a_in, qa), wide(xa_res.at[r]) + total)
        afo(u).start()

    def a_ox(u, b, s, r):
        xa_o(u).start()

    def a_o4(u, b, s, r):
        arno(u).wait_recv()
        xa_o(u).wait()
        put(final(u, a_out, qa), wide(xa_res.at[r]) + (term(u, mine, ROWS, a_out, qa)[...] + wide(rani.at[s])))
        aof(u).start()

    def a_o5(u, b, s, r):
        afo(u).wait_recv()
        ayn(u).start()

    def a_i5(u, b, s, r):
        aof(u).wait_recv()
        agm(u).start()
        ayn(u).start()

    def a_i6(u, b, s, r):
        agm(u).wait_recv()
        afm(u).start()
        ayf(u).start()

    def a_o7(u, b, s, r):
        afm(u).wait_recv()
        ayf(u).start()

    def a_en(u, b, s, r):
        ayn(u).wait_recv()

    def a_ef(u, b, s, r):
        ayf(u).wait_recv()

    def b_o0(u, b, s, r):
        put(sbfar.at[b], term(u, 0, SUB, b_far, 2 * qb_)[...])
        bfar(u).start()
        put(sbni.at[b], term(u, 0, SUB, b_in, qb_)[...])
        bni(u).start()

    def b_i1(u, b, s, r):
        bfar(u).wait_recv()
        put(sbfar.at[b], term(u, 0, SUB, b_far, 2 * qb_)[...] + wide(rbfar.at[s]))
        bmid(u).start()

    def b_i2(u, b, s, r):
        xb_i(u).start()
        bmid(u).wait_recv()
        put(sbni.at[b], term(u, 0, SUB, b_out, qb_)[...] + wide(rbmid.at[s, :, b_o]))
        brno(u).start()
        bni(u).wait_recv()
        put(sbgy.at[b], term(u, (1 - y) * ROWS, ROWS, b_in, qb_)[...] + wide(rbmid.at[s, theirs, b_i]) + wide(rbni.at[s, theirs, :]))
        bgy(u).start()
        own = term(u, mine, ROWS, b_in, qb_)
        own[...] = own[...] + wide(rbmid.at[s, ours, b_i]) + wide(rbni.at[s, ours, :])

    def b_o3(u, b, s, r):
        xb_o(u).start()
        brno(u).wait_recv()
        put(sbgy.at[b], term(u, (1 - y) * ROWS, ROWS, b_out, qb_)[...] + wide(rbni.at[s, theirs, :]))
        bgy(u).start()
        own = term(u, mine, ROWS, b_out, qb_)
        own[...] = own[...] + wide(rbni.at[s, ours, :])

    def finish_b(u, b, s, r, col, res, send):
        bgy(u).wait_recv()
        res(u).wait()
        put(final(u, col, qb_), wide(xb_res.at[r]) + (term(u, mine, ROWS, col, qb_)[...] + wide(rbgy.at[s])))
        send(u).start()

    def b_i3(u, b, s, r):
        finish_b(u, b, s, r, b_in, xb_i, bfy_i)

    def b_o4(u, b, s, r):
        finish_b(u, b, s, r, b_out, xb_o, bfy_o)

    def b_i4(u, b, s, r):
        bfy_i(u).wait_recv()
        bfo(u).start()

    def b_o5(u, b, s, r):
        bfy_o(u).wait_recv()
        bof(u).start()

    def b_i6(u, b, s, r):
        bof(u).wait_recv()
        bgm(u).start()

    def b_i7(u, b, s, r):
        bgm(u).wait_recv()
        bfm(u).start()

    def b_en(u, b, s, r):
        bfo(u).wait_recv()

    def b_ef(u, b, s, r):
        bfm(u).wait_recv()

    def d_s(u, b, s, r):
        share(u).start()
        keep(u).start()

    def d_w(u, b, s, r):
        share(u).wait_recv()
        keep(u).wait()

    steps = {
        "a_s0": (a_s0, [a0]), "a_o1": (a_o1, [afar, ani]), "a_i1": (a_i1, []), "a_i2": (a_i2, [amid]), "a_i3": (a_i3, [arno, afo]),
        "a_ox": (a_ox, []), "a_o4": (a_o4, [aof]), "a_o5": (a_o5, [ayn]), "a_i5": (a_i5, [agm, ayn]), "a_i6": (a_i6, [afm, ayf]),
        "a_o7": (a_o7, [ayf]), "a_en": (a_en, []), "a_ef": (a_ef, []), "b_o0": (b_o0, [bfar, bni]), "b_i1": (b_i1, [bmid]),
        "b_i2": (b_i2, [brno, bgy]), "b_o3": (b_o3, [bgy]), "b_i3": (b_i3, [bfy_i]), "b_o4": (b_o4, [bfy_o]), "b_i4": (b_i4, [bfo]),
        "b_o5": (b_o5, [bof]), "b_i6": (b_i6, [bgm]), "b_i7": (b_i7, [bfm]), "b_en": (b_en, []), "b_ef": (b_ef, []),
        "d_s": (d_s, [share]), "d_w": (d_w, []),
    }

    def role(name):
        return {"i": inner, "o": outer}.get(name[2]) if name not in ("b_en", "b_ef") else outer

    def exchange(t):
        n = 0
        for name, after in STEPS:
            if name[0] == "H":
                compute(t, n)
                n += 1
                continue
            do, sends = steps[name]
            u = t - PER - after
            go = (u >= 0) & (u < nsub)
            if role(name) is not None:
                go = go & role(name)

            @pl.when(go)
            def _():
                if sends:
                    @pl.when(u >= SENDS)
                    def _():
                        for m in sends:
                            m(u - SENDS).wait_send()
                do(u, lax.rem(u, SENDS), lax.rem(u, SLOTS), lax.rem(u, 4))

    def drain():
        for name in steps:
            def leave(sends=steps[name][1]):
                for m in sends:
                    for u in range(max(nsub - SENDS, 0), nsub):
                        m(u).wait_send()
            if role(name) is None:
                leave()
            elif steps[name][1]:
                pl.when(role(name))(leave)

    lanes = 1024

    def norm():
        def rows(i, _):
            r = pl.ds(pl.multiple_of(i * 16, 16), 16)
            acc = jnp.zeros((16, lanes), f32)
            for j in range(0, d, lanes):
                v = xb[r, j : j + lanes].astype(f32)
                acc = acc + v * v
            scale = lax.rsqrt(jnp.sum(acc, axis=-1, keepdims=True) * (1.0 / d) + 1e-6)
            for j in range(0, d, lanes):
                v = xb[r, j : j + lanes].astype(f32)
                xb[r, j : j + lanes] = (v * scale * gain[pl.ds(j, lanes)].astype(f32)[None]).astype(bf16)

        lax.fori_loop(0, CHUNK // 16, rows, None)

    def project(c, i):
        g, kind, j = c * 3 * nt + i, lax.div(i, nt), lax.rem(i, nt)
        acc = None
        for part in range(2):
            w_wait(2 * g + part)
            one = jnp.dot(xb[:, part * k2 : (part + 1) * k2], wb[lax.rem(2 * g + part, HELD)], preferred_element_type=f32)
            acc = one if acc is None else acc + one
            w_start(2 * g + part + HELD)
        r = acc.astype(bf16)
        tokens = pl.ds(pl.multiple_of(c * CHUNK, CHUNK), CHUNK)
        for n in range(TILE // HEAD):
            h = j * (TILE // HEAD) + n
            one = r[:, n * HEAD : (n + 1) * HEAD]

            @pl.when(kind < 2)
            def _():
                w = one.astype(f32)
                w = (w * cs[...] + pltpu.roll(w, HEAD // 2, 1) * sn[...]).astype(bf16)

                @pl.when(kind == 0)
                def _():
                    qb[h] = w

                @pl.when(kind == 1)
                def _():
                    kc[h, tokens, :] = w

            @pl.when(kind == 2)
            def _():
                vt[h, pl.ds(0, HEAD), tokens] = one.T

    e = HEAD**-0.5 * LOG2E

    def attention(c):
        top[...] = jnp.full(top.shape, NEG, f32)
        mix[...] = jnp.zeros(mix.shape, f32)

        def block(j, masked):
            here = pl.ds(pl.multiple_of(j * CHUNK, CHUNK), CHUNK)
            scores = [_dot(kc[h, here, :], qb[h], 1, 1) for h in range(hl)]
            if masked:
                ok = lax.broadcasted_iota(jnp.int32, (CHUNK, CHUNK), 1) >= lax.broadcasted_iota(jnp.int32, (CHUNK, CHUNK), 0)
            weights, keeps = [], []
            for h, s in enumerate(scores):
                if masked:
                    s = jnp.where(ok, s, 2 * NEG)
                old = top[h : h + 1, :]
                new = jnp.maximum(old, s.max(axis=0, keepdims=True))
                top[h : h + 1, :] = new
                weights.append(jnp.exp2((s - new) * e).astype(bf16))
                keeps.append(jnp.exp2((old - new) * e))
            for h in range(hl):
                mix[h] = mix[h] * keeps[h] + _dot(vt[h, :, here], weights[h], 1, 0)

        lax.fori_loop(0, c, lambda j, _: block(j, False), None)
        block(c, True)
        b = lax.rem(c, 2)
        for h in range(hl):
            total = mix[h, HEAD : HEAD + 1, :]
            seen[b, :, h * HEAD : (h + 1) * HEAD] = (mix[h, :HEAD, :] * (1 / total)).T.astype(bf16)

    def output(c, quarter):
        b, tiles = lax.rem(c, 2), half // WO_TILE

        def tile(n, _):
            for copy in o_copies(n):
                copy.wait()
            pp[b, :, pl.ds(pl.multiple_of(n * WO_TILE, WO_TILE), WO_TILE)] = jnp.dot(seen[b], ob[lax.rem(n, WO_HELD)], preferred_element_type=f32)

            @pl.when(n + WO_HELD < tiles)
            def _():
                for copy in o_copies(n + WO_HELD):
                    copy.start()

        lax.fori_loop(quarter * (tiles // 4), (quarter + 1) * (tiles // 4), tile, None)

    def compute(t, n):
        each = PARTS // PER
        c, p = lax.div(t, PER), lax.rem(t, PER) * each + n
        here = set(range(n, PARTS, each))

        def branch(parts, on, do):
            if here & set(parts):
                pl.when((t < nsub) & on)(do)

        def first():
            x_copy(c).wait()
            for copy in cs_copies(c):
                copy.wait()
            norm()

        def middle_():
            @pl.when(c + 1 < nch)
            def _():
                x_copy(c + 1).start()
                for copy in cs_copies(c + 1):
                    copy.start()

            @pl.when(c == 0)
            def _():
                ext_copy().wait_recv()

            for i in range(WO_HELD):
                for copy in o_copies(i):
                    copy.start()

            @pl.when(c >= 2)
            def _():
                seen_copy(c - 2).wait_send()
            attention(c)
            seen_copy(c).start()

        branch([0], p == 0, first)
        branch(range(1, 10), (p >= 1) & (p <= 3 * nt), lambda: project(c, p - 1))
        branch([10], p == 10, middle_)
        branch([12], p == 12, lambda: seen_copy(c).wait_recv())
        branch(range(12, 16), p >= 12, lambda: output(c, p - 12))

    x_copy(0).start()
    for copy in cs_copies(0):
        copy.start()
    for n in range(HELD):
        w_start(n)
    for h in range(hl):
        vt[h, HEAD:, :] = jnp.ones((8, vt.shape[2]), bf16)

    @pl.when(inner)
    def _():
        pl.semaphore_wait(barrier, 4)

    @pl.when(outer)
    def _():
        pl.semaphore_wait(barrier, 3)

    ext_copy().start()


    def tick(t, _):
        exchange(t)

    lax.fori_loop(0, PER + nsub + max(AFTER.values()), tick, None)
    drain()
    for c in range(max(nch - 2, 0), nch):
        seen_copy(c).wait_send()
    ext_copy().wait_send()


def layer(x, gain, wq, wk, wv, wo, cos, sin):
    rows, d = x.shape
    hl = wq.shape[1] // HEAD
    half, qa = d // 2, d // 4
    nch = rows // CHUNK
    v, dma = pltpu.VMEM, pltpu.SemaphoreType.DMA
    hbm = pl.BlockSpec(memory_space=pl.ANY)
    wa = _split(half)
    qa, qb = wa // 4, (half - wa) // 4

    def buffers(n, *shapes):
        return [v((n, *s), bf16) for s in shapes]

    scratch = [
        v((CHUNK, d), bf16), v((HELD, d // 2, TILE), bf16), v((WO_HELD, 2 * hl * HEAD, WO_TILE), bf16), v((hl, rows, HEAD), bf16),
        v((hl, HEAD + 8, rows), bf16), v((hl, CHUNK, HEAD), bf16), v((2, CHUNK, 2 * hl * HEAD), bf16), v((2, CHUNK, half), f32),
        v((hl, HEAD + 8, CHUNK), f32), v((hl, CHUNK), f32), v((CHUNK, HEAD), f32), v((CHUNK, HEAD), f32),
        *buffers(4, (ROWS, qa), (ROWS, qb)),
        *buffers(SLOTS, (ROWS, wa), (ROWS, 2 * qa), (ROWS, qa), (ROWS, 2 * qa), (SUB, 2 * qb), (SUB, qb), (SUB, 2 * qb), (ROWS, qb)),
        *buffers(SENDS, (ROWS, wa), (ROWS, 2 * qa), (ROWS, qa), (SUB, 2 * qb), (SUB, qb), (ROWS, qb)),
        v((IMAGES, SUB, half), bf16),
        dma, dma((HELD,)), dma((WO_HELD, 2)), dma((2,)), dma((2, 4)), dma((SENDS,)), dma((RS_KINDS + AG_KINDS, SENDS)), dma((RS_KINDS, SLOTS)),
        dma((AG_KINDS, MARKS)), dma((2, 2)), dma((2,)),
    ]
    out, _ = pl.pallas_call(
        functools.partial(_kernel, d=d, hl=hl, nch=nch),
        name="layer",
        in_specs=[hbm, pl.BlockSpec(memory_space=pltpu.VMEM), hbm, hbm, hbm, hbm, hbm, hbm],
        out_specs=[hbm, hbm],
        out_shape=[jax.ShapeDtypeStruct((rows, d), bf16), jax.ShapeDtypeStruct((hl * HEAD, half), bf16)],
        scratch_shapes=scratch,
        compiler_params=pltpu.CompilerParams(collective_id=0, has_side_effects=True, vmem_limit_bytes=63 * 2**20),
    )(x, gain, wq, wk, wv, wo, cos, sin)
    return handed(out)


def _hand(a, out, held, s_in, s_out):
    n, rows = held.shape[:2]
    total = a.shape[0] // rows

    def come(i):
        return pltpu.make_async_copy(a.at[pl.ds(i * rows, rows), :], held.at[i % n], s_in.at[i % n])

    def go(i):
        return pltpu.make_async_copy(held.at[i % n], out.at[pl.ds(i * rows, rows), :], s_out.at[i % n])

    for i in range(min(n // 2, total)):
        come(i).start()
    for i in range(total):
        come(i).wait()
        go(i).start()
        j = i + n // 2
        if j < total:
            if j >= n:
                go(j - n).wait()
            come(j).start()
    for i in range(max(total - n, 0), total):
        go(i).wait()


def handed(a):
    rows, n = 64, 24
    return pl.pallas_call(
        _hand,
        name="hand",
        in_specs=[pl.BlockSpec(memory_space=pl.ANY)],
        out_specs=pl.BlockSpec(memory_space=pl.ANY),
        out_shape=jax.ShapeDtypeStruct(a.shape, a.dtype),
        scratch_shapes=[pltpu.VMEM((n, rows, a.shape[1]), a.dtype), pltpu.SemaphoreType.DMA((n,)), pltpu.SemaphoreType.DMA((n,))],
        compiler_params=pltpu.CompilerParams(vmem_limit_bytes=60 * 2**20),
    )(a)


def solution(mesh):
    def step(x, gain, wq, wk, wv, wo):
        half = HEAD // 2
        angle = np.arange(x.shape[0], dtype=np.float32)[:, None] * np.float32(THETA) ** (-np.arange(half, dtype=np.float32) / half)
        cos, sin = np.cos(angle), np.sin(angle)
        cos, sin = (jnp.asarray(np.concatenate(t, -1), f32) for t in ([cos, cos], [-sin, sin]))
        return layer(x, gain, wq, wk, wv, wo, cos, sin)

    tokens, columns = P("dp", None), P(None, "tp")
    return jax.shard_map(
        step,
        mesh=mesh,
        in_specs=(tokens, P(None), columns, columns, columns, P("tp", None)),
        out_specs=tokens,
        check_vma=False,
    )
```

```python
import functools

import jax
import jax.numpy as jnp
import numpy as np
from jax import lax
from jax.experimental import pallas as pl
from jax.experimental.pallas import tpu as pltpu
from jax.sharding import PartitionSpec as P

HEAD = 128
LAYER_VMEM, HAND_VMEM = 362 * 2**20 // 10, 6 * 2**20
THETA = 10000
LOG2E = 1.4426950408889634
NEG = -1e30
CHUNK = 256
SUB = 32
PER = CHUNK // SUB
ROWS = SUB // 2
PARTS = 16
TILE = 256
HELD = 5
HOLD_TICKS = 10
WO_TILE = 512
WO_HELD = 3
SLOTS = 6
IMAGES = 14
MARKS = 16
SENDS = 3
RS_KINDS, AG_KINDS = 10, 12
A_SHARE = 7 / 12
f32, bf16 = jnp.float32, jnp.bfloat16

STEPS = (
    ("a_en", 8), ("d_w", 13), ("b_i1", 1), ("b_o5", 6), ("b_i4", 4), ("b_ef", 11), ("b_i3", 3), ("a_o5", 5), ("a_ef", 11),
    ("b_i2", 2), ("a_i3", 3), ("a_i2", 2), ("b_o0", 0), ("a_s0", 0), ("a_o7", 8), ("a_ox", 2), ("a_o1", 1), ("a_i5", 5),
    ("H1", 0), ("a_i6", 6), ("a_o4", 4), ("b_o4", 4), ("b_i6", 6), ("b_o3", 3), ("a_i1", 1), ("b_i7", 7), ("d_s", 11),
    ("b_en", 8), ("H2", 0),
)
AFTER = dict(STEPS)


def _dot(a, b, ca, cb):
    return lax.dot_general(a, b, (((ca,), (cb,)), ((), ())), preferred_element_type=f32)


def _split(half):
    return min(max(round(half * A_SHARE / 512), 1), half // 512 - 1) * 512


def _kernel(x, gain, wq, wk, wv, wo, cos, sin, out, wo_ext, wb, xb, img, ob, kc, vt, qb, seen, pp, mix, acc, top, cs, sn, xa_res, xb_res,
            ra0, rafar, rani, ramid, rbfar, rbni, rbmid, rbgy, sa0, safar, sani, sbfar, sbni, sbgy,
            s_x, s_w, s_o, s_cs, s_res, s_local, s_send, s_rs, s_ag, s_seen, s_ext, s_hold, *, d, hl, nch):
    half = d // 2
    wa = _split(half)
    qa, qb_ = wa // 4, (half - wa) // 4
    nt = hl * HEAD // TILE
    nsub = nch * PER
    pos = lax.axis_index("tp")
    y, z, core = lax.div(pos, 8), lax.rem(lax.div(pos, 2), 4), lax.rem(pos, 2)
    side = lax.div(z, 2)
    inner = (z == 1) | (z == 2)
    outer = (z == 0) | (z == 3)

    def at(y, z, core):
        return (y * 4 + z) * 2 + core

    partner = at(y, z, 1 - core)
    across = at(1 - y, z, core)
    middle = at(y, 3 - z, core)
    beside = at(y, 1 - z + 4 * side, core)
    col0 = core * half

    barrier = pltpu.get_barrier_semaphore()
    for dev in (partner, across, beside):
        pl.semaphore_signal(barrier, inc=1, device_id={"tp": dev})

    @pl.when(inner)
    def _():
        pl.semaphore_signal(barrier, inc=1, device_id={"tp": middle})

    def x_copy(c):
        return pltpu.make_async_copy(x.at[pl.ds(c * CHUNK, CHUNK), :], xb, s_x)

    def cs_copies(c):
        rows = pl.ds(c * CHUNK, CHUNK)
        return pltpu.make_async_copy(cos.at[rows, :], cs, s_cs.at[0]), pltpu.make_async_copy(sin.at[rows, :], sn, s_cs.at[1])

    k2, cuts = d // 2, 2

    def w_start(h):
        i, part, slot = lax.rem(lax.div(h, 2), 3 * nt), lax.rem(h, 2), lax.rem(h, HELD)
        kind, tile = lax.div(i, nt), lax.rem(i, nt)
        for n, w in enumerate((wq, wk, wv)):
            @pl.when((kind == n) & (h < nch * 3 * nt * 2))
            def _():
                for a in range(cuts):
                    rows = pl.ds(pl.multiple_of(part * k2 + a * (k2 // cuts), k2 // cuts), k2 // cuts)
                    pltpu.make_async_copy(w.at[rows, pl.ds(pl.multiple_of(tile * TILE, TILE), TILE)],
                                          wb.at[slot, pl.ds(a * (k2 // cuts), k2 // cuts), :], s_w.at[slot]).start()

    def w_wait(h):
        slot = lax.rem(h, HELD)
        pltpu.make_async_copy(wq.at[pl.ds(0, k2), pl.ds(0, TILE)], wb.at[slot], s_w.at[slot]).wait()

    def o_copies(n):
        slot, k = lax.rem(n, WO_HELD), hl * HEAD
        mine = pl.ds(pl.multiple_of(col0 + n * WO_TILE, WO_TILE), WO_TILE)
        theirs = pl.ds(pl.multiple_of(n * WO_TILE, WO_TILE), WO_TILE)
        return (pltpu.make_async_copy(wo.at[:, mine], ob.at[slot, pl.ds(0, k), :], s_o.at[slot, 0]),
                pltpu.make_async_copy(wo_ext.at[:, theirs], ob.at[slot, pl.ds(k, k), :], s_o.at[slot, 1]))

    def ext_copy():
        return pltpu.make_async_remote_copy(wo.at[:, pl.ds(pl.multiple_of((1 - core) * half, half), half)], wo_ext, s_ext.at[0], s_ext.at[1],
                                            device_id={"tp": partner})

    def seen_copy(c):
        k, b = hl * HEAD, lax.rem(c, 2)
        return pltpu.make_async_remote_copy(seen.at[b, :, pl.ds(0, k)], seen.at[b, :, pl.ds(k, k)], s_seen.at[0, b], s_seen.at[1, b],
                                            device_id={"tp": partner})

    kinds = {}

    def number(table, name):
        return kinds.setdefault((table, name), sum(t == table for t, _ in kinds))

    def rs(name, src, dst, dev):
        n = number("rs", name)

        def make(u):
            b = lax.rem(u, SENDS)
            return pltpu.make_async_remote_copy(src.at[b], dst.at[lax.rem(u, SLOTS)], s_send.at[n, b], s_rs.at[n, lax.rem(u, SLOTS)],
                                                device_id={"tp": dev})
        return make

    def place(row, height, col, width):
        return lambda u: (pl.ds(pl.multiple_of(u * SUB + row, 16), height), pl.ds(pl.multiple_of(col0 + col, 128), width))

    def ag(name, where, dev):
        n = number("ag", name)

        def make(u):
            there = img.at[(lax.rem(u, IMAGES), *where)]
            return pltpu.make_async_remote_copy(there, there, s_send.at[RS_KINDS + n, lax.rem(u, SENDS)], s_ag.at[n, lax.rem(u, MARKS)],
                                                device_id={"tp": dev})
        return make

    def part(row, height, col, width):
        return pl.ds(pl.multiple_of(row, 16), height), pl.ds(pl.multiple_of(col, 128), width)

    def rows_of(u):
        return out.at[pl.ds(pl.multiple_of(u * SUB, 16), SUB), pl.ds(pl.multiple_of(col0, 128), half)]

    def share(u):
        n = number("ag", "share")
        return pltpu.make_async_remote_copy(img.at[lax.rem(u, IMAGES)], rows_of(u), s_send.at[RS_KINDS + n, lax.rem(u, SENDS)],
                                            s_ag.at[n, lax.rem(u, MARKS)], device_id={"tp": partner})

    def keep(u):
        return pltpu.make_async_copy(img.at[lax.rem(u, IMAGES)], rows_of(u), s_local.at[lax.rem(u, SENDS)])

    def residual(n, dst, where):
        def make(u):
            b = lax.rem(u, 4)
            return pltpu.make_async_copy(x.at[where(u)], dst.at[b], s_res.at[n, b])
        return make

    mine = y * ROWS
    a_near, a_far = side * 2 * qa, (1 - side) * 2 * qa
    b_near, b_far = wa + side * 2 * qb_, wa + (1 - side) * 2 * qb_
    a_in, a_out = a_near + (1 - side) * qa, a_near + side * qa
    b_in, b_out = b_near + (1 - side) * qb_, b_near + side * qb_
    a_i, a_o, b_i, b_o = (pl.ds(pl.multiple_of(n * q, 128), q) for n, q in ((1 - side, qa), (side, qa), (1 - side, qb_), (side, qb_)))

    a0 = rs("a0", sa0, ra0, across)
    afar = rs("afar", safar, rafar, beside)
    ani = rs("ani", sani, rani, beside)
    amid = rs("amid", safar, ramid, middle)
    arno = rs("arno", sani, rani, beside)
    bfar = rs("bfar", sbfar, rbfar, beside)
    bni = rs("bni", sbni, rbni, beside)
    bmid = rs("bmid", sbfar, rbmid, middle)
    brno = rs("brno", sbni, rbni, beside)
    bgy = rs("bgy", sbgy, rbgy, across)

    afo = ag("afo", part(mine, ROWS, a_in, qa), beside)
    aof = ag("aof", part(mine, ROWS, a_out, qa), beside)
    ayn = ag("ayn", part(mine, ROWS, a_near, 2 * qa), across)
    ayf = ag("ayf", part(mine, ROWS, a_far, 2 * qa), across)
    agm = ag("agm", part(mine, ROWS, a_near, 2 * qa), middle)
    afm = ag("afm", part(mine, ROWS, a_far, 2 * qa), beside)
    bfy_i = ag("bfy", part(mine, ROWS, b_in, qb_), across)
    bfy_o = ag("bfy", part(mine, ROWS, b_out, qb_), across)
    bfo = ag("bfo", part(0, SUB, b_in, qb_), beside)
    bof = ag("bof", part(0, SUB, b_out, qb_), beside)
    bgm = ag("bgm", part(0, SUB, b_near, 2 * qb_), middle)
    bfm = ag("bfm", part(0, SUB, b_far, 2 * qb_), beside)
    xa_i, xa_o = (residual(0, xa_res, place(mine, ROWS, c, qa)) for c in (a_in, a_out))
    xb_i, xb_o = (residual(1, xb_res, place(mine, ROWS, c, qb_)) for c in (b_in, b_out))

    def term(u, row, height, col, width):
        rows = pl.ds(pl.multiple_of(lax.rem(u, PER) * SUB + row, 16), height)
        return pp.at[lax.rem(lax.div(u, PER), 2), rows, pl.ds(pl.multiple_of(col, 128), width)]

    def final(u, col, width):
        return img.at[(lax.rem(u, IMAGES), *part(mine, ROWS, col, width))]

    def wide(ref):
        return ref[...].astype(f32)

    def put(ref, value):
        ref[...] = value.astype(bf16)

    ours, theirs = pl.ds(pl.multiple_of(y * ROWS, 16), ROWS), pl.ds(pl.multiple_of((1 - y) * ROWS, 16), ROWS)

    def a_s0(u, b, s, r):
        put(sa0.at[b], term(u, (1 - y) * ROWS, ROWS, 0, wa)[...])
        a0(u).start()

    def a_o1(u, b, s, r):
        a0(u).wait_recv()

        def part(col, width):
            return term(u, mine, ROWS, col, width)[...] + wide(ra0.at[s, :, pl.ds(pl.multiple_of(col, 128), width)])

        put(safar.at[b], part(a_far, 2 * qa))
        afar(u).start()
        put(sani.at[b], part(a_in, qa))
        ani(u).start()
        term(u, mine, ROWS, a_out, qa)[...] = part(a_out, qa)

    def a_i1(u, b, s, r):
        a0(u).wait_recv()
        own = term(u, mine, ROWS, 0, wa)
        own[...] = own[...] + wide(ra0.at[s])

    def a_i2(u, b, s, r):
        xa_i(u).start()
        afar(u).wait_recv()
        put(safar.at[b], term(u, mine, ROWS, a_far, 2 * qa)[...] + wide(rafar.at[s]))
        amid(u).start()

    def a_i3(u, b, s, r):
        amid(u).wait_recv()
        put(sani.at[b], term(u, mine, ROWS, a_out, qa)[...] + wide(ramid.at[s, :, a_o]))
        arno(u).start()
        ani(u).wait_recv()
        xa_i(u).wait()
        total = term(u, mine, ROWS, a_in, qa)[...] + wide(ramid.at[s, :, a_i]) + wide(rani.at[s])
        put(final(u, a_in, qa), wide(xa_res.at[r]) + total)
        afo(u).start()

    def a_ox(u, b, s, r):
        xa_o(u).start()

    def a_o4(u, b, s, r):
        arno(u).wait_recv()
        xa_o(u).wait()
        put(final(u, a_out, qa), wide(xa_res.at[r]) + (term(u, mine, ROWS, a_out, qa)[...] + wide(rani.at[s])))
        aof(u).start()

    def a_o5(u, b, s, r):
        afo(u).wait_recv()
        ayn(u).start()

    def a_i5(u, b, s, r):
        aof(u).wait_recv()
        agm(u).start()
        ayn(u).start()

    def a_i6(u, b, s, r):
        agm(u).wait_recv()
        afm(u).start()
        ayf(u).start()

    def a_o7(u, b, s, r):
        afm(u).wait_recv()
        ayf(u).start()

    def a_en(u, b, s, r):
        ayn(u).wait_recv()

    def a_ef(u, b, s, r):
        ayf(u).wait_recv()

    def b_o0(u, b, s, r):
        put(sbfar.at[b], term(u, 0, SUB, b_far, 2 * qb_)[...])
        bfar(u).start()
        put(sbni.at[b], term(u, 0, SUB, b_in, qb_)[...])
        bni(u).start()

    def b_i1(u, b, s, r):
        bfar(u).wait_recv()
        put(sbfar.at[b], term(u, 0, SUB, b_far, 2 * qb_)[...] + wide(rbfar.at[s]))
        bmid(u).start()

    def b_i2(u, b, s, r):
        xb_i(u).start()
        bmid(u).wait_recv()
        put(sbni.at[b], term(u, 0, SUB, b_out, qb_)[...] + wide(rbmid.at[s, :, b_o]))
        brno(u).start()
        bni(u).wait_recv()
        put(sbgy.at[b], term(u, (1 - y) * ROWS, ROWS, b_in, qb_)[...] + wide(rbmid.at[s, theirs, b_i]) + wide(rbni.at[s, theirs, :]))
        bgy(u).start()
        own = term(u, mine, ROWS, b_in, qb_)
        own[...] = own[...] + wide(rbmid.at[s, ours, b_i]) + wide(rbni.at[s, ours, :])

    def b_o3(u, b, s, r):
        xb_o(u).start()
        brno(u).wait_recv()
        put(sbgy.at[b], term(u, (1 - y) * ROWS, ROWS, b_out, qb_)[...] + wide(rbni.at[s, theirs, :]))
        bgy(u).start()
        own = term(u, mine, ROWS, b_out, qb_)
        own[...] = own[...] + wide(rbni.at[s, ours, :])

    def finish_b(u, b, s, r, col, res, send):
        bgy(u).wait_recv()
        res(u).wait()
        put(final(u, col, qb_), wide(xb_res.at[r]) + (term(u, mine, ROWS, col, qb_)[...] + wide(rbgy.at[s])))
        send(u).start()

    def b_i3(u, b, s, r):
        finish_b(u, b, s, r, b_in, xb_i, bfy_i)

    def b_o4(u, b, s, r):
        finish_b(u, b, s, r, b_out, xb_o, bfy_o)

    def b_i4(u, b, s, r):
        bfy_i(u).wait_recv()
        bfo(u).start()

    def b_o5(u, b, s, r):
        bfy_o(u).wait_recv()
        bof(u).start()

    def b_i6(u, b, s, r):
        bof(u).wait_recv()
        bgm(u).start()

    def b_i7(u, b, s, r):
        bgm(u).wait_recv()
        bfm(u).start()

    def b_en(u, b, s, r):
        bfo(u).wait_recv()

    def b_ef(u, b, s, r):
        bfm(u).wait_recv()

    def d_s(u, b, s, r):
        share(u).start()

        @pl.when(u < nsub - IMAGES)
        def _():
            keep(u).start()

    def d_w(u, b, s, r):
        share(u).wait_recv()

        @pl.when(u < nsub - IMAGES)
        def _():
            keep(u).wait()

    steps = {
        "a_s0": (a_s0, [a0]), "a_o1": (a_o1, [afar, ani]), "a_i1": (a_i1, []), "a_i2": (a_i2, [amid]), "a_i3": (a_i3, [arno, afo]),
        "a_ox": (a_ox, []), "a_o4": (a_o4, [aof]), "a_o5": (a_o5, [ayn]), "a_i5": (a_i5, [agm, ayn]), "a_i6": (a_i6, [afm, ayf]),
        "a_o7": (a_o7, [ayf]), "a_en": (a_en, []), "a_ef": (a_ef, []), "b_o0": (b_o0, [bfar, bni]), "b_i1": (b_i1, [bmid]),
        "b_i2": (b_i2, [brno, bgy]), "b_o3": (b_o3, [bgy]), "b_i3": (b_i3, [bfy_i]), "b_o4": (b_o4, [bfy_o]), "b_i4": (b_i4, [bfo]),
        "b_o5": (b_o5, [bof]), "b_i6": (b_i6, [bgm]), "b_i7": (b_i7, [bfm]), "b_en": (b_en, []), "b_ef": (b_ef, []),
        "d_s": (d_s, [share]), "d_w": (d_w, []),
    }

    def role(name):
        return {"i": inner, "o": outer}.get(name[2]) if name not in ("b_en", "b_ef") else outer

    def exchange(t):
        n = 0
        for name, after in STEPS:
            if name[0] == "H":
                compute(t, n)
                n += 1
                continue
            do, sends = steps[name]
            u = t - PER - after
            go = (u >= 0) & (u < nsub)
            if role(name) is not None:
                go = go & role(name)

            @pl.when(go)
            def _():
                if sends:
                    @pl.when(u >= SENDS)
                    def _():
                        for m in sends:
                            m(u - SENDS).wait_send()
                do(u, lax.rem(u, SENDS), lax.rem(u, SLOTS), lax.rem(u, 4))

    def drain():
        for name in steps:
            def leave(sends=steps[name][1]):
                for m in sends:
                    for u in range(max(nsub - SENDS, 0), nsub):
                        m(u).wait_send()
            if role(name) is None:
                leave()
            elif steps[name][1]:
                pl.when(role(name))(leave)

    lanes = 1024

    def norm():
        def rows(i, _):
            r = pl.ds(pl.multiple_of(i * 16, 16), 16)
            acc = jnp.zeros((16, lanes), f32)
            for j in range(0, d, lanes):
                v = xb[r, j : j + lanes].astype(f32)
                acc = acc + v * v
            scale = lax.rsqrt(jnp.sum(acc, axis=-1, keepdims=True) * (1.0 / d) + 1e-6)
            for j in range(0, d, lanes):
                v = xb[r, j : j + lanes].astype(f32)
                xb[r, j : j + lanes] = (v * scale * gain[pl.ds(j, lanes)].astype(f32)[None]).astype(bf16)

        lax.fori_loop(0, CHUNK // 16, rows, None)

    def project(c, i):
        g, kind, j = c * 3 * nt + i, lax.div(i, nt), lax.rem(i, nt)

        def part(p, _):
            w_wait(2 * g + p)
            columns = pl.ds(pl.multiple_of(p * k2, 128), k2)
            one = jnp.dot(xb[:, columns], wb[lax.rem(2 * g + p, HELD)], preferred_element_type=f32)
            w_start(2 * g + p + HELD)

            @pl.when(p == 0)
            def _():
                acc[...] = one

            @pl.when(p == 1)
            def _():
                acc[...] = acc[...] + one

        lax.fori_loop(0, 2, part, None)
        r = acc[...].astype(bf16)
        tokens = pl.ds(pl.multiple_of(c * CHUNK, CHUNK), CHUNK)
        for n in range(TILE // HEAD):
            h = j * (TILE // HEAD) + n
            one = r[:, n * HEAD : (n + 1) * HEAD]

            @pl.when(kind < 2)
            def _():
                w = one.astype(f32)
                w = (w * cs[...] + pltpu.roll(w, HEAD // 2, 1) * sn[...]).astype(bf16)

                @pl.when(kind == 0)
                def _():
                    qb[h] = w

                @pl.when(kind == 1)
                def _():
                    kc[h, tokens, :] = w

            @pl.when(kind == 2)
            def _():
                vt[h, pl.ds(0, HEAD), tokens] = one.T

    e = HEAD**-0.5 * LOG2E

    def attention(c):
        top[...] = jnp.full(top.shape, NEG, f32)
        mix[...] = jnp.zeros(mix.shape, f32)

        def block(j, masked):
            here = pl.ds(pl.multiple_of(j * CHUNK, CHUNK), CHUNK)
            scores = [_dot(kc[h, here, :], qb[h], 1, 1) for h in range(hl)]
            if masked:
                ok = lax.broadcasted_iota(jnp.int32, (CHUNK, CHUNK), 1) >= lax.broadcasted_iota(jnp.int32, (CHUNK, CHUNK), 0)
            weights, keeps = [], []
            for h, s in enumerate(scores):
                if masked:
                    s = jnp.where(ok, s, 2 * NEG)
                old = top[h : h + 1, :]
                new = jnp.maximum(old, s.max(axis=0, keepdims=True))
                top[h : h + 1, :] = new
                weights.append(jnp.exp2((s - new) * e).astype(bf16))
                keeps.append(jnp.exp2((old - new) * e))
            for h in range(hl):
                mix[h] = mix[h] * keeps[h] + _dot(vt[h, :, here], weights[h], 1, 0)

        lax.fori_loop(0, c, lambda j, _: block(j, False), None)
        block(c, True)
        b = lax.rem(c, 2)
        for h in range(hl):
            total = mix[h, HEAD : HEAD + 1, :]
            seen[b, :, h * HEAD : (h + 1) * HEAD] = (mix[h, :HEAD, :] * (1 / total)).T.astype(bf16)

    def output(c, quarter):
        b, tiles = lax.rem(c, 2), half // WO_TILE

        def tile(n, _):
            for copy in o_copies(n):
                copy.wait()
            pp[b, :, pl.ds(pl.multiple_of(n * WO_TILE, WO_TILE), WO_TILE)] = jnp.dot(seen[b], ob[lax.rem(n, WO_HELD)], preferred_element_type=f32)

            @pl.when(n + WO_HELD < tiles)
            def _():
                for copy in o_copies(n + WO_HELD):
                    copy.start()

        lax.fori_loop(quarter * (tiles // 4), (quarter + 1) * (tiles // 4), tile, None)

    def compute(t, n):
        each = PARTS // PER
        c, p = lax.div(t, PER), lax.rem(t, PER) * each + n
        here = set(range(n, PARTS, each))

        def branch(parts, on, do):
            if here & set(parts):
                pl.when((t < nsub) & on)(do)

        def first():
            x_copy(c).wait()
            for copy in cs_copies(c):
                copy.wait()
            norm()

        def middle_():
            @pl.when(c + 1 < nch)
            def _():
                x_copy(c + 1).start()
                for copy in cs_copies(c + 1):
                    copy.start()

            @pl.when(c == 0)
            def _():
                ext_copy().wait_recv()

            for i in range(WO_HELD):
                for copy in o_copies(i):
                    copy.start()

            @pl.when(c >= 2)
            def _():
                seen_copy(c - 2).wait_send()
            attention(c)
            seen_copy(c).start()

        branch([0], p == 0, first)
        branch(range(1, 10), (p >= 1) & (p <= 3 * nt), lambda: project(c, p - 1))
        branch([10], p == 10, middle_)
        branch([12], p == 12, lambda: seen_copy(c).wait_recv())
        branch(range(12, 16), p >= 12, lambda: output(c, p - 12))

    x_copy(0).start()
    for copy in cs_copies(0):
        copy.start()
    for n in range(HELD):
        w_start(n)
    for h in range(hl):
        vt[h, HEAD:, :] = jnp.ones((8, vt.shape[2]), bf16)

    @pl.when(inner)
    def _():
        pl.semaphore_wait(barrier, 4)

    @pl.when(outer)
    def _():
        pl.semaphore_wait(barrier, 3)

    ext_copy().start()


    held = _held(wb, xb, d)

    def tick(t, _):
        exchange(t)
        for i, (count, copies) in enumerate(held):
            share_of = -(-count // HOLD_TICKS)

            @pl.when((t >= nsub) & (t < nsub + HOLD_TICKS))
            def _():
                def one(j, _):
                    @pl.when(j < count)
                    def _():
                        there, here = copies(j)
                        pltpu.make_async_copy(out.at[there], here, s_hold.at[i]).start()

                lax.fori_loop((t - nsub) * share_of, (t - nsub + 1) * share_of, one, None)

    lax.fori_loop(0, PER + nsub + max(AFTER.values()), tick, None)
    drain()
    for i in range(wb.shape[0]):
        pltpu.make_async_copy(wq.at[pl.ds(0, k2), pl.ds(0, TILE)], wb.at[i], s_hold.at[0]).wait()
    pltpu.make_async_copy(x.at[pl.ds(0, CHUNK), :], xb, s_hold.at[1]).wait()
    for c in range(max(nch - 2, 0), nch):
        seen_copy(c).wait_send()
    ext_copy().wait_send()


def _held(wb, xb, d):
    kinds, row = [], 0

    def add(count, rows, width, where):
        nonlocal row
        across, start = d // width, row

        def piece(j):
            block, at = lax.div(j, across), lax.rem(j, across)
            there = pl.ds(pl.multiple_of(start + block * rows, 16), rows), pl.ds(pl.multiple_of(at * width, 128), width)
            return there, where(block, at)

        kinds.append((count * across, piece))
        row += count * rows

    h = wb.shape[1] * TILE // d
    add(wb.shape[0], h, TILE, lambda block, at: wb.at[block, pl.ds(pl.multiple_of(at * h, 16), h), :])
    add(xb.shape[0] // 64, 64, d, lambda block, at: xb.at[pl.ds(pl.multiple_of(block * 64, 16), 64), :])
    return kinds


def _held_rows(d):
    return HELD * (d // 2 * TILE // d) + CHUNK


def layer(x, gain, wq, wk, wv, wo, cos, sin):
    rows, d = x.shape
    hl = wq.shape[1] // HEAD
    half, qa = d // 2, d // 4
    nch = rows // CHUNK
    v, dma = pltpu.VMEM, pltpu.SemaphoreType.DMA
    hbm = pl.BlockSpec(memory_space=pl.ANY)
    wa = _split(half)
    qa, qb = wa // 4, (half - wa) // 4

    def buffers(n, *shapes):
        return [v((n, *s), bf16) for s in shapes]

    scratch = [
        v((WO_HELD, 2 * hl * HEAD, WO_TILE), bf16), v((hl, rows, HEAD), bf16), v((hl, HEAD + 8, rows), bf16), v((hl, CHUNK, HEAD), bf16), v((2, CHUNK, 2 * hl * HEAD), bf16), v((2, CHUNK, half), f32),
        v((hl, HEAD + 8, CHUNK), f32), v((CHUNK, TILE), f32), v((hl, CHUNK), f32), v((CHUNK, HEAD), f32), v((CHUNK, HEAD), f32),
        *buffers(4, (ROWS, qa), (ROWS, qb)),
        *buffers(SLOTS, (ROWS, wa), (ROWS, 2 * qa), (ROWS, qa), (ROWS, 2 * qa), (SUB, 2 * qb), (SUB, qb), (SUB, 2 * qb), (ROWS, qb)),
        *buffers(SENDS, (ROWS, wa), (ROWS, 2 * qa), (ROWS, qa), (SUB, 2 * qb), (SUB, qb), (ROWS, qb)),
        dma, dma((HELD,)), dma((WO_HELD, 2)), dma((2,)), dma((2, 4)), dma((SENDS,)), dma((RS_KINDS + AG_KINDS, SENDS)), dma((RS_KINDS, SLOTS)),
        dma((AG_KINDS, MARKS)), dma((2, 2)), dma((2,)), dma((2,)),
    ]
    kept = [v((HELD, d // 2, TILE), bf16), v((CHUNK, d), bf16), v((IMAGES, SUB, half), bf16)]
    out, _, *held = pl.pallas_call(
        functools.partial(_kernel, d=d, hl=hl, nch=nch),
        name="layer",
        in_specs=[hbm, pl.BlockSpec(memory_space=pltpu.VMEM), hbm, hbm, hbm, hbm, hbm, hbm],
        out_specs=[hbm, hbm] + [pl.BlockSpec(memory_space=pltpu.VMEM)] * len(kept),
        out_shape=[jax.ShapeDtypeStruct((rows, d), bf16), jax.ShapeDtypeStruct((hl * HEAD, half), bf16), *kept],
        scratch_shapes=scratch,
        compiler_params=pltpu.CompilerParams(collective_id=0, has_side_effects=True, vmem_limit_bytes=LAYER_VMEM),
    )(x, gain, wq, wk, wv, wo, cos, sin)
    return handed(out, *held)


def _hand(a, wb, xb, img, out, ring, s_in, s_out, s_held, *, first, last):
    d = a.shape[1]
    half, nsub, (slots, rows) = d // 2, a.shape[0] // SUB, ring.shape[:2]
    core = lax.rem(lax.axis_index("tp"), 2)
    mine, other = (pl.ds(pl.multiple_of(n * half, 128), half) for n in (core, 1 - core))
    whole = (last - first) // rows
    total = whole + (a.shape[0] - last) // rows

    def ends(i):
        at = pl.ds(first + i * rows, rows)
        return (at, ring.at[i % slots]) if i < whole else ((at, other), ring.at[i % slots, :, pl.ds(0, half)])

    def come(i):
        there, here = ends(i)
        return pltpu.make_async_copy(a.at[there], here, s_in.at[i % slots])

    def go(i):
        there, here = ends(i)
        return pltpu.make_async_copy(here, out.at[there], s_out.at[i % slots])

    kinds = _held(wb, xb, d)
    kinds.append((IMAGES, lambda j: ((pl.ds(pl.multiple_of(last + j * SUB, 16), SUB), mine), img.at[lax.rem(nsub - IMAGES + j, IMAGES)])))

    def held(n, low, high, act):
        def one(j, _):
            there, here = kinds[n][1](j)
            act(pltpu.make_async_copy(here, out.at[there], s_held.at[n]))

        lax.fori_loop(low, high, one, None)

    ahead = slots // 2
    for i in range(min(ahead, total)):
        come(i).start()
    for i in range(total):
        for n, (count, _) in enumerate(kinds):
            held(n, count * i // total, count * (i + 1) // total, lambda copy: copy.start())
        come(i).wait()
        go(i).start()
        j = i + ahead
        if j < total:
            if j >= slots:
                go(j - slots).wait()
            come(j).start()
    for i in range(max(total - slots, 0), total):
        go(i).wait()
    for n, (count, _) in enumerate(kinds):
        held(n, 0, count, lambda copy: copy.wait())


def handed(a, wb, xb, img):
    d = a.shape[1]
    first, last = _held_rows(d), a.shape[0] - IMAGES * SUB
    slots, rows = 7, 32
    dma = pltpu.SemaphoreType.DMA
    any_, vmem = pl.BlockSpec(memory_space=pl.ANY), pl.BlockSpec(memory_space=pltpu.VMEM)
    return pl.pallas_call(
        functools.partial(_hand, first=first, last=last),
        name="hand",
        in_specs=[any_] + [vmem] * 3,
        out_specs=any_,
        out_shape=jax.ShapeDtypeStruct(a.shape, a.dtype),
        scratch_shapes=[pltpu.VMEM((slots, rows, d), bf16), dma((slots,)), dma((slots,)), dma((3,))],
        compiler_params=pltpu.CompilerParams(vmem_limit_bytes=HAND_VMEM),
    )(a, wb, xb, img)


def solution(mesh):
    def step(x, gain, wq, wk, wv, wo):
        half = HEAD // 2
        angle = np.arange(x.shape[0], dtype=np.float32)[:, None] * np.float32(THETA) ** (-np.arange(half, dtype=np.float32) / half)
        cos, sin = np.cos(angle), np.sin(angle)
        cos, sin = (jnp.asarray(np.concatenate(t, -1), f32) for t in ([cos, cos], [-sin, sin]))
        return layer(x, gain, wq, wk, wv, wo, cos, sin)

    tokens, columns = P("dp", None), P(None, "tp")
    return jax.shard_map(
        step,
        mesh=mesh,
        in_specs=(tokens, P(None), columns, columns, columns, P("tp", None)),
        out_specs=tokens,
        check_vma=False,
    )
```

```python
import functools

import jax
import jax.numpy as jnp
import numpy as np
from jax import lax
from jax.experimental import pallas as pl
from jax.experimental.pallas import tpu as pltpu
from jax.sharding import PartitionSpec as P

HEAD = 128
LAYER_VMEM, HAND_VMEM = 362 * 2**20 // 10, 6 * 2**20
THETA = 10000
LOG2E = 1.4426950408889634
NEG = -1e30
CHUNK = 256
SUB = 32
PER = CHUNK // SUB
ROWS = SUB // 2
PARTS = 16
TILE = 256
HELD = 5
HOLD_TICKS = 10
WO_TILE = 512
WO_HELD = 3
SLOTS = 6
IMAGES = 14
MARKS = 16
SENDS = 3
RS_KINDS, AG_KINDS = 10, 12
A_SHARE = 5 / 8
INNER = 0.46
f32, bf16 = jnp.float32, jnp.bfloat16

STEPS = (
    ("b_i1", 1), ("b_i4", 4), ("b_i3", 3), ("b_o5", 6), ("b_i2", 2), ("a_i2", 2), ("a_s0", 0), ("b_o0", 0), ("a_i3", 3),
    ("b_en", 9), ("H1", 0), ("a_ox", 4), ("b_ef", 12), ("a_en", 8), ("a_o1", 1), ("b_o3", 3), ("d_w", 14), ("b_o4", 4),
    ("a_ef", 12), ("d_s", 12), ("a_i5", 5), ("a_o5", 6), ("a_i6", 6), ("b_i6", 6), ("b_i7", 7), ("a_i1", 1), ("a_o7", 8),
    ("a_o4", 4), ("H2", 0),
)
AFTER = dict(STEPS)


def _dot(a, b, ca, cb):
    return lax.dot_general(a, b, (((ca,), (cb,)), ((), ())), preferred_element_type=f32)


def _split(half):
    def near(share, unit, all_):
        return min(max(round(all_ * share / unit), 1), all_ // unit - 1) * unit

    wa = near(A_SHARE, 256, half)
    na, nb = wa // 2, (half - wa) // 2
    ia, ib = near(INNER, 128, na), near(INNER, 128, nb)
    return wa, ia, na - ia, ib, nb - ib


def _kernel(x, gain, wq, wk, wv, wo, cos, sin, out, wo_ext, wb, xb, img, ob, kc, vt, qb, seen, pp, mix, acc, top, cs, sn, xa_res, xb_res,
            ra0, rafar, rani, ramid, rbfar, rbni, rbmid, rbgy, sa0, safar, sani, sbfar, sbni, sbgy,
            s_x, s_w, s_o, s_cs, s_res, s_local, s_send, s_rs, s_ag, s_seen, s_ext, s_hold, s_term, free, *, d, hl, nch):
    half = d // 2
    wa, ia, oa, ib, ob_ = _split(half)
    na, nb = ia + oa, ib + ob_
    nt = hl * HEAD // TILE
    nsub = nch * PER
    pos = lax.axis_index("tp")
    y, z, core = lax.div(pos, 8), lax.rem(lax.div(pos, 2), 4), lax.rem(pos, 2)
    side = lax.div(z, 2)
    inner = (z == 1) | (z == 2)
    outer = (z == 0) | (z == 3)

    def at(y, z, core):
        return (y * 4 + z) * 2 + core

    partner = at(y, z, 1 - core)
    across = at(1 - y, z, core)
    middle = at(y, 3 - z, core)
    beside = at(y, 1 - z + 4 * side, core)
    col0 = core * half

    barrier = pltpu.get_barrier_semaphore()
    for dev in (partner, across, beside):
        pl.semaphore_signal(barrier, inc=1, device_id={"tp": dev})

    @pl.when(inner)
    def _():
        pl.semaphore_signal(barrier, inc=1, device_id={"tp": middle})

    def x_copies(c):
        rows = pl.ds(pl.multiple_of(c * CHUNK, CHUNK), CHUNK)
        return [pltpu.make_async_copy(x.at[rows, cut], xb.at[:, cut], s_x.at[i]) for i, cut in enumerate((pl.ds(0, half), pl.ds(half, half)))]

    def cs_copies(c):
        rows = pl.ds(c * CHUNK, CHUNK)
        return pltpu.make_async_copy(cos.at[rows, :], cs, s_cs.at[0]), pltpu.make_async_copy(sin.at[rows, :], sn, s_cs.at[1])

    k2, cuts = d // 2, 2

    def held_part(slot):
        return wb.at[pl.ds(pl.multiple_of(slot * k2, k2), k2), :]

    def w_start(h):
        i, part, slot = lax.rem(lax.div(h, 2), 3 * nt), lax.rem(h, 2), lax.rem(h, HELD)
        kind, tile = lax.div(i, nt), lax.rem(i, nt)
        for n, w in enumerate((wq, wk, wv)):
            @pl.when((kind == n) & (h < nch * 3 * nt * 2))
            def _():
                for a in range(cuts):
                    rows = pl.ds(pl.multiple_of(part * k2 + a * (k2 // cuts), k2 // cuts), k2 // cuts)
                    there = pl.ds(pl.multiple_of(slot * k2 + a * (k2 // cuts), k2 // cuts), k2 // cuts)
                    pltpu.make_async_copy(w.at[rows, pl.ds(pl.multiple_of(tile * TILE, TILE), TILE)], wb.at[there, :], s_w.at[slot]).start()

    def w_wait(h):
        slot = lax.rem(h, HELD)
        pltpu.make_async_copy(wq.at[pl.ds(0, k2), pl.ds(0, TILE)], held_part(slot), s_w.at[slot]).wait()

    def o_starts(c, n):
        slot, k = lax.rem(n, WO_HELD), hl * HEAD
        own, far, ext = (pl.ds(pl.multiple_of(at + n * WO_TILE, WO_TILE), WO_TILE) for at in (col0, (1 - core) * half, 0))
        low, high = ob.at[slot, pl.ds(0, k), :], ob.at[slot, pl.ds(k, k), :]

        @pl.when(c == 0)
        def _():
            pltpu.make_async_copy(wo.at[:, far], low, s_o.at[slot, 0]).start()
            pltpu.make_async_copy(wo.at[:, own], high, s_o.at[slot, 1]).start()

        @pl.when(c > 0)
        def _():
            pltpu.make_async_copy(wo.at[:, own], low, s_o.at[slot, 0]).start()
            pltpu.make_async_copy(wo_ext.at[:, ext], high, s_o.at[slot, 1]).start()

    def o_wait(n):
        slot, k = lax.rem(n, WO_HELD), hl * HEAD
        for i in range(2):
            pltpu.make_async_copy(wo.at[:, pl.ds(0, WO_TILE)], ob.at[slot, pl.ds(i * k, k), :], s_o.at[slot, i]).wait()

    def term_copy(n):
        at = pl.multiple_of(n * WO_TILE, WO_TILE)
        return pltpu.make_async_remote_copy(xb.at[:, pl.ds(half + at, WO_TILE)], xb.at[:, pl.ds(at, WO_TILE)], s_term.at[0, n], s_term.at[1, n],
                                            device_id={"tp": partner})

    def ext_copy():
        return pltpu.make_async_remote_copy(wo.at[:, pl.ds(pl.multiple_of((1 - core) * half, half), half)], wo_ext, s_ext.at[0], s_ext.at[1],
                                            device_id={"tp": partner})

    def seen_copy(c):
        k, b = hl * HEAD, lax.rem(c, 2)
        return pltpu.make_async_remote_copy(seen.at[b, :, pl.ds(0, k)], seen.at[b, :, pl.ds(k, k)], s_seen.at[0, b], s_seen.at[1, b],
                                            device_id={"tp": partner})

    kinds = {}

    def number(table, name):
        return kinds.setdefault((table, name), sum(t == table for t, _ in kinds))

    def rs(name, src, dst, dev, width=None):
        n = number("rs", name)

        def make(u):
            b, cut = lax.rem(u, SENDS), (slice(None), pl.ds(0, width or src.shape[2]))
            return pltpu.make_async_remote_copy(src.at[(b, *cut)], dst.at[(lax.rem(u, SLOTS), *cut)], s_send.at[n, b], s_rs.at[n, lax.rem(u, SLOTS)],
                                                device_id={"tp": dev})
        return make

    def place(row, height, col, width):
        return lambda u: (pl.ds(pl.multiple_of(u * SUB + row, 16), height), pl.ds(pl.multiple_of(col0 + col, 128), width))

    def ag(name, where, dev):
        n = number("ag", name)

        def make(u):
            there = img.at[(lax.rem(u, IMAGES), *where)]
            return pltpu.make_async_remote_copy(there, there, s_send.at[RS_KINDS + n, lax.rem(u, SENDS)], s_ag.at[n, lax.rem(u, MARKS)],
                                                device_id={"tp": dev})
        return make

    def part(row, height, col, width):
        return pl.ds(pl.multiple_of(row, 16), height), pl.ds(pl.multiple_of(col, 128), width)

    def rows_of(u):
        return out.at[pl.ds(pl.multiple_of(u * SUB, 16), SUB), pl.ds(pl.multiple_of(col0, 128), half)]

    def share(u):
        n = number("ag", "share")
        return pltpu.make_async_remote_copy(img.at[lax.rem(u, IMAGES)], rows_of(u), s_send.at[RS_KINDS + n, lax.rem(u, SENDS)],
                                            s_ag.at[n, lax.rem(u, MARKS)], device_id={"tp": partner})

    def keep(u):
        return pltpu.make_async_copy(img.at[lax.rem(u, IMAGES)], rows_of(u), s_local.at[lax.rem(u, SENDS)])

    def residual(n, dst, where, width):
        def make(u):
            b = lax.rem(u, 4)
            return pltpu.make_async_copy(x.at[where(u)], dst.at[b, :, pl.ds(0, width)], s_res.at[n, b])
        return make

    mine = y * ROWS
    a_near, a_far = side * na, (1 - side) * na
    b_near, b_far = wa + side * nb, wa + (1 - side) * nb
    a_in, a_out = a_near + (1 - side) * oa, a_near + side * ia
    b_in, b_out = b_near + (1 - side) * ob_, b_near + side * ib
    a_i, a_o, b_i, b_o = (pl.ds(pl.multiple_of(n, 128), w)
                          for n, w in (((1 - side) * oa, ia), (side * ia, oa), ((1 - side) * ob_, ib), (side * ib, ob_)))

    a0 = rs("a0", sa0, ra0, across)
    afar = rs("afar", safar, rafar, beside)
    ani = rs("ani", sani, rani, beside, ia)
    amid = rs("amid", safar, ramid, middle)
    arno = rs("arno", sani, rani, beside, oa)
    bfar = rs("bfar", sbfar, rbfar, beside)
    bni = rs("bni", sbni, rbni, beside, ib)
    bmid = rs("bmid", sbfar, rbmid, middle)
    brno = rs("brno", sbni, rbni, beside, ob_)
    bgy_i = rs("bgy", sbgy, rbgy, across, ib)
    bgy_o = rs("bgy", sbgy, rbgy, across, ob_)

    afo = ag("afo", part(mine, ROWS, a_in, ia), beside)
    aof = ag("aof", part(mine, ROWS, a_out, oa), beside)
    ayn = ag("ayn", part(mine, ROWS, a_near, na), across)
    ayf = ag("ayf", part(mine, ROWS, a_far, na), across)
    agm = ag("agm", part(mine, ROWS, a_near, na), middle)
    afm = ag("afm", part(mine, ROWS, a_far, na), beside)
    bfy_i = ag("bfy", part(mine, ROWS, b_in, ib), across)
    bfy_o = ag("bfy", part(mine, ROWS, b_out, ob_), across)
    bfo = ag("bfo", part(0, SUB, b_in, ib), beside)
    bof = ag("bof", part(0, SUB, b_out, ob_), beside)
    bgm = ag("bgm", part(0, SUB, b_near, nb), middle)
    bfm = ag("bfm", part(0, SUB, b_far, nb), beside)
    xa_i, xa_o = (residual(0, xa_res, place(mine, ROWS, c, w), w) for c, w in ((a_in, ia), (a_out, oa)))
    xb_i, xb_o = (residual(1, xb_res, place(mine, ROWS, c, w), w) for c, w in ((b_in, ib), (b_out, ob_)))

    def term(u, row, height, col, width):
        rows = pl.ds(pl.multiple_of(lax.rem(u, PER) * SUB + row, 16), height)
        return pp.at[lax.rem(lax.div(u, PER), 2), rows, pl.ds(pl.multiple_of(col, 128), width)]

    def final(u, col, width):
        return img.at[(lax.rem(u, IMAGES), *part(mine, ROWS, col, width))]

    def wide(ref):
        return ref[...].astype(f32)

    def put(ref, value):
        ref[...] = value.astype(bf16)

    ours, theirs = pl.ds(pl.multiple_of(y * ROWS, 16), ROWS), pl.ds(pl.multiple_of((1 - y) * ROWS, 16), ROWS)

    def a_s0(u, b, s, r):
        put(sa0.at[b], term(u, (1 - y) * ROWS, ROWS, 0, wa)[...])
        a0(u).start()

    def a_o1(u, b, s, r):
        a0(u).wait_recv()

        def part(col, width):
            return term(u, mine, ROWS, col, width)[...] + wide(ra0.at[s, :, pl.ds(pl.multiple_of(col, 128), width)])

        put(safar.at[b], part(a_far, na))
        afar(u).start()
        put(sani.at[b, :, pl.ds(0, ia)], part(a_in, ia))
        ani(u).start()
        term(u, mine, ROWS, a_out, oa)[...] = part(a_out, oa)

    def a_i1(u, b, s, r):
        a0(u).wait_recv()
        own = term(u, mine, ROWS, 0, wa)
        own[...] = own[...] + wide(ra0.at[s])

    def a_i2(u, b, s, r):
        xa_i(u).start()
        afar(u).wait_recv()
        put(safar.at[b], term(u, mine, ROWS, a_far, na)[...] + wide(rafar.at[s]))
        amid(u).start()

    def a_i3(u, b, s, r):
        amid(u).wait_recv()
        put(sani.at[b, :, pl.ds(0, oa)], term(u, mine, ROWS, a_out, oa)[...] + wide(ramid.at[s, :, a_o]))
        arno(u).start()
        ani(u).wait_recv()
        xa_i(u).wait()
        total = term(u, mine, ROWS, a_in, ia)[...] + wide(ramid.at[s, :, a_i]) + wide(rani.at[s, :, pl.ds(0, ia)])
        put(final(u, a_in, ia), wide(xa_res.at[r, :, pl.ds(0, ia)]) + total)
        afo(u).start()

    def a_ox(u, b, s, r):
        xa_o(u).start()

    def a_o4(u, b, s, r):
        arno(u).wait_recv()
        xa_o(u).wait()
        total = term(u, mine, ROWS, a_out, oa)[...] + wide(rani.at[s, :, pl.ds(0, oa)])
        put(final(u, a_out, oa), wide(xa_res.at[r, :, pl.ds(0, oa)]) + total)
        aof(u).start()

    def a_o5(u, b, s, r):
        afo(u).wait_recv()
        ayn(u).start()

    def a_i5(u, b, s, r):
        aof(u).wait_recv()
        agm(u).start()
        ayn(u).start()

    def a_i6(u, b, s, r):
        agm(u).wait_recv()
        afm(u).start()
        ayf(u).start()

    def a_o7(u, b, s, r):
        afm(u).wait_recv()
        ayf(u).start()

    def a_en(u, b, s, r):
        ayn(u).wait_recv()

    def a_ef(u, b, s, r):
        ayf(u).wait_recv()

    def b_o0(u, b, s, r):
        put(sbfar.at[b], term(u, 0, SUB, b_far, nb)[...])
        bfar(u).start()
        put(sbni.at[b, :, pl.ds(0, ib)], term(u, 0, SUB, b_in, ib)[...])
        bni(u).start()

    def b_i1(u, b, s, r):
        bfar(u).wait_recv()
        put(sbfar.at[b], term(u, 0, SUB, b_far, nb)[...] + wide(rbfar.at[s]))
        bmid(u).start()

    def b_i2(u, b, s, r):
        xb_i(u).start()
        bmid(u).wait_recv()
        put(sbni.at[b, :, pl.ds(0, ob_)], term(u, 0, SUB, b_out, ob_)[...] + wide(rbmid.at[s, :, b_o]))
        brno(u).start()
        bni(u).wait_recv()
        cut = pl.ds(0, ib)
        put(sbgy.at[b, :, cut],
            term(u, (1 - y) * ROWS, ROWS, b_in, ib)[...] + wide(rbmid.at[s, theirs, b_i]) + wide(rbni.at[s, theirs, cut]))
        bgy_i(u).start()
        own = term(u, mine, ROWS, b_in, ib)
        own[...] = own[...] + wide(rbmid.at[s, ours, b_i]) + wide(rbni.at[s, ours, cut])

    def b_o3(u, b, s, r):
        xb_o(u).start()
        brno(u).wait_recv()
        cut = pl.ds(0, ob_)
        put(sbgy.at[b, :, cut], term(u, (1 - y) * ROWS, ROWS, b_out, ob_)[...] + wide(rbni.at[s, theirs, cut]))
        bgy_o(u).start()
        own = term(u, mine, ROWS, b_out, ob_)
        own[...] = own[...] + wide(rbni.at[s, ours, cut])

    def finish_b(u, s, r, col, width, came, res, send):
        came(u).wait_recv()
        res(u).wait()
        cut = pl.ds(0, width)
        put(final(u, col, width), wide(xb_res.at[r, :, cut]) + (term(u, mine, ROWS, col, width)[...] + wide(rbgy.at[s, :, cut])))
        send(u).start()

    def b_i3(u, b, s, r):
        finish_b(u, s, r, b_in, ib, bgy_i, xb_i, bfy_i)

    def b_o4(u, b, s, r):
        finish_b(u, s, r, b_out, ob_, bgy_o, xb_o, bfy_o)

    def b_i4(u, b, s, r):
        bfy_i(u).wait_recv()
        bfo(u).start()

    def b_o5(u, b, s, r):
        bfy_o(u).wait_recv()
        bof(u).start()

    def b_i6(u, b, s, r):
        bof(u).wait_recv()
        bgm(u).start()

    def b_i7(u, b, s, r):
        bgm(u).wait_recv()
        bfm(u).start()

    def b_en(u, b, s, r):
        bfo(u).wait_recv()

    def b_ef(u, b, s, r):
        bfm(u).wait_recv()

    def d_s(u, b, s, r):
        share(u).start()

        @pl.when(u < nsub - IMAGES)
        def _():
            keep(u).start()

    def d_w(u, b, s, r):
        share(u).wait_recv()

        @pl.when(u < nsub - IMAGES)
        def _():
            keep(u).wait()

    steps = {
        "a_s0": (a_s0, [a0]), "a_o1": (a_o1, [afar, ani]), "a_i1": (a_i1, []), "a_i2": (a_i2, [amid]), "a_i3": (a_i3, [arno, afo]),
        "a_ox": (a_ox, []), "a_o4": (a_o4, [aof]), "a_o5": (a_o5, [ayn]), "a_i5": (a_i5, [agm, ayn]), "a_i6": (a_i6, [afm, ayf]),
        "a_o7": (a_o7, [ayf]), "a_en": (a_en, []), "a_ef": (a_ef, []), "b_o0": (b_o0, [bfar, bni]), "b_i1": (b_i1, [bmid]),
        "b_i2": (b_i2, [brno, bgy_i]), "b_o3": (b_o3, [bgy_o]), "b_i3": (b_i3, [bfy_i]), "b_o4": (b_o4, [bfy_o]), "b_i4": (b_i4, [bfo]),
        "b_o5": (b_o5, [bof]), "b_i6": (b_i6, [bgm]), "b_i7": (b_i7, [bfm]), "b_en": (b_en, []), "b_ef": (b_ef, []),
        "d_s": (d_s, [share]), "d_w": (d_w, []),
    }

    def role(name):
        return {"i": inner, "o": outer}.get(name[2]) if name not in ("b_en", "b_ef") else outer

    def exchange(t):
        n = 0
        for name, after in STEPS:
            if name[0] == "H":
                compute(t, n)
                n += 1
                continue
            do, sends = steps[name]
            u = t - PER - after
            go = (u >= 0) & (u < nsub)
            if role(name) is not None:
                go = go & role(name)

            @pl.when(go)
            def _():
                if sends:
                    @pl.when(u >= SENDS)
                    def _():
                        for m in sends:
                            m(u - SENDS).wait_send()
                do(u, lax.rem(u, SENDS), lax.rem(u, SLOTS), lax.rem(u, 4))

    def drain():
        for name in steps:
            def leave(sends=steps[name][1]):
                for m in sends:
                    for u in range(max(nsub - SENDS, 0), nsub):
                        m(u).wait_send()
            if role(name) is None:
                leave()
            elif steps[name][1]:
                pl.when(role(name))(leave)

    lanes = 1024

    def norm():
        def rows(i, _):
            r = pl.ds(pl.multiple_of(i * 16, 16), 16)
            acc = jnp.zeros((16, lanes), f32)
            for j in range(0, d, lanes):
                v = xb[r, j : j + lanes].astype(f32)
                acc = acc + v * v
            scale = lax.rsqrt(jnp.sum(acc, axis=-1, keepdims=True) * (1.0 / d) + 1e-6)
            for j in range(0, d, lanes):
                v = xb[r, j : j + lanes].astype(f32)
                xb[r, j : j + lanes] = (v * scale * gain[pl.ds(j, lanes)].astype(f32)[None]).astype(bf16)

        lax.fori_loop(0, CHUNK // 16, rows, None)

    def project(c, i):
        g, kind, j = c * 3 * nt + i, lax.div(i, nt), lax.rem(i, nt)

        def part(p, _):
            w_wait(2 * g + p)
            columns = pl.ds(pl.multiple_of(p * k2, 128), k2)
            one = jnp.dot(xb[:, columns], held_part(lax.rem(2 * g + p, HELD))[...], preferred_element_type=f32)
            w_start(2 * g + p + HELD)

            @pl.when(p == 0)
            def _():
                acc[...] = one

            @pl.when(p == 1)
            def _():
                acc[...] = acc[...] + one

        lax.fori_loop(0, 2, part, None)
        r = acc[...].astype(bf16)
        tokens = pl.ds(pl.multiple_of(c * CHUNK, CHUNK), CHUNK)
        for n in range(TILE // HEAD):
            h = j * (TILE // HEAD) + n
            one = r[:, n * HEAD : (n + 1) * HEAD]

            @pl.when(kind < 2)
            def _():
                w = one.astype(f32)
                w = (w * cs[...] + pltpu.roll(w, HEAD // 2, 1) * sn[...]).astype(bf16)

                @pl.when(kind == 0)
                def _():
                    qb[h] = w

                @pl.when(kind == 1)
                def _():
                    kc[h, tokens, :] = w

            @pl.when(kind == 2)
            def _():
                vt[h, pl.ds(0, HEAD), tokens] = one.T

    e = HEAD**-0.5 * LOG2E

    def attention(c):
        top[...] = jnp.full(top.shape, NEG, f32)
        mix[...] = jnp.zeros(mix.shape, f32)

        def block(j, masked):
            here = pl.ds(pl.multiple_of(j * CHUNK, CHUNK), CHUNK)
            scores = [_dot(kc[h, here, :], qb[h], 1, 1) for h in range(hl)]
            if masked:
                ok = lax.broadcasted_iota(jnp.int32, (CHUNK, CHUNK), 1) >= lax.broadcasted_iota(jnp.int32, (CHUNK, CHUNK), 0)
            weights, keeps = [], []
            for h, s in enumerate(scores):
                if masked:
                    s = jnp.where(ok, s, 2 * NEG)
                old = top[h : h + 1, :]
                new = jnp.maximum(old, s.max(axis=0, keepdims=True))
                top[h : h + 1, :] = new
                weights.append(jnp.exp2((s - new) * e).astype(bf16))
                keeps.append(jnp.exp2((old - new) * e))
            for h in range(hl):
                mix[h] = mix[h] * keeps[h] + _dot(vt[h, :, here], weights[h], 1, 0)

        lax.fori_loop(0, c, lambda j, _: block(j, False), None)
        block(c, True)
        b = lax.rem(c, 2)
        for h in range(hl):
            total = mix[h, HEAD : HEAD + 1, :]
            seen[b, :, h * HEAD : (h + 1) * HEAD] = (mix[h, :HEAD, :] * (1 / total)).T.astype(bf16)

    def output(c, quarter):
        b, tiles, k = lax.rem(c, 2), half // WO_TILE, hl * HEAD

        def tile(n, _):
            o_wait(n)
            columns, slot = pl.ds(pl.multiple_of(n * WO_TILE, WO_TILE), WO_TILE), lax.rem(n, WO_HELD)

            @pl.when(c > 0)
            def _():
                pp[b, :, columns] = jnp.dot(seen[b], ob[slot], preferred_element_type=f32)

            @pl.when(c == 0)
            def _():
                one = jnp.dot(seen[0, :, :k], ob[slot, :k, :], preferred_element_type=f32)
                put(xb.at[:, pl.ds(pl.multiple_of(half + n * WO_TILE, WO_TILE), WO_TILE)], one)
                term_copy(n).start()
                pp[0, :, columns] = jnp.dot(seen[0, :, :k], ob[slot, k:, :], preferred_element_type=f32)

            @pl.when(n + WO_HELD < tiles)
            def _():
                o_starts(c, n + WO_HELD)

        lax.fori_loop(quarter * (tiles // 4), (quarter + 1) * (tiles // 4), tile, None)

    def join():
        def tile(n, _):
            term_copy(n).wait_recv()
            columns = pl.ds(pl.multiple_of(n * WO_TILE, WO_TILE), WO_TILE)
            pp[0, :, columns] = pp[0, :, columns] + wide(xb.at[:, columns])
            term_copy(n).wait_send()

        lax.fori_loop(0, half // WO_TILE, tile, None)
        for copy in (*x_copies(1), *cs_copies(1)):
            copy.start()
        ext_copy().start()

    def compute(t, n):
        each = PARTS // PER
        c, p = lax.div(t, PER), lax.rem(t, PER) * each + n
        here = set(range(n, PARTS, each))

        def branch(parts, on, do):
            if here & set(parts):
                pl.when((t < nsub) & on)(do)

        def first():
            for copy in (*x_copies(c), *cs_copies(c)):
                copy.wait()
            norm()

        def middle_():
            @pl.when(c == 0)
            def _():
                pl.semaphore_signal(free, inc=1, device_id={"tp": partner})

            @pl.when((c > 0) & (c + 1 < nch))
            def _():
                for copy in (*x_copies(c + 1), *cs_copies(c + 1)):
                    copy.start()

            @pl.when(c >= 3)
            def _():
                seen_copy(c - 2).wait_send()
            attention(c)

            @pl.when(c > 0)
            def _():
                seen_copy(c).start()

            @pl.when(c == 0)
            def _():
                pl.semaphore_wait(free, 1)

        def early():
            @pl.when(c == 1)
            def _():
                ext_copy().wait_recv()

            for i in range(WO_HELD):
                o_starts(c, i)

        branch([0], p == 0, first)
        branch(range(1, 10), (p >= 1) & (p <= 3 * nt), lambda: project(c, p - 1))
        branch([6], p == 6, early)
        branch([10], p == 10, middle_)
        branch([12], (p == 12) & (c > 0), lambda: seen_copy(c).wait_recv())
        branch(range(12, 16), p >= 12, lambda: output(c, p - 12))
        branch([15], (p == 15) & (c == 0), join)

    for copy in (*x_copies(0), *cs_copies(0)):
        copy.start()
    for n in range(HELD):
        w_start(n)
    for h in range(hl):
        vt[h, HEAD:, :] = jnp.ones((8, vt.shape[2]), bf16)

    @pl.when(inner)
    def _():
        pl.semaphore_wait(barrier, 4)

    @pl.when(outer)
    def _():
        pl.semaphore_wait(barrier, 3)


    held = _held(wb, xb, d)

    def tick(t, _):
        exchange(t)
        for i, (count, copies) in enumerate(held):
            share_of = -(-count // HOLD_TICKS)

            @pl.when((t >= nsub) & (t < nsub + HOLD_TICKS))
            def _():
                def one(j, _):
                    @pl.when(j < count)
                    def _():
                        there, here = copies(j)
                        pltpu.make_async_copy(out.at[there], here, s_hold.at[i]).start()

                lax.fori_loop((t - nsub) * share_of, (t - nsub + 1) * share_of, one, None)

    lax.fori_loop(0, PER + nsub + max(AFTER.values()), tick, None)
    drain()
    for i in range(HELD):
        pltpu.make_async_copy(wq.at[pl.ds(0, k2), pl.ds(0, TILE)], held_part(i), s_hold.at[0]).wait()
    pltpu.make_async_copy(x.at[pl.ds(0, CHUNK), :], xb, s_hold.at[1]).wait()
    for c in range(max(nch - 2, 1), nch):
        seen_copy(c).wait_send()
    ext_copy().wait_send()


def _held(wb, xb, d):
    kinds, row = [], 0

    def add(count, rows, width, where):
        nonlocal row
        across, start = d // width, row

        def piece(j):
            block, at = lax.div(j, across), lax.rem(j, across)
            there = pl.ds(pl.multiple_of(start + block * rows, 16), rows), pl.ds(pl.multiple_of(at * width, 128), width)
            return there, where(block, at)

        kinds.append((count * across, piece))
        row += count * rows

    h = wb.shape[0] * TILE // d
    add(1, h, TILE, lambda block, at: wb.at[pl.ds(pl.multiple_of(at * h, 16), h), :])
    add(xb.shape[0] // 64, 64, d, lambda block, at: xb.at[pl.ds(pl.multiple_of(block * 64, 16), 64), :])
    return kinds


def _held_rows(d):
    return HELD * (d // 2 * TILE // d) + CHUNK


def layer(x, gain, wq, wk, wv, wo, cos, sin):
    rows, d = x.shape
    hl = wq.shape[1] // HEAD
    half, qa = d // 2, d // 4
    nch = rows // CHUNK
    v, dma = pltpu.VMEM, pltpu.SemaphoreType.DMA
    hbm = pl.BlockSpec(memory_space=pl.ANY)
    wa, ia, oa, ib, ob = _split(half)
    na, nb, qa, qb = ia + oa, ib + ob, max(ia, oa), max(ib, ob)

    def buffers(n, *shapes):
        return [v((n, *s), bf16) for s in shapes]

    scratch = [
        v((WO_HELD, 2 * hl * HEAD, WO_TILE), bf16), v((hl, rows, HEAD), bf16), v((hl, HEAD + 8, rows), bf16), v((hl, CHUNK, HEAD), bf16), v((2, CHUNK, 2 * hl * HEAD), bf16), v((2, CHUNK, half), f32),
        v((hl, HEAD + 8, CHUNK), f32), v((CHUNK, TILE), f32), v((hl, CHUNK), f32), v((CHUNK, HEAD), f32), v((CHUNK, HEAD), f32),
        *buffers(4, (ROWS, qa), (ROWS, qb)),
        *buffers(SLOTS, (ROWS, wa), (ROWS, na), (ROWS, qa), (ROWS, na), (SUB, nb), (SUB, qb), (SUB, nb), (ROWS, qb)),
        *buffers(SENDS, (ROWS, wa), (ROWS, na), (ROWS, qa), (SUB, nb), (SUB, qb), (ROWS, qb)),
        dma((2,)), dma((HELD,)), dma((WO_HELD, 2)), dma((2,)), dma((2, 4)), dma((SENDS,)), dma((RS_KINDS + AG_KINDS, SENDS)), dma((RS_KINDS, SLOTS)),
        dma((AG_KINDS, MARKS)), dma((2, 2)), dma((2,)), dma((2,)), dma((2, half // WO_TILE)), pltpu.SemaphoreType.REGULAR,
    ]
    kept = [v((HELD * (d // 2), TILE), bf16), v((CHUNK, d), bf16), v((IMAGES, SUB, half), bf16)]
    out, _, *held = pl.pallas_call(
        functools.partial(_kernel, d=d, hl=hl, nch=nch),
        name="layer",
        in_specs=[hbm, pl.BlockSpec(memory_space=pltpu.VMEM), hbm, hbm, hbm, hbm, hbm, hbm],
        out_specs=[hbm, hbm] + [pl.BlockSpec(memory_space=pltpu.VMEM)] * len(kept),
        out_shape=[jax.ShapeDtypeStruct((rows, d), bf16), jax.ShapeDtypeStruct((hl * HEAD, half), bf16), *kept],
        scratch_shapes=scratch,
        compiler_params=pltpu.CompilerParams(collective_id=0, has_side_effects=True, vmem_limit_bytes=LAYER_VMEM),
    )(x, gain, wq, wk, wv, wo, cos, sin)
    return handed(out, *held)


def _hand(a, wb, xb, img, out, ring, s_in, s_out, s_held, *, first, last):
    d = a.shape[1]
    half, nsub, (slots, rows) = d // 2, a.shape[0] // SUB, ring.shape[:2]
    core = lax.rem(lax.axis_index("tp"), 2)
    mine, other = (pl.ds(pl.multiple_of(n * half, 128), half) for n in (core, 1 - core))
    whole = (last - first) // rows
    total = whole + (a.shape[0] - last) // rows

    def ends(i):
        at = pl.ds(first + i * rows, rows)
        return (at, ring.at[i % slots]) if i < whole else ((at, other), ring.at[i % slots, :, pl.ds(0, half)])

    def come(i):
        there, here = ends(i)
        return pltpu.make_async_copy(a.at[there], here, s_in.at[i % slots])

    def go(i):
        there, here = ends(i)
        return pltpu.make_async_copy(here, out.at[there], s_out.at[i % slots])

    kinds = _held(wb, xb, d)
    kinds.append((IMAGES, lambda j: ((pl.ds(pl.multiple_of(last + j * SUB, 16), SUB), mine), img.at[lax.rem(nsub - IMAGES + j, IMAGES)])))

    def held(n, low, high, act):
        def one(j, _):
            there, here = kinds[n][1](j)
            act(pltpu.make_async_copy(here, out.at[there], s_held.at[n]))

        lax.fori_loop(low, high, one, None)

    ahead = slots // 2
    for i in range(min(ahead, total)):
        come(i).start()
    for i in range(total):
        for n, (count, _) in enumerate(kinds):
            held(n, count * i // total, count * (i + 1) // total, lambda copy: copy.start())
        come(i).wait()
        go(i).start()
        j = i + ahead
        if j < total:
            if j >= slots:
                go(j - slots).wait()
            come(j).start()
    for i in range(max(total - slots, 0), total):
        go(i).wait()
    for n, (count, _) in enumerate(kinds):
        held(n, 0, count, lambda copy: copy.wait())


def handed(a, wb, xb, img):
    d = a.shape[1]
    first, last = _held_rows(d), a.shape[0] - IMAGES * SUB
    slots, rows = 7, 32
    dma = pltpu.SemaphoreType.DMA
    any_, vmem = pl.BlockSpec(memory_space=pl.ANY), pl.BlockSpec(memory_space=pltpu.VMEM)
    return pl.pallas_call(
        functools.partial(_hand, first=first, last=last),
        name="hand",
        in_specs=[any_] + [vmem] * 3,
        out_specs=any_,
        out_shape=jax.ShapeDtypeStruct(a.shape, a.dtype),
        scratch_shapes=[pltpu.VMEM((slots, rows, d), bf16), dma((slots,)), dma((slots,)), dma((3,))],
        compiler_params=pltpu.CompilerParams(vmem_limit_bytes=HAND_VMEM),
    )(a, wb, xb, img)


def solution(mesh):
    def step(x, gain, wq, wk, wv, wo):
        half = HEAD // 2
        angle = np.arange(x.shape[0], dtype=np.float32)[:, None] * np.float32(THETA) ** (-np.arange(half, dtype=np.float32) / half)
        cos, sin = np.cos(angle), np.sin(angle)
        cos, sin = (jnp.asarray(np.concatenate(t, -1), f32) for t in ([cos, cos], [-sin, sin]))
        return layer(x, gain, wq, wk, wv, wo, cos, sin)

    tokens, columns = P("dp", None), P(None, "tp")
    return jax.shard_map(
        step,
        mesh=mesh,
        in_specs=(tokens, P(None), columns, columns, columns, P("tp", None)),
        out_specs=tokens,
        check_vma=False,
    )
```

```python
import functools

import jax
import jax.numpy as jnp
import numpy as np
from jax import lax
from jax.experimental import pallas as pl
from jax.experimental.pallas import tpu as pltpu
from jax.sharding import PartitionSpec as P

HEAD = 128
LAYER_VMEM, HAND_VMEM = 362 * 2**20 // 10, 6 * 2**20
THETA = 10000
LOG2E = 1.4426950408889634
NEG = -1e30
CHUNK = 256
SUB = 32
PER = CHUNK // SUB
ROWS = SUB // 2
PARTS = 16
TILE = 256
HELD = 5
HOLD_TICKS = 10
WO_TILE = 512
WO_HELD = 3
EARLY = 10
SLOTS = 6
IMAGES = 14
MARKS = 16
SENDS = 3
RS_KINDS, AG_KINDS = 10, 12
A_SHARE = 7 / 12
INNER = 0.5
f32, bf16 = jnp.float32, jnp.bfloat16

STEPS = (
    ("b_i1", 1), ("b_i2", 2), ("b_en", 7), ("b_i3", 3), ("a_i2", 2), ("b_o5", 6), ("d_s", 12), ("a_en", 8), ("d_w", 15),
    ("a_ox", 3), ("a_i5", 5), ("a_s0", 0), ("a_i3", 3), ("b_i4", 4), ("b_o0", 0), ("H1", 0), ("b_i6", 6), ("a_i6", 6),
    ("b_o3", 3), ("a_o1", 1), ("b_o4", 4), ("a_o5", 6), ("a_o7", 9), ("a_o4", 4), ("a_i1", 1), ("b_ef", 11), ("a_ef", 11),
    ("b_i7", 7), ("H2", 0),
)
AFTER = dict(STEPS)


def _dot(a, b, ca, cb):
    return lax.dot_general(a, b, (((ca,), (cb,)), ((), ())), preferred_element_type=f32)


def _split(half):
    def near(share, unit, all_):
        return min(max(round(all_ * share / unit), 1), all_ // unit - 1) * unit

    wa = near(A_SHARE, 256, half)
    na, nb = wa // 2, (half - wa) // 2
    ia, ib = near(INNER, 128, na), near(INNER, 128, nb)
    return wa, ia, na - ia, ib, nb - ib


def _kernel(x, gain, wq, wk, wv, wo, cos, sin, out, wo_ext, wb, xb, img, ob, kc, vt, qb, seen, pp, mix, acc, top, cs, sn, xa_res, xb_res,
            ra0, rafar, rani, ramid, rbfar, rbni, rbmid, rbgy, sa0, safar, sani, sbfar, sbni, sbgy,
            s_x, s_w, s_o, s_cs, s_res, s_local, s_send, s_rs, s_ag, s_seen, s_ext, s_hold, *, d, hl, nch):
    half = d // 2
    wa, ia, oa, ib, ob_ = _split(half)
    na, nb = ia + oa, ib + ob_
    nt = hl * HEAD // TILE
    nsub = nch * PER
    pos = lax.axis_index("tp")
    y, z, core = lax.div(pos, 8), lax.rem(lax.div(pos, 2), 4), lax.rem(pos, 2)
    side = lax.div(z, 2)
    inner = (z == 1) | (z == 2)
    outer = (z == 0) | (z == 3)

    def at(y, z, core):
        return (y * 4 + z) * 2 + core

    partner = at(y, z, 1 - core)
    across = at(1 - y, z, core)
    middle = at(y, 3 - z, core)
    beside = at(y, 1 - z + 4 * side, core)
    col0 = core * half

    barrier = pltpu.get_barrier_semaphore()
    for dev in (partner, across, beside):
        pl.semaphore_signal(barrier, inc=1, device_id={"tp": dev})

    @pl.when(inner)
    def _():
        pl.semaphore_signal(barrier, inc=1, device_id={"tp": middle})

    pieces = 4

    def x_copies(c):
        n = CHUNK // pieces
        return [pltpu.make_async_copy(x.at[pl.ds(pl.multiple_of(c * CHUNK + i * n, n), n), :], xb.at[pl.ds(i * n, n), :], s_x.at[i])
                for i in range(pieces)]

    def cs_copies(c):
        rows = pl.ds(c * CHUNK, CHUNK)
        return pltpu.make_async_copy(cos.at[rows, :], cs, s_cs.at[0]), pltpu.make_async_copy(sin.at[rows, :], sn, s_cs.at[1])

    k2, cuts = d // 2, 2

    def held_part(slot):
        return wb.at[pl.ds(pl.multiple_of(slot * k2, k2), k2), :]

    def w_start(h):
        i, part, slot = lax.rem(lax.div(h, 2), 3 * nt), lax.rem(h, 2), lax.rem(h, HELD)
        kind, tile = lax.div(i, nt), lax.rem(i, nt)
        for n, w in enumerate((wq, wk, wv)):
            @pl.when((kind == n) & (h < nch * 3 * nt * 2))
            def _():
                for a in range(cuts):
                    rows = pl.ds(pl.multiple_of(part * k2 + a * (k2 // cuts), k2 // cuts), k2 // cuts)
                    there = pl.ds(pl.multiple_of(slot * k2 + a * (k2 // cuts), k2 // cuts), k2 // cuts)
                    pltpu.make_async_copy(w.at[rows, pl.ds(pl.multiple_of(tile * TILE, TILE), TILE)], wb.at[there, :], s_w.at[slot]).start()

    def w_wait(h):
        slot = lax.rem(h, HELD)
        pltpu.make_async_copy(wq.at[pl.ds(0, k2), pl.ds(0, TILE)], held_part(slot), s_w.at[slot]).wait()

    def o_starts(c, n):
        slot, k = lax.rem(n, WO_HELD), hl * HEAD
        own, ext = (pl.ds(pl.multiple_of(at + n * WO_TILE, WO_TILE), WO_TILE) for at in (col0, 0))
        pltpu.make_async_copy(wo.at[:, own], ob.at[slot, pl.ds(0, k), :], s_o.at[slot, 0]).start()
        pltpu.make_async_copy(wo_ext.at[:, ext], ob.at[slot, pl.ds(k, k), :], s_o.at[slot, 1]).start()

    def o_wait(n):
        slot, k = lax.rem(n, WO_HELD), hl * HEAD
        for i in range(2):
            pltpu.make_async_copy(wo.at[:, pl.ds(0, WO_TILE)], ob.at[slot, pl.ds(i * k, k), :], s_o.at[slot, i]).wait()

    def ext_copy():
        return pltpu.make_async_remote_copy(wo.at[:, pl.ds(pl.multiple_of((1 - core) * half, half), half)], wo_ext, s_ext.at[0], s_ext.at[1],
                                            device_id={"tp": partner})

    def seen_copy(c):
        k, b = hl * HEAD, lax.rem(c, 2)
        return pltpu.make_async_remote_copy(seen.at[b, :, pl.ds(0, k)], seen.at[b, :, pl.ds(k, k)], s_seen.at[0, b], s_seen.at[1, b],
                                            device_id={"tp": partner})

    kinds = {}

    def number(table, name):
        return kinds.setdefault((table, name), sum(t == table for t, _ in kinds))

    def rs(name, src, dst, dev, width=None):
        n = number("rs", name)

        def make(u):
            b, cut = lax.rem(u, SENDS), (slice(None), pl.ds(0, width or src.shape[2]))
            return pltpu.make_async_remote_copy(src.at[(b, *cut)], dst.at[(lax.rem(u, SLOTS), *cut)], s_send.at[n, b], s_rs.at[n, lax.rem(u, SLOTS)],
                                                device_id={"tp": dev})
        return make

    def place(row, height, col, width):
        return lambda u: (pl.ds(pl.multiple_of(u * SUB + row, 16), height), pl.ds(pl.multiple_of(col0 + col, 128), width))

    def ag(name, where, dev):
        n = number("ag", name)

        def make(u):
            there = img.at[(lax.rem(u, IMAGES), *where)]
            return pltpu.make_async_remote_copy(there, there, s_send.at[RS_KINDS + n, lax.rem(u, SENDS)], s_ag.at[n, lax.rem(u, MARKS)],
                                                device_id={"tp": dev})
        return make

    def part(row, height, col, width):
        return pl.ds(pl.multiple_of(row, 16), height), pl.ds(pl.multiple_of(col, 128), width)

    def rows_of(u):
        return out.at[pl.ds(pl.multiple_of(u * SUB, 16), SUB), pl.ds(pl.multiple_of(col0, 128), half)]

    def share(u):
        n = number("ag", "share")
        return pltpu.make_async_remote_copy(img.at[lax.rem(u, IMAGES)], rows_of(u), s_send.at[RS_KINDS + n, lax.rem(u, SENDS)],
                                            s_ag.at[n, lax.rem(u, MARKS)], device_id={"tp": partner})

    def keep(u):
        return pltpu.make_async_copy(img.at[lax.rem(u, IMAGES)], rows_of(u), s_local.at[lax.rem(u, 8)])

    def residual(n, dst, where, width):
        def make(u):
            b = lax.rem(u, 4)
            return pltpu.make_async_copy(x.at[where(u)], dst.at[b, :, pl.ds(0, width)], s_res.at[n, b])
        return make

    mine = y * ROWS
    a_near, a_far = side * na, (1 - side) * na
    b_near, b_far = wa + side * nb, wa + (1 - side) * nb
    a_in, a_out = a_near + (1 - side) * oa, a_near + side * ia
    b_in, b_out = b_near + (1 - side) * ob_, b_near + side * ib
    a_i, a_o, b_i, b_o = (pl.ds(pl.multiple_of(n, 128), w)
                          for n, w in (((1 - side) * oa, ia), (side * ia, oa), ((1 - side) * ob_, ib), (side * ib, ob_)))

    a0 = rs("a0", sa0, ra0, across)
    afar = rs("afar", safar, rafar, beside)
    ani = rs("ani", sani, rani, beside, ia)
    amid = rs("amid", safar, ramid, middle)
    arno = rs("arno", sani, rani, beside, oa)
    bfar = rs("bfar", sbfar, rbfar, beside)
    bni = rs("bni", sbni, rbni, beside, ib)
    bmid = rs("bmid", sbfar, rbmid, middle)
    brno = rs("brno", sbni, rbni, beside, ob_)
    bgy_i = rs("bgy", sbgy, rbgy, across, ib)
    bgy_o = rs("bgy", sbgy, rbgy, across, ob_)

    afo = ag("afo", part(mine, ROWS, a_in, ia), beside)
    aof = ag("aof", part(mine, ROWS, a_out, oa), beside)
    ayn = ag("ayn", part(mine, ROWS, a_near, na), across)
    ayf = ag("ayf", part(mine, ROWS, a_far, na), across)
    agm = ag("agm", part(mine, ROWS, a_near, na), middle)
    afm = ag("afm", part(mine, ROWS, a_far, na), beside)
    bfy_i = ag("bfy", part(mine, ROWS, b_in, ib), across)
    bfy_o = ag("bfy", part(mine, ROWS, b_out, ob_), across)
    bfo = ag("bfo", part(0, SUB, b_in, ib), beside)
    bof = ag("bof", part(0, SUB, b_out, ob_), beside)
    bgm = ag("bgm", part(0, SUB, b_near, nb), middle)
    bfm = ag("bfm", part(0, SUB, b_far, nb), beside)
    xa_i, xa_o = (residual(0, xa_res, place(mine, ROWS, c, w), w) for c, w in ((a_in, ia), (a_out, oa)))
    xb_i, xb_o = (residual(1, xb_res, place(mine, ROWS, c, w), w) for c, w in ((b_in, ib), (b_out, ob_)))

    def term(u, row, height, col, width):
        rows = pl.ds(pl.multiple_of(lax.rem(u, PER) * SUB + row, 16), height)
        return pp.at[lax.rem(lax.div(u, PER), 2), rows, pl.ds(pl.multiple_of(col, 128), width)]

    def final(u, col, width):
        return img.at[(lax.rem(u, IMAGES), *part(mine, ROWS, col, width))]

    def wide(ref):
        return ref[...].astype(f32)

    def put(ref, value):
        ref[...] = value.astype(bf16)

    ours, theirs = pl.ds(pl.multiple_of(y * ROWS, 16), ROWS), pl.ds(pl.multiple_of((1 - y) * ROWS, 16), ROWS)

    def a_s0(u, b, s, r):
        put(sa0.at[b], term(u, (1 - y) * ROWS, ROWS, 0, wa)[...])
        a0(u).start()

    def a_o1(u, b, s, r):
        a0(u).wait_recv()

        def part(col, width):
            return term(u, mine, ROWS, col, width)[...] + wide(ra0.at[s, :, pl.ds(pl.multiple_of(col, 128), width)])

        put(safar.at[b], part(a_far, na))
        afar(u).start()
        put(sani.at[b, :, pl.ds(0, ia)], part(a_in, ia))
        ani(u).start()
        term(u, mine, ROWS, a_out, oa)[...] = part(a_out, oa)

    def a_i1(u, b, s, r):
        a0(u).wait_recv()
        own = term(u, mine, ROWS, 0, wa)
        own[...] = own[...] + wide(ra0.at[s])

    def a_i2(u, b, s, r):
        xa_i(u).start()
        afar(u).wait_recv()
        put(safar.at[b], term(u, mine, ROWS, a_far, na)[...] + wide(rafar.at[s]))
        amid(u).start()

    def a_i3(u, b, s, r):
        amid(u).wait_recv()
        put(sani.at[b, :, pl.ds(0, oa)], term(u, mine, ROWS, a_out, oa)[...] + wide(ramid.at[s, :, a_o]))
        arno(u).start()
        ani(u).wait_recv()
        xa_i(u).wait()
        total = term(u, mine, ROWS, a_in, ia)[...] + wide(ramid.at[s, :, a_i]) + wide(rani.at[s, :, pl.ds(0, ia)])
        put(final(u, a_in, ia), wide(xa_res.at[r, :, pl.ds(0, ia)]) + total)
        afo(u).start()

    def a_ox(u, b, s, r):
        xa_o(u).start()

    def a_o4(u, b, s, r):
        arno(u).wait_recv()
        xa_o(u).wait()
        total = term(u, mine, ROWS, a_out, oa)[...] + wide(rani.at[s, :, pl.ds(0, oa)])
        put(final(u, a_out, oa), wide(xa_res.at[r, :, pl.ds(0, oa)]) + total)
        aof(u).start()

    def a_o5(u, b, s, r):
        afo(u).wait_recv()
        ayn(u).start()

    def a_i5(u, b, s, r):
        aof(u).wait_recv()
        agm(u).start()
        ayn(u).start()

    def a_i6(u, b, s, r):
        agm(u).wait_recv()
        afm(u).start()
        ayf(u).start()

    def a_o7(u, b, s, r):
        afm(u).wait_recv()
        ayf(u).start()

    def a_en(u, b, s, r):
        ayn(u).wait_recv()

    def a_ef(u, b, s, r):
        ayf(u).wait_recv()

    def b_o0(u, b, s, r):
        put(sbfar.at[b], term(u, 0, SUB, b_far, nb)[...])
        bfar(u).start()
        put(sbni.at[b, :, pl.ds(0, ib)], term(u, 0, SUB, b_in, ib)[...])
        bni(u).start()

    def b_i1(u, b, s, r):
        bfar(u).wait_recv()
        put(sbfar.at[b], term(u, 0, SUB, b_far, nb)[...] + wide(rbfar.at[s]))
        bmid(u).start()

    def b_i2(u, b, s, r):
        xb_i(u).start()
        bmid(u).wait_recv()
        put(sbni.at[b, :, pl.ds(0, ob_)], term(u, 0, SUB, b_out, ob_)[...] + wide(rbmid.at[s, :, b_o]))
        brno(u).start()
        bni(u).wait_recv()
        cut = pl.ds(0, ib)
        put(sbgy.at[b, :, cut],
            term(u, (1 - y) * ROWS, ROWS, b_in, ib)[...] + wide(rbmid.at[s, theirs, b_i]) + wide(rbni.at[s, theirs, cut]))
        bgy_i(u).start()
        own = term(u, mine, ROWS, b_in, ib)
        own[...] = own[...] + wide(rbmid.at[s, ours, b_i]) + wide(rbni.at[s, ours, cut])

    def b_o3(u, b, s, r):
        xb_o(u).start()
        brno(u).wait_recv()
        cut = pl.ds(0, ob_)
        put(sbgy.at[b, :, cut], term(u, (1 - y) * ROWS, ROWS, b_out, ob_)[...] + wide(rbni.at[s, theirs, cut]))
        bgy_o(u).start()
        own = term(u, mine, ROWS, b_out, ob_)
        own[...] = own[...] + wide(rbni.at[s, ours, cut])

    def finish_b(u, s, r, col, width, came, res, send):
        came(u).wait_recv()
        res(u).wait()
        cut = pl.ds(0, width)
        put(final(u, col, width), wide(xb_res.at[r, :, cut]) + (term(u, mine, ROWS, col, width)[...] + wide(rbgy.at[s, :, cut])))
        send(u).start()

    def b_i3(u, b, s, r):
        finish_b(u, s, r, b_in, ib, bgy_i, xb_i, bfy_i)

    def b_o4(u, b, s, r):
        finish_b(u, s, r, b_out, ob_, bgy_o, xb_o, bfy_o)

    def b_i4(u, b, s, r):
        bfy_i(u).wait_recv()
        bfo(u).start()

    def b_o5(u, b, s, r):
        bfy_o(u).wait_recv()
        bof(u).start()

    def b_i6(u, b, s, r):
        bof(u).wait_recv()
        bgm(u).start()

    def b_i7(u, b, s, r):
        bgm(u).wait_recv()
        bfm(u).start()

    def b_en(u, b, s, r):
        bfo(u).wait_recv()

    def b_ef(u, b, s, r):
        bfm(u).wait_recv()

    def d_s(u, b, s, r):
        share(u).start()

        @pl.when(u < nsub - IMAGES)
        def _():
            keep(u).start()

    def d_w(u, b, s, r):
        share(u).wait_recv()

        @pl.when(u < nsub - IMAGES)
        def _():
            keep(u).wait()

    steps = {
        "a_s0": (a_s0, [a0]), "a_o1": (a_o1, [afar, ani]), "a_i1": (a_i1, []), "a_i2": (a_i2, [amid]), "a_i3": (a_i3, [arno, afo]),
        "a_ox": (a_ox, []), "a_o4": (a_o4, [aof]), "a_o5": (a_o5, [ayn]), "a_i5": (a_i5, [agm, ayn]), "a_i6": (a_i6, [afm, ayf]),
        "a_o7": (a_o7, [ayf]), "a_en": (a_en, []), "a_ef": (a_ef, []), "b_o0": (b_o0, [bfar, bni]), "b_i1": (b_i1, [bmid]),
        "b_i2": (b_i2, [brno, bgy_i]), "b_o3": (b_o3, [bgy_o]), "b_i3": (b_i3, [bfy_i]), "b_o4": (b_o4, [bfy_o]), "b_i4": (b_i4, [bfo]),
        "b_o5": (b_o5, [bof]), "b_i6": (b_i6, [bgm]), "b_i7": (b_i7, [bfm]), "b_en": (b_en, []), "b_ef": (b_ef, []),
        "d_s": (d_s, [share]), "d_w": (d_w, []),
    }

    def role(name):
        return {"i": inner, "o": outer}.get(name[2]) if name not in ("b_en", "b_ef") else outer

    def exchange(t):
        n = 0
        for name, after in STEPS:
            if name[0] == "H":
                compute(t, n)
                n += 1
                continue
            do, sends = steps[name]
            u = t - PER - after
            go = (u >= 0) & (u < nsub)
            if role(name) is not None:
                go = go & role(name)

            @pl.when(go)
            def _():
                if sends:
                    @pl.when(u >= SENDS)
                    def _():
                        for m in sends:
                            m(u - SENDS).wait_send()
                do(u, lax.rem(u, SENDS), lax.rem(u, SLOTS), lax.rem(u, 4))

    def drain():
        for name in steps:
            def leave(sends=steps[name][1]):
                for m in sends:
                    for u in range(max(nsub - SENDS, 0), nsub):
                        m(u).wait_send()
            if role(name) is None:
                leave()
            elif steps[name][1]:
                pl.when(role(name))(leave)

    lanes = 1024

    def norm(first, last):
        def rows(i, _):
            r = pl.ds(pl.multiple_of(i * 16, 16), 16)
            acc = jnp.zeros((16, lanes), f32)
            for j in range(0, d, lanes):
                v = xb[r, j : j + lanes].astype(f32)
                acc = acc + v * v
            scale = lax.rsqrt(jnp.sum(acc, axis=-1, keepdims=True) * (1.0 / d) + 1e-6)
            for j in range(0, d, lanes):
                v = xb[r, j : j + lanes].astype(f32)
                xb[r, j : j + lanes] = (v * scale * gain[pl.ds(j, lanes)].astype(f32)[None]).astype(bf16)

        lax.fori_loop(first // 16, last // 16, rows, None)

    def project(c, i):
        g, kind, j = c * 3 * nt + i, lax.div(i, nt), lax.rem(i, nt)

        def part(p, _):
            w_wait(2 * g + p)
            columns = pl.ds(pl.multiple_of(p * k2, 128), k2)
            one = jnp.dot(xb[:, columns], held_part(lax.rem(2 * g + p, HELD))[...], preferred_element_type=f32)
            w_start(2 * g + p + HELD)

            @pl.when(p == 0)
            def _():
                acc[...] = one

            @pl.when(p == 1)
            def _():
                acc[...] = acc[...] + one

        lax.fori_loop(0, 2, part, None)
        r = acc[...].astype(bf16)
        tokens = pl.ds(pl.multiple_of(c * CHUNK, CHUNK), CHUNK)
        for n in range(TILE // HEAD):
            h = j * (TILE // HEAD) + n
            one = r[:, n * HEAD : (n + 1) * HEAD]

            @pl.when(kind < 2)
            def _():
                w = one.astype(f32)
                w = (w * cs[...] + pltpu.roll(w, HEAD // 2, 1) * sn[...]).astype(bf16)

                @pl.when(kind == 0)
                def _():
                    qb[h] = w

                @pl.when(kind == 1)
                def _():
                    kc[h, tokens, :] = w

            @pl.when(kind == 2)
            def _():
                vt[h, pl.ds(0, HEAD), tokens] = one.T

    e = HEAD**-0.5 * LOG2E

    def attention(c):
        top[...] = jnp.full(top.shape, NEG, f32)
        mix[...] = jnp.zeros(mix.shape, f32)

        def block(j, masked):
            here = pl.ds(pl.multiple_of(j * CHUNK, CHUNK), CHUNK)
            scores = [_dot(kc[h, here, :], qb[h], 1, 1) for h in range(hl)]
            if masked:
                ok = lax.broadcasted_iota(jnp.int32, (CHUNK, CHUNK), 1) >= lax.broadcasted_iota(jnp.int32, (CHUNK, CHUNK), 0)
            weights, keeps = [], []
            for h, s in enumerate(scores):
                if masked:
                    s = jnp.where(ok, s, 2 * NEG)
                old = top[h : h + 1, :]
                new = jnp.maximum(old, s.max(axis=0, keepdims=True))
                top[h : h + 1, :] = new
                weights.append(jnp.exp2((s - new) * e).astype(bf16))
                keeps.append(jnp.exp2((old - new) * e))
            for h in range(hl):
                mix[h] = mix[h] * keeps[h] + _dot(vt[h, :, here], weights[h], 1, 0)

        lax.fori_loop(0, c, lambda j, _: block(j, False), None)
        block(c, True)
        b = lax.rem(c, 2)
        for h in range(hl):
            total = mix[h, HEAD : HEAD + 1, :]
            seen[b, :, h * HEAD : (h + 1) * HEAD] = (mix[h, :HEAD, :] * (1 / total)).T.astype(bf16)

    def output(c, quarter):
        b, tiles = lax.rem(c, 2), half // WO_TILE

        def tile(n, _):
            o_wait(n)
            columns, slot = pl.ds(pl.multiple_of(n * WO_TILE, WO_TILE), WO_TILE), lax.rem(n, WO_HELD)

            pp[b, :, columns] = jnp.dot(seen[b], ob[slot], preferred_element_type=f32)

            @pl.when(n + WO_HELD < tiles)
            def _():
                o_starts(c, n + WO_HELD)

        lax.fori_loop(quarter * (tiles // 4), (quarter + 1) * (tiles // 4), tile, None)

    def compute(t, n):
        each = PARTS // PER
        c, p = lax.div(t, PER), lax.rem(t, PER) * each + n
        here = set(range(n, PARTS, each))

        def branch(parts, on, do):
            if here & set(parts):
                pl.when((t < nsub) & on)(do)

        def first():
            n = CHUNK // pieces
            for i, copy in enumerate(x_copies(c)):
                copy.wait()

                @pl.when(c == 0)
                def _():
                    w_start(i)
                    if i == pieces - 1:
                        for h in range(pieces, HELD):
                            w_start(h)
                        ext_copy().start()

                norm(i * n, (i + 1) * n)
            for copy in cs_copies(c):
                copy.wait()

        def middle_():
            @pl.when(c + 1 < nch)
            def _():
                for copy in (*x_copies(c + 1), *cs_copies(c + 1)):
                    copy.start()

            @pl.when(c >= 2)
            def _():
                seen_copy(c - 2).wait_send()
            attention(c)
            seen_copy(c).start()

        def early():
            @pl.when(c == 0)
            def _():
                ext_copy().wait_recv()

            for i in range(WO_HELD):
                o_starts(c, i)

        branch([0], p == 0, first)
        branch(range(1, 10), (p >= 1) & (p <= 3 * nt), lambda: project(c, p - 1))
        branch([EARLY], p == EARLY, early)
        branch([10], p == 10, middle_)
        branch([12], p == 12, lambda: seen_copy(c).wait_recv())
        branch(range(12, 16), p >= 12, lambda: output(c, p - 12))

    for copy in (*x_copies(0), *cs_copies(0)):
        copy.start()
    for h in range(hl):
        vt[h, HEAD:, :] = jnp.ones((8, vt.shape[2]), bf16)

    @pl.when(inner)
    def _():
        pl.semaphore_wait(barrier, 4)

    @pl.when(outer)
    def _():
        pl.semaphore_wait(barrier, 3)

    held = _held(wb, xb, d)

    def tick(t, _):
        exchange(t)
        for i, (count, copies) in enumerate(held):
            share_of = -(-count // HOLD_TICKS)

            @pl.when((t >= nsub) & (t < nsub + HOLD_TICKS))
            def _():
                def one(j, _):
                    @pl.when(j < count)
                    def _():
                        there, here = copies(j)
                        pltpu.make_async_copy(out.at[there], here, s_hold.at[i]).start()

                lax.fori_loop((t - nsub) * share_of, (t - nsub + 1) * share_of, one, None)

    lax.fori_loop(0, PER + nsub + max(AFTER.values()), tick, None)
    drain()
    for i in range(HELD):
        pltpu.make_async_copy(wq.at[pl.ds(0, k2), pl.ds(0, TILE)], held_part(i), s_hold.at[0]).wait()
    pltpu.make_async_copy(x.at[pl.ds(0, CHUNK), :], xb, s_hold.at[1]).wait()
    for c in range(max(nch - 2, 0), nch):
        seen_copy(c).wait_send()
    ext_copy().wait_send()


def _held(wb, xb, d):
    kinds, row = [], 0

    def add(count, rows, width, where):
        nonlocal row
        across, start = d // width, row

        def piece(j):
            block, at = lax.div(j, across), lax.rem(j, across)
            there = pl.ds(pl.multiple_of(start + block * rows, 16), rows), pl.ds(pl.multiple_of(at * width, 128), width)
            return there, where(block, at)

        kinds.append((count * across, piece))
        row += count * rows

    h = wb.shape[0] * TILE // d
    add(1, h, TILE, lambda block, at: wb.at[pl.ds(pl.multiple_of(at * h, 16), h), :])
    add(xb.shape[0] // 64, 64, d, lambda block, at: xb.at[pl.ds(pl.multiple_of(block * 64, 16), 64), :])
    return kinds


def _held_rows(d):
    return HELD * (d // 2 * TILE // d) + CHUNK


def layer(x, gain, wq, wk, wv, wo, cos, sin):
    rows, d = x.shape
    hl = wq.shape[1] // HEAD
    half, qa = d // 2, d // 4
    nch = rows // CHUNK
    v, dma = pltpu.VMEM, pltpu.SemaphoreType.DMA
    hbm = pl.BlockSpec(memory_space=pl.ANY)
    wa, ia, oa, ib, ob = _split(half)
    na, nb, qa, qb = ia + oa, ib + ob, max(ia, oa), max(ib, ob)

    def buffers(n, *shapes):
        return [v((n, *s), bf16) for s in shapes]

    scratch = [
        v((WO_HELD, 2 * hl * HEAD, WO_TILE), bf16), v((hl, rows, HEAD), bf16), v((hl, HEAD + 8, rows), bf16), v((hl, CHUNK, HEAD), bf16), v((2, CHUNK, 2 * hl * HEAD), bf16), v((2, CHUNK, half), f32),
        v((hl, HEAD + 8, CHUNK), f32), v((CHUNK, TILE), f32), v((hl, CHUNK), f32), v((CHUNK, HEAD), f32), v((CHUNK, HEAD), f32),
        *buffers(4, (ROWS, qa), (ROWS, qb)),
        *buffers(SLOTS, (ROWS, wa), (ROWS, na), (ROWS, qa), (ROWS, na), (SUB, nb), (SUB, qb), (SUB, nb), (ROWS, qb)),
        *buffers(SENDS, (ROWS, wa), (ROWS, na), (ROWS, qa), (SUB, nb), (SUB, qb), (ROWS, qb)),
        dma((4,)), dma((HELD,)), dma((WO_HELD, 2)), dma((2,)), dma((2, 4)), dma((8,)), dma((RS_KINDS + AG_KINDS, SENDS)), dma((RS_KINDS, SLOTS)),
        dma((AG_KINDS, MARKS)), dma((2, 2)), dma((2,)), dma((2,)),
    ]
    kept = [v((HELD * (d // 2), TILE), bf16), v((CHUNK, d), bf16), v((IMAGES, SUB, half), bf16)]
    out, _, *held = pl.pallas_call(
        functools.partial(_kernel, d=d, hl=hl, nch=nch),
        name="layer",
        in_specs=[hbm, pl.BlockSpec(memory_space=pltpu.VMEM), hbm, hbm, hbm, hbm, hbm, hbm],
        out_specs=[hbm, hbm] + [pl.BlockSpec(memory_space=pltpu.VMEM)] * len(kept),
        out_shape=[jax.ShapeDtypeStruct((rows, d), bf16), jax.ShapeDtypeStruct((hl * HEAD, half), bf16), *kept],
        scratch_shapes=scratch,
        compiler_params=pltpu.CompilerParams(collective_id=0, has_side_effects=True, vmem_limit_bytes=LAYER_VMEM),
    )(x, gain, wq, wk, wv, wo, cos, sin)
    return handed(out, *held)


def _hand(a, wb, xb, img, out, ring, s_in, s_out, s_held, *, first, last):
    d = a.shape[1]
    half, nsub, (slots, rows) = d // 2, a.shape[0] // SUB, ring.shape[:2]
    core = lax.rem(lax.axis_index("tp"), 2)
    mine, other = (pl.ds(pl.multiple_of(n * half, 128), half) for n in (core, 1 - core))
    whole = (last - first) // rows
    total = whole + (a.shape[0] - last) // rows

    def ends(i):
        at = pl.ds(first + i * rows, rows)
        return (at, ring.at[i % slots]) if i < whole else ((at, other), ring.at[i % slots, :, pl.ds(0, half)])

    def come(i):
        there, here = ends(i)
        return pltpu.make_async_copy(a.at[there], here, s_in.at[i % slots])

    def go(i):
        there, here = ends(i)
        return pltpu.make_async_copy(here, out.at[there], s_out.at[i % slots])

    kinds = _held(wb, xb, d)
    kinds.append((IMAGES, lambda j: ((pl.ds(pl.multiple_of(last + j * SUB, 16), SUB), mine), img.at[lax.rem(nsub - IMAGES + j, IMAGES)])))

    def held(n, low, high, act):
        def one(j, _):
            there, here = kinds[n][1](j)
            act(pltpu.make_async_copy(here, out.at[there], s_held.at[n]))

        lax.fori_loop(low, high, one, None)

    ahead = slots // 2
    for i in range(min(ahead, total)):
        come(i).start()
    for i in range(total):
        for n, (count, _) in enumerate(kinds):
            held(n, count * i // total, count * (i + 1) // total, lambda copy: copy.start())
        come(i).wait()
        go(i).start()
        j = i + ahead
        if j < total:
            if j >= slots:
                go(j - slots).wait()
            come(j).start()
    for i in range(max(total - slots, 0), total):
        go(i).wait()
    for n, (count, _) in enumerate(kinds):
        held(n, 0, count, lambda copy: copy.wait())


def handed(a, wb, xb, img):
    d = a.shape[1]
    first, last = _held_rows(d), a.shape[0] - IMAGES * SUB
    slots, rows = 7, 32
    dma = pltpu.SemaphoreType.DMA
    any_, vmem = pl.BlockSpec(memory_space=pl.ANY), pl.BlockSpec(memory_space=pltpu.VMEM)
    return pl.pallas_call(
        functools.partial(_hand, first=first, last=last),
        name="hand",
        in_specs=[any_] + [vmem] * 3,
        out_specs=any_,
        out_shape=jax.ShapeDtypeStruct(a.shape, a.dtype),
        scratch_shapes=[pltpu.VMEM((slots, rows, d), bf16), dma((slots,)), dma((slots,)), dma((3,))],
        compiler_params=pltpu.CompilerParams(vmem_limit_bytes=HAND_VMEM),
    )(a, wb, xb, img)


def solution(mesh):
    def step(x, gain, wq, wk, wv, wo):
        half = HEAD // 2
        angle = np.arange(x.shape[0], dtype=np.float32)[:, None] * np.float32(THETA) ** (-np.arange(half, dtype=np.float32) / half)
        cos, sin = np.cos(angle), np.sin(angle)
        cos, sin = (jnp.asarray(np.concatenate(t, -1), f32) for t in ([cos, cos], [-sin, sin]))
        return layer(x, gain, wq, wk, wv, wo, cos, sin)

    tokens, columns = P("dp", None), P(None, "tp")
    return jax.shard_map(
        step,
        mesh=mesh,
        in_specs=(tokens, P(None), columns, columns, columns, P("tp", None)),
        out_specs=tokens,
        check_vma=False,
    )
```

```python
import functools

import jax
import jax.numpy as jnp
import numpy as np
from jax import lax
from jax.experimental import pallas as pl
from jax.experimental.pallas import tpu as pltpu
from jax.sharding import PartitionSpec as P

HEAD = 128
LAYER_VMEM, HAND_VMEM = 362 * 2**20 // 10, 6 * 2**20
THETA = 10000
LOG2E = 1.4426950408889634
NEG = -1e30
CHUNK = 256
SUB = 32
PER = CHUNK // SUB
ROWS = SUB // 2
PARTS = 16
TILE = 256
HELD = 5
HOLD_TICKS = 10
WO_TILE = 512
WO_HELD = 3
EARLY = 10
SLOTS = 6
IMAGES = 14
MARKS = 16
SENDS = 3
RS_KINDS, AG_KINDS = 10, 12
A_SHARE = 7 / 12
INNER = 0.5
f32, bf16 = jnp.float32, jnp.bfloat16

STEPS = (
    ("a_i2", 2), ("a_i3", 3), ("b_i3", 3), ("a_i5", 5), ("b_o0", -1), ("b_o3", 3), ("a_s0", 0), ("b_i2", 1), ("d_w", 14),
    ("a_ox", 3), ("b_ef", 11), ("b_i4", 4), ("a_ef", 11), ("b_i6", 6), ("a_i6", 6), ("b_en", 7), ("b_o4", 4), ("H1", 0),
    ("a_o1", 1), ("a_o7", 8), ("a_o5", 5), ("a_o4", 4), ("b_i7", 7), ("b_i1", -1), ("d_s", 11), ("a_en", 8), ("b_o5", 5),
    ("a_i1", 1), ("H2", 0),
)
AFTER = dict(STEPS)


def _dot(a, b, ca, cb):
    return lax.dot_general(a, b, (((ca,), (cb,)), ((), ())), preferred_element_type=f32)


def _split(half):
    def near(share, unit, all_):
        return min(max(round(all_ * share / unit), 1), all_ // unit - 1) * unit

    wa = near(A_SHARE, 256, half)
    na, nb = wa // 2, (half - wa) // 2
    ia, ib = near(INNER, 128, na), near(INNER, 128, nb)
    return wa, ia, na - ia, ib, nb - ib


def _kernel(x, gain, wq, wk, wv, wo, cos, sin, out, wo_ext, wb, xb, img, ob, kc, vt, qb, seen, pp, mix, acc, top, cs, sn, xa_res, xb_res,
            ra0, rafar, rani, ramid, rbfar, rbni, rbmid, rbgy, sa0, safar, sani, sbfar, sbni, sbgy,
            s_x, s_w, s_o, s_cs, s_res, s_local, s_send, s_rs, s_ag, s_seen, s_ext, s_hold, *, d, hl, nch):
    half = d // 2
    wa, ia, oa, ib, ob_ = _split(half)
    na, nb = ia + oa, ib + ob_
    nt = hl * HEAD // TILE
    nsub = nch * PER
    pos = lax.axis_index("tp")
    y, z, core = lax.div(pos, 8), lax.rem(lax.div(pos, 2), 4), lax.rem(pos, 2)
    side = lax.div(z, 2)
    inner = (z == 1) | (z == 2)
    outer = (z == 0) | (z == 3)

    def at(y, z, core):
        return (y * 4 + z) * 2 + core

    partner = at(y, z, 1 - core)
    across = at(1 - y, z, core)
    middle = at(y, 3 - z, core)
    beside = at(y, 1 - z + 4 * side, core)
    col0 = core * half

    barrier = pltpu.get_barrier_semaphore()
    for dev in (partner, across, beside):
        pl.semaphore_signal(barrier, inc=1, device_id={"tp": dev})

    @pl.when(inner)
    def _():
        pl.semaphore_signal(barrier, inc=1, device_id={"tp": middle})

    pieces = 4

    def x_copies(c):
        n = CHUNK // pieces
        return [pltpu.make_async_copy(x.at[pl.ds(pl.multiple_of(c * CHUNK + i * n, n), n), :], xb.at[pl.ds(i * n, n), :], s_x.at[i])
                for i in range(pieces)]

    def cs_copies(c):
        rows = pl.ds(c * CHUNK, CHUNK)
        return pltpu.make_async_copy(cos.at[rows, :], cs, s_cs.at[0]), pltpu.make_async_copy(sin.at[rows, :], sn, s_cs.at[1])

    k2, cuts = d // 2, 2

    def held_part(slot):
        return wb.at[pl.ds(pl.multiple_of(slot * k2, k2), k2), :]

    def w_start(h):
        i, part, slot = lax.rem(lax.div(h, 2), 3 * nt), lax.rem(h, 2), lax.rem(h, HELD)
        kind, tile = lax.div(i, nt), lax.rem(i, nt)
        for n, w in enumerate((wq, wk, wv)):
            @pl.when((kind == n) & (h < nch * 3 * nt * 2))
            def _():
                for a in range(cuts):
                    rows = pl.ds(pl.multiple_of(part * k2 + a * (k2 // cuts), k2 // cuts), k2 // cuts)
                    there = pl.ds(pl.multiple_of(slot * k2 + a * (k2 // cuts), k2 // cuts), k2 // cuts)
                    pltpu.make_async_copy(w.at[rows, pl.ds(pl.multiple_of(tile * TILE, TILE), TILE)], wb.at[there, :], s_w.at[slot]).start()

    def w_wait(h):
        slot = lax.rem(h, HELD)
        pltpu.make_async_copy(wq.at[pl.ds(0, k2), pl.ds(0, TILE)], held_part(slot), s_w.at[slot]).wait()

    def tile_of(n):
        return lax.rem(n + wa // WO_TILE, half // WO_TILE)

    def o_starts(c, n):
        slot, k = lax.rem(n, WO_HELD), hl * HEAD
        own, ext = (pl.ds(pl.multiple_of(at + tile_of(n) * WO_TILE, WO_TILE), WO_TILE) for at in (col0, 0))
        pltpu.make_async_copy(wo.at[:, own], ob.at[slot, pl.ds(0, k), :], s_o.at[slot, 0]).start()
        pltpu.make_async_copy(wo_ext.at[:, ext], ob.at[slot, pl.ds(k, k), :], s_o.at[slot, 1]).start()

    def o_wait(n):
        slot, k = lax.rem(n, WO_HELD), hl * HEAD
        for i in range(2):
            pltpu.make_async_copy(wo.at[:, pl.ds(0, WO_TILE)], ob.at[slot, pl.ds(i * k, k), :], s_o.at[slot, i]).wait()

    def ext_copy():
        return pltpu.make_async_remote_copy(wo.at[:, pl.ds(pl.multiple_of((1 - core) * half, half), half)], wo_ext, s_ext.at[0], s_ext.at[1],
                                            device_id={"tp": partner})

    def seen_copy(c):
        k, b = hl * HEAD, lax.rem(c, 2)
        return pltpu.make_async_remote_copy(seen.at[b, :, pl.ds(0, k)], seen.at[b, :, pl.ds(k, k)], s_seen.at[0, b], s_seen.at[1, b],
                                            device_id={"tp": partner})

    kinds = {}

    def number(table, name):
        return kinds.setdefault((table, name), sum(t == table for t, _ in kinds))

    def rs(name, src, dst, dev, width=None):
        n = number("rs", name)

        def make(u):
            b, cut = lax.rem(u, SENDS), (slice(None), pl.ds(0, width or src.shape[2]))
            return pltpu.make_async_remote_copy(src.at[(b, *cut)], dst.at[(lax.rem(u, SLOTS), *cut)], s_send.at[n, b], s_rs.at[n, lax.rem(u, SLOTS)],
                                                device_id={"tp": dev})
        return make

    def place(row, height, col, width):
        return lambda u: (pl.ds(pl.multiple_of(u * SUB + row, 16), height), pl.ds(pl.multiple_of(col0 + col, 128), width))

    def ag(name, where, dev):
        n = number("ag", name)

        def make(u):
            there = img.at[(lax.rem(u, IMAGES), *where)]
            return pltpu.make_async_remote_copy(there, there, s_send.at[RS_KINDS + n, lax.rem(u, SENDS)], s_ag.at[n, lax.rem(u, MARKS)],
                                                device_id={"tp": dev})
        return make

    def part(row, height, col, width):
        return pl.ds(pl.multiple_of(row, 16), height), pl.ds(pl.multiple_of(col, 128), width)

    def rows_of(u):
        return out.at[pl.ds(pl.multiple_of(u * SUB, 16), SUB), pl.ds(pl.multiple_of(col0, 128), half)]

    def share(u):
        n = number("ag", "share")
        return pltpu.make_async_remote_copy(img.at[lax.rem(u, IMAGES)], rows_of(u), s_send.at[RS_KINDS + n, lax.rem(u, SENDS)],
                                            s_ag.at[n, lax.rem(u, MARKS)], device_id={"tp": partner})

    def keep(u):
        return pltpu.make_async_copy(img.at[lax.rem(u, IMAGES)], rows_of(u), s_local.at[lax.rem(u, 8)])

    def residual(n, dst, where, width):
        def make(u):
            b = lax.rem(u, 4)
            return pltpu.make_async_copy(x.at[where(u)], dst.at[b, :, pl.ds(0, width)], s_res.at[n, b])
        return make

    mine = y * ROWS
    a_near, a_far = side * na, (1 - side) * na
    b_near, b_far = wa + side * nb, wa + (1 - side) * nb
    a_in, a_out = a_near + (1 - side) * oa, a_near + side * ia
    b_in, b_out = b_near + (1 - side) * ob_, b_near + side * ib
    a_i, a_o, b_i, b_o = (pl.ds(pl.multiple_of(n, 128), w)
                          for n, w in (((1 - side) * oa, ia), (side * ia, oa), ((1 - side) * ob_, ib), (side * ib, ob_)))

    a0 = rs("a0", sa0, ra0, across)
    afar = rs("afar", safar, rafar, beside)
    ani = rs("ani", sani, rani, beside, ia)
    amid = rs("amid", safar, ramid, middle)
    arno = rs("arno", sani, rani, beside, oa)
    bfar = rs("bfar", sbfar, rbfar, beside)
    bni = rs("bni", sbni, rbni, beside, ib)
    bmid = rs("bmid", sbfar, rbmid, middle)
    brno = rs("brno", sbni, rbni, beside, ob_)
    bgy_i = rs("bgy", sbgy, rbgy, across, ib)
    bgy_o = rs("bgy", sbgy, rbgy, across, ob_)

    afo = ag("afo", part(mine, ROWS, a_in, ia), beside)
    aof = ag("aof", part(mine, ROWS, a_out, oa), beside)
    ayn = ag("ayn", part(mine, ROWS, a_near, na), across)
    ayf = ag("ayf", part(mine, ROWS, a_far, na), across)
    agm = ag("agm", part(mine, ROWS, a_near, na), middle)
    afm = ag("afm", part(mine, ROWS, a_far, na), beside)
    bfy_i = ag("bfy", part(mine, ROWS, b_in, ib), across)
    bfy_o = ag("bfy", part(mine, ROWS, b_out, ob_), across)
    bfo = ag("bfo", part(0, SUB, b_in, ib), beside)
    bof = ag("bof", part(0, SUB, b_out, ob_), beside)
    bgm = ag("bgm", part(0, SUB, b_near, nb), middle)
    bfm = ag("bfm", part(0, SUB, b_far, nb), beside)
    xa_i, xa_o = (residual(0, xa_res, place(mine, ROWS, c, w), w) for c, w in ((a_in, ia), (a_out, oa)))
    xb_i, xb_o = (residual(1, xb_res, place(mine, ROWS, c, w), w) for c, w in ((b_in, ib), (b_out, ob_)))

    def term(u, row, height, col, width):
        rows = pl.ds(pl.multiple_of(lax.rem(u, PER) * SUB + row, 16), height)
        return pp.at[lax.rem(lax.div(u, PER), 2), rows, pl.ds(pl.multiple_of(col, 128), width)]

    def final(u, col, width):
        return img.at[(lax.rem(u, IMAGES), *part(mine, ROWS, col, width))]

    def wide(ref):
        return ref[...].astype(f32)

    def put(ref, value):
        ref[...] = value.astype(bf16)

    ours, theirs = pl.ds(pl.multiple_of(y * ROWS, 16), ROWS), pl.ds(pl.multiple_of((1 - y) * ROWS, 16), ROWS)

    def a_s0(u, b, s, r):
        put(sa0.at[b], term(u, (1 - y) * ROWS, ROWS, 0, wa)[...])
        a0(u).start()

    def a_o1(u, b, s, r):
        a0(u).wait_recv()

        def part(col, width):
            return term(u, mine, ROWS, col, width)[...] + wide(ra0.at[s, :, pl.ds(pl.multiple_of(col, 128), width)])

        put(safar.at[b], part(a_far, na))
        afar(u).start()
        put(sani.at[b, :, pl.ds(0, ia)], part(a_in, ia))
        ani(u).start()
        term(u, mine, ROWS, a_out, oa)[...] = part(a_out, oa)

    def a_i1(u, b, s, r):
        a0(u).wait_recv()
        own = term(u, mine, ROWS, 0, wa)
        own[...] = own[...] + wide(ra0.at[s])

    def a_i2(u, b, s, r):
        xa_i(u).start()
        afar(u).wait_recv()
        put(safar.at[b], term(u, mine, ROWS, a_far, na)[...] + wide(rafar.at[s]))
        amid(u).start()

    def a_i3(u, b, s, r):
        amid(u).wait_recv()
        put(sani.at[b, :, pl.ds(0, oa)], term(u, mine, ROWS, a_out, oa)[...] + wide(ramid.at[s, :, a_o]))
        arno(u).start()
        ani(u).wait_recv()
        xa_i(u).wait()
        total = term(u, mine, ROWS, a_in, ia)[...] + wide(ramid.at[s, :, a_i]) + wide(rani.at[s, :, pl.ds(0, ia)])
        put(final(u, a_in, ia), wide(xa_res.at[r, :, pl.ds(0, ia)]) + total)
        afo(u).start()

    def a_ox(u, b, s, r):
        xa_o(u).start()

    def a_o4(u, b, s, r):
        arno(u).wait_recv()
        xa_o(u).wait()
        total = term(u, mine, ROWS, a_out, oa)[...] + wide(rani.at[s, :, pl.ds(0, oa)])
        put(final(u, a_out, oa), wide(xa_res.at[r, :, pl.ds(0, oa)]) + total)
        aof(u).start()

    def a_o5(u, b, s, r):
        afo(u).wait_recv()
        ayn(u).start()

    def a_i5(u, b, s, r):
        aof(u).wait_recv()
        agm(u).start()
        ayn(u).start()

    def a_i6(u, b, s, r):
        agm(u).wait_recv()
        afm(u).start()
        ayf(u).start()

    def a_o7(u, b, s, r):
        afm(u).wait_recv()
        ayf(u).start()

    def a_en(u, b, s, r):
        ayn(u).wait_recv()

    def a_ef(u, b, s, r):
        ayf(u).wait_recv()

    def b_o0(u, b, s, r):
        put(sbfar.at[b], term(u, 0, SUB, b_far, nb)[...])
        bfar(u).start()
        put(sbni.at[b, :, pl.ds(0, ib)], term(u, 0, SUB, b_in, ib)[...])
        bni(u).start()

    def b_i1(u, b, s, r):
        bfar(u).wait_recv()
        put(sbfar.at[b], term(u, 0, SUB, b_far, nb)[...] + wide(rbfar.at[s]))
        bmid(u).start()

    def b_i2(u, b, s, r):
        xb_i(u).start()
        bmid(u).wait_recv()
        put(sbni.at[b, :, pl.ds(0, ob_)], term(u, 0, SUB, b_out, ob_)[...] + wide(rbmid.at[s, :, b_o]))
        brno(u).start()
        bni(u).wait_recv()
        cut = pl.ds(0, ib)
        put(sbgy.at[b, :, cut],
            term(u, (1 - y) * ROWS, ROWS, b_in, ib)[...] + wide(rbmid.at[s, theirs, b_i]) + wide(rbni.at[s, theirs, cut]))
        bgy_i(u).start()
        own = term(u, mine, ROWS, b_in, ib)
        own[...] = own[...] + wide(rbmid.at[s, ours, b_i]) + wide(rbni.at[s, ours, cut])

    def b_o3(u, b, s, r):
        xb_o(u).start()
        brno(u).wait_recv()
        cut = pl.ds(0, ob_)
        put(sbgy.at[b, :, cut], term(u, (1 - y) * ROWS, ROWS, b_out, ob_)[...] + wide(rbni.at[s, theirs, cut]))
        bgy_o(u).start()
        own = term(u, mine, ROWS, b_out, ob_)
        own[...] = own[...] + wide(rbni.at[s, ours, cut])

    def finish_b(u, s, r, col, width, came, res, send):
        came(u).wait_recv()
        res(u).wait()
        cut = pl.ds(0, width)
        put(final(u, col, width), wide(xb_res.at[r, :, cut]) + (term(u, mine, ROWS, col, width)[...] + wide(rbgy.at[s, :, cut])))
        send(u).start()

    def b_i3(u, b, s, r):
        finish_b(u, s, r, b_in, ib, bgy_i, xb_i, bfy_i)

    def b_o4(u, b, s, r):
        finish_b(u, s, r, b_out, ob_, bgy_o, xb_o, bfy_o)

    def b_i4(u, b, s, r):
        bfy_i(u).wait_recv()
        bfo(u).start()

    def b_o5(u, b, s, r):
        bfy_o(u).wait_recv()
        bof(u).start()

    def b_i6(u, b, s, r):
        bof(u).wait_recv()
        bgm(u).start()

    def b_i7(u, b, s, r):
        bgm(u).wait_recv()
        bfm(u).start()

    def b_en(u, b, s, r):
        bfo(u).wait_recv()

    def b_ef(u, b, s, r):
        bfm(u).wait_recv()

    def d_s(u, b, s, r):
        share(u).start()

        @pl.when(u < nsub - IMAGES)
        def _():
            keep(u).start()

    def d_w(u, b, s, r):
        share(u).wait_recv()

        @pl.when(u < nsub - IMAGES)
        def _():
            keep(u).wait()

    steps = {
        "a_s0": (a_s0, [a0]), "a_o1": (a_o1, [afar, ani]), "a_i1": (a_i1, []), "a_i2": (a_i2, [amid]), "a_i3": (a_i3, [arno, afo]),
        "a_ox": (a_ox, []), "a_o4": (a_o4, [aof]), "a_o5": (a_o5, [ayn]), "a_i5": (a_i5, [agm, ayn]), "a_i6": (a_i6, [afm, ayf]),
        "a_o7": (a_o7, [ayf]), "a_en": (a_en, []), "a_ef": (a_ef, []), "b_o0": (b_o0, [bfar, bni]), "b_i1": (b_i1, [bmid]),
        "b_i2": (b_i2, [brno, bgy_i]), "b_o3": (b_o3, [bgy_o]), "b_i3": (b_i3, [bfy_i]), "b_o4": (b_o4, [bfy_o]), "b_i4": (b_i4, [bfo]),
        "b_o5": (b_o5, [bof]), "b_i6": (b_i6, [bgm]), "b_i7": (b_i7, [bfm]), "b_en": (b_en, []), "b_ef": (b_ef, []),
        "d_s": (d_s, [share]), "d_w": (d_w, []),
    }

    def role(name):
        return {"i": inner, "o": outer}.get(name[2]) if name not in ("b_en", "b_ef") else outer

    def exchange(t):
        n = 0
        for name, after in STEPS:
            if name[0] == "H":
                compute(t, n)
                n += 1
                continue
            do, sends = steps[name]
            u = t - PER - after
            go = (u >= 0) & (u < nsub)
            if role(name) is not None:
                go = go & role(name)

            @pl.when(go)
            def _():
                if sends:
                    @pl.when(u >= SENDS)
                    def _():
                        for m in sends:
                            m(u - SENDS).wait_send()
                do(u, lax.rem(u, SENDS), lax.rem(u, SLOTS), lax.rem(u, 4))

    def drain():
        for name in steps:
            def leave(sends=steps[name][1]):
                for m in sends:
                    for u in range(max(nsub - SENDS, 0), nsub):
                        m(u).wait_send()
            if role(name) is None:
                leave()
            elif steps[name][1]:
                pl.when(role(name))(leave)

    lanes = 1024

    def norm(first, last):
        def rows(i, _):
            r = pl.ds(pl.multiple_of(i * 16, 16), 16)
            acc = jnp.zeros((16, lanes), f32)
            for j in range(0, d, lanes):
                v = xb[r, j : j + lanes].astype(f32)
                acc = acc + v * v
            scale = lax.rsqrt(jnp.sum(acc, axis=-1, keepdims=True) * (1.0 / d) + 1e-6)
            for j in range(0, d, lanes):
                v = xb[r, j : j + lanes].astype(f32)
                xb[r, j : j + lanes] = (v * scale * gain[pl.ds(j, lanes)].astype(f32)[None]).astype(bf16)

        lax.fori_loop(first // 16, last // 16, rows, None)

    def project(c, i):
        g, kind, j = c * 3 * nt + i, lax.div(i, nt), lax.rem(i, nt)

        def part(p, _):
            w_wait(2 * g + p)
            columns = pl.ds(pl.multiple_of(p * k2, 128), k2)
            one = jnp.dot(xb[:, columns], held_part(lax.rem(2 * g + p, HELD))[...], preferred_element_type=f32)
            w_start(2 * g + p + HELD)

            @pl.when(p == 0)
            def _():
                acc[...] = one

            @pl.when(p == 1)
            def _():
                acc[...] = acc[...] + one

        lax.fori_loop(0, 2, part, None)
        r = acc[...].astype(bf16)
        tokens = pl.ds(pl.multiple_of(c * CHUNK, CHUNK), CHUNK)
        for n in range(TILE // HEAD):
            h = j * (TILE // HEAD) + n
            one = r[:, n * HEAD : (n + 1) * HEAD]

            @pl.when(kind < 2)
            def _():
                w = one.astype(f32)
                w = (w * cs[...] + pltpu.roll(w, HEAD // 2, 1) * sn[...]).astype(bf16)

                @pl.when(kind == 0)
                def _():
                    qb[h] = w

                @pl.when(kind == 1)
                def _():
                    kc[h, tokens, :] = w

            @pl.when(kind == 2)
            def _():
                vt[h, pl.ds(0, HEAD), tokens] = one.T

    e = HEAD**-0.5 * LOG2E

    def attention(c):
        top[...] = jnp.full(top.shape, NEG, f32)
        mix[...] = jnp.zeros(mix.shape, f32)

        def block(j, masked):
            here = pl.ds(pl.multiple_of(j * CHUNK, CHUNK), CHUNK)
            scores = [_dot(kc[h, here, :], qb[h], 1, 1) for h in range(hl)]
            if masked:
                ok = lax.broadcasted_iota(jnp.int32, (CHUNK, CHUNK), 1) >= lax.broadcasted_iota(jnp.int32, (CHUNK, CHUNK), 0)
            weights, keeps = [], []
            for h, s in enumerate(scores):
                if masked:
                    s = jnp.where(ok, s, 2 * NEG)
                old = top[h : h + 1, :]
                new = jnp.maximum(old, s.max(axis=0, keepdims=True))
                top[h : h + 1, :] = new
                weights.append(jnp.exp2((s - new) * e).astype(bf16))
                keeps.append(jnp.exp2((old - new) * e))
            for h in range(hl):
                mix[h] = mix[h] * keeps[h] + _dot(vt[h, :, here], weights[h], 1, 0)

        lax.fori_loop(0, c, lambda j, _: block(j, False), None)
        block(c, True)
        b = lax.rem(c, 2)
        for h in range(hl):
            total = mix[h, HEAD : HEAD + 1, :]
            seen[b, :, h * HEAD : (h + 1) * HEAD] = (mix[h, :HEAD, :] * (1 / total)).T.astype(bf16)

    def output(c, quarter):
        b, tiles = lax.rem(c, 2), half // WO_TILE

        def tile(n, _):
            o_wait(n)
            columns, slot = pl.ds(pl.multiple_of(tile_of(n) * WO_TILE, WO_TILE), WO_TILE), lax.rem(n, WO_HELD)

            pp[b, :, columns] = jnp.dot(seen[b], ob[slot], preferred_element_type=f32)

            @pl.when(n + WO_HELD < tiles)
            def _():
                o_starts(c, n + WO_HELD)

        lax.fori_loop(quarter * (tiles // 4), (quarter + 1) * (tiles // 4), tile, None)

    def compute(t, n):
        each = PARTS // PER
        c, p = lax.div(t, PER), lax.rem(t, PER) * each + n
        here = set(range(n, PARTS, each))

        def branch(parts, on, do):
            if here & set(parts):
                pl.when((t < nsub) & on)(do)

        def first():
            for copy in (*x_copies(c), *cs_copies(c)):
                copy.wait()
            norm(0, CHUNK)

        def middle_():
            @pl.when(c + 1 < nch)
            def _():
                for copy in (*x_copies(c + 1), *cs_copies(c + 1)):
                    copy.start()

            @pl.when(c >= 2)
            def _():
                seen_copy(c - 2).wait_send()
            attention(c)
            seen_copy(c).start()

        def early():
            @pl.when(c == 0)
            def _():
                ext_copy().wait_recv()

            for i in range(WO_HELD):
                o_starts(c, i)

        branch([0], (p == 0) & (c > 0), first)
        branch(range(1, 10), (p >= 1) & (p <= 3 * nt), lambda: project(c, p - 1))
        branch([EARLY], p == EARLY, early)
        branch([10], p == 10, middle_)
        branch([12], p == 12, lambda: seen_copy(c).wait_recv())
        branch(range(12, 16), p >= 12, lambda: output(c, p - 12))

    for copy in (*x_copies(0), *cs_copies(0)):
        copy.start()
    for h in range(hl):
        vt[h, HEAD:, :] = jnp.ones((8, vt.shape[2]), bf16)

    for i, copy in enumerate(x_copies(0)):
        copy.wait()
        w_start(i)
        norm(i * (CHUNK // pieces), (i + 1) * (CHUNK // pieces))
    for h in range(pieces, HELD):
        w_start(h)
    for copy in cs_copies(0):
        copy.wait()

    @pl.when(inner)
    def _():
        pl.semaphore_wait(barrier, 4)

    @pl.when(outer)
    def _():
        pl.semaphore_wait(barrier, 3)

    ext_copy().start()

    held = _held(wb, xb, d)

    def tick(t, _):
        exchange(t)
        for i, (count, copies) in enumerate(held):
            share_of = -(-count // HOLD_TICKS)

            @pl.when((t >= nsub) & (t < nsub + HOLD_TICKS))
            def _():
                def one(j, _):
                    @pl.when(j < count)
                    def _():
                        there, here = copies(j)
                        pltpu.make_async_copy(out.at[there], here, s_hold.at[i]).start()

                lax.fori_loop((t - nsub) * share_of, (t - nsub + 1) * share_of, one, None)

    lax.fori_loop(0, PER + nsub + max(AFTER.values()), tick, None)
    drain()
    for i in range(HELD):
        pltpu.make_async_copy(wq.at[pl.ds(0, k2), pl.ds(0, TILE)], held_part(i), s_hold.at[0]).wait()
    pltpu.make_async_copy(x.at[pl.ds(0, CHUNK), :], xb, s_hold.at[1]).wait()
    for c in range(max(nch - 2, 0), nch):
        seen_copy(c).wait_send()
    ext_copy().wait_send()


def _held(wb, xb, d):
    kinds, row = [], 0

    def add(count, rows, width, where):
        nonlocal row
        across, start = d // width, row

        def piece(j):
            block, at = lax.div(j, across), lax.rem(j, across)
            there = pl.ds(pl.multiple_of(start + block * rows, 16), rows), pl.ds(pl.multiple_of(at * width, 128), width)
            return there, where(block, at)

        kinds.append((count * across, piece))
        row += count * rows

    h = wb.shape[0] * TILE // d
    add(1, h, TILE, lambda block, at: wb.at[pl.ds(pl.multiple_of(at * h, 16), h), :])
    add(xb.shape[0] // 64, 64, d, lambda block, at: xb.at[pl.ds(pl.multiple_of(block * 64, 16), 64), :])
    return kinds


def _held_rows(d):
    return HELD * (d // 2 * TILE // d) + CHUNK


def layer(x, gain, wq, wk, wv, wo, cos, sin):
    rows, d = x.shape
    hl = wq.shape[1] // HEAD
    half, qa = d // 2, d // 4
    nch = rows // CHUNK
    v, dma = pltpu.VMEM, pltpu.SemaphoreType.DMA
    hbm = pl.BlockSpec(memory_space=pl.ANY)
    wa, ia, oa, ib, ob = _split(half)
    na, nb, qa, qb = ia + oa, ib + ob, max(ia, oa), max(ib, ob)

    def buffers(n, *shapes):
        return [v((n, *s), bf16) for s in shapes]

    scratch = [
        v((WO_HELD, 2 * hl * HEAD, WO_TILE), bf16), v((hl, rows, HEAD), bf16), v((hl, HEAD + 8, rows), bf16), v((hl, CHUNK, HEAD), bf16), v((2, CHUNK, 2 * hl * HEAD), bf16), v((2, CHUNK, half), f32),
        v((hl, HEAD + 8, CHUNK), f32), v((CHUNK, TILE), f32), v((hl, CHUNK), f32), v((CHUNK, HEAD), f32), v((CHUNK, HEAD), f32),
        *buffers(4, (ROWS, qa), (ROWS, qb)),
        *buffers(SLOTS, (ROWS, wa), (ROWS, na), (ROWS, qa), (ROWS, na), (SUB, nb), (SUB, qb), (SUB, nb), (ROWS, qb)),
        *buffers(SENDS, (ROWS, wa), (ROWS, na), (ROWS, qa), (SUB, nb), (SUB, qb), (ROWS, qb)),
        dma((4,)), dma((HELD,)), dma((WO_HELD, 2)), dma((2,)), dma((2, 4)), dma((8,)), dma((RS_KINDS + AG_KINDS, SENDS)), dma((RS_KINDS, SLOTS)),
        dma((AG_KINDS, MARKS)), dma((2, 2)), dma((2,)), dma((2,)),
    ]
    kept = [v((HELD * (d // 2), TILE), bf16), v((CHUNK, d), bf16), v((IMAGES, SUB, half), bf16)]
    out, _, *held = pl.pallas_call(
        functools.partial(_kernel, d=d, hl=hl, nch=nch),
        name="layer",
        in_specs=[hbm, pl.BlockSpec(memory_space=pltpu.VMEM), hbm, hbm, hbm, hbm, hbm, hbm],
        out_specs=[hbm, hbm] + [pl.BlockSpec(memory_space=pltpu.VMEM)] * len(kept),
        out_shape=[jax.ShapeDtypeStruct((rows, d), bf16), jax.ShapeDtypeStruct((hl * HEAD, half), bf16), *kept],
        scratch_shapes=scratch,
        compiler_params=pltpu.CompilerParams(collective_id=0, has_side_effects=True, vmem_limit_bytes=LAYER_VMEM),
    )(x, gain, wq, wk, wv, wo, cos, sin)
    return handed(out, *held)


def _hand(a, wb, xb, img, out, ring, s_in, s_out, s_held, *, first, last):
    d = a.shape[1]
    half, nsub, (slots, rows) = d // 2, a.shape[0] // SUB, ring.shape[:2]
    core = lax.rem(lax.axis_index("tp"), 2)
    mine, other = (pl.ds(pl.multiple_of(n * half, 128), half) for n in (core, 1 - core))
    whole = (last - first) // rows
    total = whole + (a.shape[0] - last) // rows

    def ends(i):
        at = pl.ds(first + i * rows, rows)
        return (at, ring.at[i % slots]) if i < whole else ((at, other), ring.at[i % slots, :, pl.ds(0, half)])

    def come(i):
        there, here = ends(i)
        return pltpu.make_async_copy(a.at[there], here, s_in.at[i % slots])

    def go(i):
        there, here = ends(i)
        return pltpu.make_async_copy(here, out.at[there], s_out.at[i % slots])

    kinds = _held(wb, xb, d)
    kinds.append((IMAGES, lambda j: ((pl.ds(pl.multiple_of(last + j * SUB, 16), SUB), mine), img.at[lax.rem(nsub - IMAGES + j, IMAGES)])))

    def held(n, low, high, act):
        def one(j, _):
            there, here = kinds[n][1](j)
            act(pltpu.make_async_copy(here, out.at[there], s_held.at[n]))

        lax.fori_loop(low, high, one, None)

    ahead = slots // 2
    for i in range(min(ahead, total)):
        come(i).start()
    for i in range(total):
        for n, (count, _) in enumerate(kinds):
            held(n, count * i // total, count * (i + 1) // total, lambda copy: copy.start())
        come(i).wait()
        go(i).start()
        j = i + ahead
        if j < total:
            if j >= slots:
                go(j - slots).wait()
            come(j).start()
    for i in range(max(total - slots, 0), total):
        go(i).wait()
    for n, (count, _) in enumerate(kinds):
        held(n, 0, count, lambda copy: copy.wait())


def handed(a, wb, xb, img):
    d = a.shape[1]
    first, last = _held_rows(d), a.shape[0] - IMAGES * SUB
    slots, rows = 7, 32
    dma = pltpu.SemaphoreType.DMA
    any_, vmem = pl.BlockSpec(memory_space=pl.ANY), pl.BlockSpec(memory_space=pltpu.VMEM)
    return pl.pallas_call(
        functools.partial(_hand, first=first, last=last),
        name="hand",
        in_specs=[any_] + [vmem] * 3,
        out_specs=any_,
        out_shape=jax.ShapeDtypeStruct(a.shape, a.dtype),
        scratch_shapes=[pltpu.VMEM((slots, rows, d), bf16), dma((slots,)), dma((slots,)), dma((3,))],
        compiler_params=pltpu.CompilerParams(vmem_limit_bytes=HAND_VMEM),
    )(a, wb, xb, img)


def solution(mesh):
    def step(x, gain, wq, wk, wv, wo):
        half = HEAD // 2
        angle = np.arange(x.shape[0], dtype=np.float32)[:, None] * np.float32(THETA) ** (-np.arange(half, dtype=np.float32) / half)
        cos, sin = np.cos(angle), np.sin(angle)
        cos, sin = (jnp.asarray(np.concatenate(t, -1), f32) for t in ([cos, cos], [-sin, sin]))
        return layer(x, gain, wq, wk, wv, wo, cos, sin)

    tokens, columns = P("dp", None), P(None, "tp")
    return jax.shard_map(
        step,
        mesh=mesh,
        in_specs=(tokens, P(None), columns, columns, columns, P("tp", None)),
        out_specs=tokens,
        check_vma=False,
    )
```

```python
import functools

import jax
import jax.numpy as jnp
import numpy as np
from jax import lax
from jax.experimental import pallas as pl
from jax.experimental.pallas import tpu as pltpu
from jax.sharding import PartitionSpec as P

HEAD = 128
LAYER_VMEM, HAND_VMEM = 362 * 2**20 // 10, 9 * 2**20
THETA = 10000
LOG2E = 1.4426950408889634
NEG = -1e30
CHUNK = 256
SUB = 32
PER = CHUNK // SUB
ROWS = SUB // 2
PARTS = 16
TILE = 256
HELD = 5
HOLD_TICKS = 10
WO_TILE = 512
WO_HELD = 3
EARLY = 10
SLOTS = 6
IMAGES = 14
MARKS = 16
SENDS = 3
RS_KINDS, AG_KINDS = 10, 12
A_SHARE = 7 / 12
INNER = 0.5
f32, bf16 = jnp.float32, jnp.bfloat16

STEPS = (
    ("a_i2", 2), ("a_i3", 3), ("b_i3", 3), ("a_i5", 5), ("b_o0", -1), ("b_o3", 3), ("a_s0", 0), ("b_i2", 1), ("d_w", 14),
    ("a_ox", 3), ("b_ef", 11), ("b_i4", 4), ("a_ef", 11), ("b_i6", 6), ("a_i6", 6), ("b_en", 7), ("b_o4", 4), ("H1", 0),
    ("a_o1", 1), ("a_o7", 8), ("a_o5", 5), ("a_o4", 4), ("b_i7", 7), ("b_i1", -1), ("d_s", 11), ("a_en", 8), ("b_o5", 5),
    ("a_i1", 1), ("H2", 0),
)
AFTER = dict(STEPS)


def _dot(a, b, ca, cb):
    return lax.dot_general(a, b, (((ca,), (cb,)), ((), ())), preferred_element_type=f32)


def _split(half):
    def near(share, unit, all_):
        return min(max(round(all_ * share / unit), 1), all_ // unit - 1) * unit

    wa = near(A_SHARE, 256, half)
    na, nb = wa // 2, (half - wa) // 2
    ia, ib = near(INNER, 128, na), near(INNER, 128, nb)
    return wa, ia, na - ia, ib, nb - ib


def _kernel(x, gain, wq, wk, wv, wo, cos, sin, out, wo_ext, wb, xb, img, ob, kc, vt, qb, seen, pp, mix, acc, top, cs, sn, xa_res, xb_res,
            ra0, rafar, rani, ramid, rbfar, rbni, rbmid, rbgy, sa0, safar, sani, sbfar, sbni, sbgy,
            s_x, s_w, s_o, s_cs, s_res, s_local, s_send, s_rs, s_ag, s_seen, s_ext, s_hold, *, d, hl, nch):
    half = d // 2
    wa, ia, oa, ib, ob_ = _split(half)
    na, nb = ia + oa, ib + ob_
    nt = hl * HEAD // TILE
    nsub = nch * PER
    pos = lax.axis_index("tp")
    y, z, core = lax.div(pos, 8), lax.rem(lax.div(pos, 2), 4), lax.rem(pos, 2)
    side = lax.div(z, 2)
    inner = (z == 1) | (z == 2)
    outer = (z == 0) | (z == 3)

    def at(y, z, core):
        return (y * 4 + z) * 2 + core

    partner = at(y, z, 1 - core)
    across = at(1 - y, z, core)
    middle = at(y, 3 - z, core)
    beside = at(y, 1 - z + 4 * side, core)
    col0 = core * half

    barrier = pltpu.get_barrier_semaphore()
    for dev in (partner, across, beside):
        pl.semaphore_signal(barrier, inc=1, device_id={"tp": dev})

    @pl.when(inner)
    def _():
        pl.semaphore_signal(barrier, inc=1, device_id={"tp": middle})

    pieces = 4

    def x_copies(c):
        n = CHUNK // pieces
        return [pltpu.make_async_copy(x.at[pl.ds(pl.multiple_of(c * CHUNK + i * n, n), n), :], xb.at[pl.ds(i * n, n), :], s_x.at[i])
                for i in range(pieces)]

    def cs_copies(c):
        rows = pl.ds(c * CHUNK, CHUNK)
        return pltpu.make_async_copy(cos.at[rows, :], cs, s_cs.at[0]), pltpu.make_async_copy(sin.at[rows, :], sn, s_cs.at[1])

    k2, cuts = d // 2, 2

    def held_part(slot):
        return wb.at[pl.ds(pl.multiple_of(slot * k2, k2), k2), :]

    def w_start(h):
        i, part, slot = lax.rem(lax.div(h, 2), 3 * nt), lax.rem(h, 2), lax.rem(h, HELD)
        kind, tile = lax.div(i, nt), lax.rem(i, nt)
        for n, w in enumerate((wq, wk, wv)):
            @pl.when((kind == n) & (h < nch * 3 * nt * 2))
            def _():
                for a in range(cuts):
                    rows = pl.ds(pl.multiple_of(part * k2 + a * (k2 // cuts), k2 // cuts), k2 // cuts)
                    there = pl.ds(pl.multiple_of(slot * k2 + a * (k2 // cuts), k2 // cuts), k2 // cuts)
                    pltpu.make_async_copy(w.at[rows, pl.ds(pl.multiple_of(tile * TILE, TILE), TILE)], wb.at[there, :], s_w.at[slot]).start()

    def w_wait(h):
        slot = lax.rem(h, HELD)
        pltpu.make_async_copy(wq.at[pl.ds(0, k2), pl.ds(0, TILE)], held_part(slot), s_w.at[slot]).wait()

    def tile_of(n):
        return lax.rem(n + wa // WO_TILE, half // WO_TILE)

    def o_starts(c, n):
        slot, k = lax.rem(n, WO_HELD), hl * HEAD
        own, ext = (pl.ds(pl.multiple_of(at + tile_of(n) * WO_TILE, WO_TILE), WO_TILE) for at in (col0, 0))
        pltpu.make_async_copy(wo.at[:, own], ob.at[slot, pl.ds(0, k), :], s_o.at[slot, 0]).start()
        pltpu.make_async_copy(wo_ext.at[:, ext], ob.at[slot, pl.ds(k, k), :], s_o.at[slot, 1]).start()

    def o_wait(n):
        slot, k = lax.rem(n, WO_HELD), hl * HEAD
        for i in range(2):
            pltpu.make_async_copy(wo.at[:, pl.ds(0, WO_TILE)], ob.at[slot, pl.ds(i * k, k), :], s_o.at[slot, i]).wait()

    def ext_copy():
        return pltpu.make_async_remote_copy(wo.at[:, pl.ds(pl.multiple_of((1 - core) * half, half), half)], wo_ext, s_ext.at[0], s_ext.at[1],
                                            device_id={"tp": partner})

    def seen_copy(c):
        k, b = hl * HEAD, lax.rem(c, 2)
        return pltpu.make_async_remote_copy(seen.at[b, :, pl.ds(0, k)], seen.at[b, :, pl.ds(k, k)], s_seen.at[0, b], s_seen.at[1, b],
                                            device_id={"tp": partner})

    kinds = {}

    def number(table, name):
        return kinds.setdefault((table, name), sum(t == table for t, _ in kinds))

    def rs(name, src, dst, dev, width=None):
        n = number("rs", name)

        def make(u):
            b, cut = lax.rem(u, SENDS), (slice(None), pl.ds(0, width or src.shape[2]))
            return pltpu.make_async_remote_copy(src.at[(b, *cut)], dst.at[(lax.rem(u, SLOTS), *cut)], s_send.at[n, b], s_rs.at[n, lax.rem(u, SLOTS)],
                                                device_id={"tp": dev})
        return make

    def place(row, height, col, width):
        return lambda u: (pl.ds(pl.multiple_of(u * SUB + row, 16), height), pl.ds(pl.multiple_of(col0 + col, 128), width))

    def ag(name, where, dev):
        n = number("ag", name)

        def make(u):
            there = img.at[(lax.rem(u, IMAGES), *where)]
            return pltpu.make_async_remote_copy(there, there, s_send.at[RS_KINDS + n, lax.rem(u, SENDS)], s_ag.at[n, lax.rem(u, MARKS)],
                                                device_id={"tp": dev})
        return make

    def part(row, height, col, width):
        return pl.ds(pl.multiple_of(row, 16), height), pl.ds(pl.multiple_of(col, 128), width)

    def rows_of(u):
        return out.at[pl.ds(pl.multiple_of(u * SUB, 16), SUB), pl.ds(pl.multiple_of(col0, 128), half)]

    def share(u):
        n = number("ag", "share")
        return pltpu.make_async_remote_copy(img.at[lax.rem(u, IMAGES)], rows_of(u), s_send.at[RS_KINDS + n, lax.rem(u, SENDS)],
                                            s_ag.at[n, lax.rem(u, MARKS)], device_id={"tp": partner})

    def keep(u):
        return pltpu.make_async_copy(img.at[lax.rem(u, IMAGES)], rows_of(u), s_local.at[lax.rem(u, 8)])

    def residual(n, dst, where, width):
        def make(u):
            b = lax.rem(u, 4)
            return pltpu.make_async_copy(x.at[where(u)], dst.at[b, :, pl.ds(0, width)], s_res.at[n, b])
        return make

    mine = y * ROWS
    a_near, a_far = side * na, (1 - side) * na
    b_near, b_far = wa + side * nb, wa + (1 - side) * nb
    a_in, a_out = a_near + (1 - side) * oa, a_near + side * ia
    b_in, b_out = b_near + (1 - side) * ob_, b_near + side * ib
    a_i, a_o, b_i, b_o = (pl.ds(pl.multiple_of(n, 128), w)
                          for n, w in (((1 - side) * oa, ia), (side * ia, oa), ((1 - side) * ob_, ib), (side * ib, ob_)))

    a0 = rs("a0", sa0, ra0, across)
    afar = rs("afar", safar, rafar, beside)
    ani = rs("ani", sani, rani, beside, ia)
    amid = rs("amid", safar, ramid, middle)
    arno = rs("arno", sani, rani, beside, oa)
    bfar = rs("bfar", sbfar, rbfar, beside)
    bni = rs("bni", sbni, rbni, beside, ib)
    bmid = rs("bmid", sbfar, rbmid, middle)
    brno = rs("brno", sbni, rbni, beside, ob_)
    bgy_i = rs("bgy", sbgy, rbgy, across, ib)
    bgy_o = rs("bgy", sbgy, rbgy, across, ob_)

    afo = ag("afo", part(mine, ROWS, a_in, ia), beside)
    aof = ag("aof", part(mine, ROWS, a_out, oa), beside)
    ayn = ag("ayn", part(mine, ROWS, a_near, na), across)
    ayf = ag("ayf", part(mine, ROWS, a_far, na), across)
    agm = ag("agm", part(mine, ROWS, a_near, na), middle)
    afm = ag("afm", part(mine, ROWS, a_far, na), beside)
    bfy_i = ag("bfy", part(mine, ROWS, b_in, ib), across)
    bfy_o = ag("bfy", part(mine, ROWS, b_out, ob_), across)
    bfo = ag("bfo", part(0, SUB, b_in, ib), beside)
    bof = ag("bof", part(0, SUB, b_out, ob_), beside)
    bgm = ag("bgm", part(0, SUB, b_near, nb), middle)
    bfm = ag("bfm", part(0, SUB, b_far, nb), beside)
    xa_i, xa_o = (residual(0, xa_res, place(mine, ROWS, c, w), w) for c, w in ((a_in, ia), (a_out, oa)))
    xb_i, xb_o = (residual(1, xb_res, place(mine, ROWS, c, w), w) for c, w in ((b_in, ib), (b_out, ob_)))

    def term(u, row, height, col, width):
        rows = pl.ds(pl.multiple_of(lax.rem(u, PER) * SUB + row, 16), height)
        return pp.at[lax.rem(lax.div(u, PER), 2), rows, pl.ds(pl.multiple_of(col, 128), width)]

    def final(u, col, width):
        return img.at[(lax.rem(u, IMAGES), *part(mine, ROWS, col, width))]

    def wide(ref):
        return ref[...].astype(f32)

    def put(ref, value):
        ref[...] = value.astype(bf16)

    ours, theirs = pl.ds(pl.multiple_of(y * ROWS, 16), ROWS), pl.ds(pl.multiple_of((1 - y) * ROWS, 16), ROWS)

    def a_s0(u, b, s, r):
        put(sa0.at[b], term(u, (1 - y) * ROWS, ROWS, 0, wa)[...])
        a0(u).start()

    def a_o1(u, b, s, r):
        a0(u).wait_recv()

        def part(col, width):
            return term(u, mine, ROWS, col, width)[...] + wide(ra0.at[s, :, pl.ds(pl.multiple_of(col, 128), width)])

        put(safar.at[b], part(a_far, na))
        afar(u).start()
        put(sani.at[b, :, pl.ds(0, ia)], part(a_in, ia))
        ani(u).start()
        term(u, mine, ROWS, a_out, oa)[...] = part(a_out, oa)

    def a_i1(u, b, s, r):
        a0(u).wait_recv()
        own = term(u, mine, ROWS, 0, wa)
        own[...] = own[...] + wide(ra0.at[s])

    def a_i2(u, b, s, r):
        xa_i(u).start()
        afar(u).wait_recv()
        put(safar.at[b], term(u, mine, ROWS, a_far, na)[...] + wide(rafar.at[s]))
        amid(u).start()

    def a_i3(u, b, s, r):
        amid(u).wait_recv()
        put(sani.at[b, :, pl.ds(0, oa)], term(u, mine, ROWS, a_out, oa)[...] + wide(ramid.at[s, :, a_o]))
        arno(u).start()
        ani(u).wait_recv()
        xa_i(u).wait()
        total = term(u, mine, ROWS, a_in, ia)[...] + wide(ramid.at[s, :, a_i]) + wide(rani.at[s, :, pl.ds(0, ia)])
        put(final(u, a_in, ia), wide(xa_res.at[r, :, pl.ds(0, ia)]) + total)
        afo(u).start()

    def a_ox(u, b, s, r):
        xa_o(u).start()

    def a_o4(u, b, s, r):
        arno(u).wait_recv()
        xa_o(u).wait()
        total = term(u, mine, ROWS, a_out, oa)[...] + wide(rani.at[s, :, pl.ds(0, oa)])
        put(final(u, a_out, oa), wide(xa_res.at[r, :, pl.ds(0, oa)]) + total)
        aof(u).start()

    def a_o5(u, b, s, r):
        afo(u).wait_recv()
        ayn(u).start()

    def a_i5(u, b, s, r):
        aof(u).wait_recv()
        agm(u).start()
        ayn(u).start()

    def a_i6(u, b, s, r):
        agm(u).wait_recv()
        afm(u).start()
        ayf(u).start()

    def a_o7(u, b, s, r):
        afm(u).wait_recv()
        ayf(u).start()

    def a_en(u, b, s, r):
        ayn(u).wait_recv()

    def a_ef(u, b, s, r):
        ayf(u).wait_recv()

    def b_o0(u, b, s, r):
        put(sbfar.at[b], term(u, 0, SUB, b_far, nb)[...])
        bfar(u).start()
        put(sbni.at[b, :, pl.ds(0, ib)], term(u, 0, SUB, b_in, ib)[...])
        bni(u).start()

    def b_i1(u, b, s, r):
        bfar(u).wait_recv()
        put(sbfar.at[b], term(u, 0, SUB, b_far, nb)[...] + wide(rbfar.at[s]))
        bmid(u).start()

    def b_i2(u, b, s, r):
        xb_i(u).start()
        bmid(u).wait_recv()
        put(sbni.at[b, :, pl.ds(0, ob_)], term(u, 0, SUB, b_out, ob_)[...] + wide(rbmid.at[s, :, b_o]))
        brno(u).start()
        bni(u).wait_recv()
        cut = pl.ds(0, ib)
        put(sbgy.at[b, :, cut],
            term(u, (1 - y) * ROWS, ROWS, b_in, ib)[...] + wide(rbmid.at[s, theirs, b_i]) + wide(rbni.at[s, theirs, cut]))
        bgy_i(u).start()
        own = term(u, mine, ROWS, b_in, ib)
        own[...] = own[...] + wide(rbmid.at[s, ours, b_i]) + wide(rbni.at[s, ours, cut])

    def b_o3(u, b, s, r):
        xb_o(u).start()
        brno(u).wait_recv()
        cut = pl.ds(0, ob_)
        put(sbgy.at[b, :, cut], term(u, (1 - y) * ROWS, ROWS, b_out, ob_)[...] + wide(rbni.at[s, theirs, cut]))
        bgy_o(u).start()
        own = term(u, mine, ROWS, b_out, ob_)
        own[...] = own[...] + wide(rbni.at[s, ours, cut])

    def finish_b(u, s, r, col, width, came, res, send):
        came(u).wait_recv()
        res(u).wait()
        cut = pl.ds(0, width)
        put(final(u, col, width), wide(xb_res.at[r, :, cut]) + (term(u, mine, ROWS, col, width)[...] + wide(rbgy.at[s, :, cut])))
        send(u).start()

    def b_i3(u, b, s, r):
        finish_b(u, s, r, b_in, ib, bgy_i, xb_i, bfy_i)

    def b_o4(u, b, s, r):
        finish_b(u, s, r, b_out, ob_, bgy_o, xb_o, bfy_o)

    def b_i4(u, b, s, r):
        bfy_i(u).wait_recv()
        bfo(u).start()

    def b_o5(u, b, s, r):
        bfy_o(u).wait_recv()
        bof(u).start()

    def b_i6(u, b, s, r):
        bof(u).wait_recv()
        bgm(u).start()

    def b_i7(u, b, s, r):
        bgm(u).wait_recv()
        bfm(u).start()

    def b_en(u, b, s, r):
        bfo(u).wait_recv()

    def b_ef(u, b, s, r):
        bfm(u).wait_recv()

    def d_s(u, b, s, r):
        share(u).start()

        @pl.when(u < nsub - IMAGES)
        def _():
            keep(u).start()

    def d_w(u, b, s, r):
        share(u).wait_recv()

        @pl.when(u < nsub - IMAGES)
        def _():
            keep(u).wait()

    steps = {
        "a_s0": (a_s0, [a0]), "a_o1": (a_o1, [afar, ani]), "a_i1": (a_i1, []), "a_i2": (a_i2, [amid]), "a_i3": (a_i3, [arno, afo]),
        "a_ox": (a_ox, []), "a_o4": (a_o4, [aof]), "a_o5": (a_o5, [ayn]), "a_i5": (a_i5, [agm, ayn]), "a_i6": (a_i6, [afm, ayf]),
        "a_o7": (a_o7, [ayf]), "a_en": (a_en, []), "a_ef": (a_ef, []), "b_o0": (b_o0, [bfar, bni]), "b_i1": (b_i1, [bmid]),
        "b_i2": (b_i2, [brno, bgy_i]), "b_o3": (b_o3, [bgy_o]), "b_i3": (b_i3, [bfy_i]), "b_o4": (b_o4, [bfy_o]), "b_i4": (b_i4, [bfo]),
        "b_o5": (b_o5, [bof]), "b_i6": (b_i6, [bgm]), "b_i7": (b_i7, [bfm]), "b_en": (b_en, []), "b_ef": (b_ef, []),
        "d_s": (d_s, [share]), "d_w": (d_w, []),
    }

    def role(name):
        return {"i": inner, "o": outer}.get(name[2]) if name not in ("b_en", "b_ef") else outer

    def exchange(t):
        n = 0
        for name, after in STEPS:
            if name[0] == "H":
                compute(t, n)
                n += 1
                continue
            do, sends = steps[name]
            u = t - PER - after
            go = (u >= 0) & (u < nsub)
            if role(name) is not None:
                go = go & role(name)

            @pl.when(go)
            def _():
                if sends:
                    @pl.when(u >= SENDS)
                    def _():
                        for m in sends:
                            m(u - SENDS).wait_send()
                do(u, lax.rem(u, SENDS), lax.rem(u, SLOTS), lax.rem(u, 4))

    def drain():
        for name in steps:
            def leave(sends=steps[name][1]):
                for m in sends:
                    for u in range(max(nsub - SENDS, 0), nsub):
                        m(u).wait_send()
            if role(name) is None:
                leave()
            elif steps[name][1]:
                pl.when(role(name))(leave)

    lanes = 1024

    def norm(first, last):
        def rows(i, _):
            r = pl.ds(pl.multiple_of(i * 16, 16), 16)
            acc = jnp.zeros((16, lanes), f32)
            for j in range(0, d, lanes):
                v = xb[r, j : j + lanes].astype(f32)
                acc = acc + v * v
            scale = lax.rsqrt(jnp.sum(acc, axis=-1, keepdims=True) * (1.0 / d) + 1e-6)
            for j in range(0, d, lanes):
                v = xb[r, j : j + lanes].astype(f32)
                xb[r, j : j + lanes] = (v * scale * gain[pl.ds(j, lanes)].astype(f32)[None]).astype(bf16)

        lax.fori_loop(first // 16, last // 16, rows, None)

    def project(c, i):
        g, kind, j = c * 3 * nt + i, lax.div(i, nt), lax.rem(i, nt)

        def part(p, _):
            w_wait(2 * g + p)
            columns = pl.ds(pl.multiple_of(p * k2, 128), k2)
            one = jnp.dot(xb[:, columns], held_part(lax.rem(2 * g + p, HELD))[...], preferred_element_type=f32)
            w_start(2 * g + p + HELD)

            @pl.when(p == 0)
            def _():
                acc[...] = one

            @pl.when(p == 1)
            def _():
                acc[...] = acc[...] + one

        lax.fori_loop(0, 2, part, None)
        r = acc[...].astype(bf16)
        tokens = pl.ds(pl.multiple_of(c * CHUNK, CHUNK), CHUNK)
        for n in range(TILE // HEAD):
            h = j * (TILE // HEAD) + n
            one = r[:, n * HEAD : (n + 1) * HEAD]

            @pl.when(kind < 2)
            def _():
                w = one.astype(f32)
                w = (w * cs[...] + pltpu.roll(w, HEAD // 2, 1) * sn[...]).astype(bf16)

                @pl.when(kind == 0)
                def _():
                    qb[h] = w

                @pl.when(kind == 1)
                def _():
                    kc[h, tokens, :] = w

            @pl.when(kind == 2)
            def _():
                vt[h, pl.ds(0, HEAD), tokens] = one.T

    e = HEAD**-0.5 * LOG2E

    def attention(c):
        top[...] = jnp.full(top.shape, NEG, f32)
        mix[...] = jnp.zeros(mix.shape, f32)

        def block(j, masked):
            here = pl.ds(pl.multiple_of(j * CHUNK, CHUNK), CHUNK)
            scores = [_dot(kc[h, here, :], qb[h], 1, 1) for h in range(hl)]
            if masked:
                ok = lax.broadcasted_iota(jnp.int32, (CHUNK, CHUNK), 1) >= lax.broadcasted_iota(jnp.int32, (CHUNK, CHUNK), 0)
            weights, keeps = [], []
            for h, s in enumerate(scores):
                if masked:
                    s = jnp.where(ok, s, 2 * NEG)
                old = top[h : h + 1, :]
                new = jnp.maximum(old, s.max(axis=0, keepdims=True))
                top[h : h + 1, :] = new
                weights.append(jnp.exp2((s - new) * e).astype(bf16))
                keeps.append(jnp.exp2((old - new) * e))
            for h in range(hl):
                mix[h] = mix[h] * keeps[h] + _dot(vt[h, :, here], weights[h], 1, 0)

        lax.fori_loop(0, c, lambda j, _: block(j, False), None)
        block(c, True)
        b = lax.rem(c, 2)
        for h in range(hl):
            total = mix[h, HEAD : HEAD + 1, :]
            seen[b, :, h * HEAD : (h + 1) * HEAD] = (mix[h, :HEAD, :] * (1 / total)).T.astype(bf16)

    def output(c, quarter):
        b, tiles = lax.rem(c, 2), half // WO_TILE

        def tile(n, _):
            o_wait(n)
            columns, slot = pl.ds(pl.multiple_of(tile_of(n) * WO_TILE, WO_TILE), WO_TILE), lax.rem(n, WO_HELD)

            pp[b, :, columns] = jnp.dot(seen[b], ob[slot], preferred_element_type=f32)

            @pl.when(n + WO_HELD < tiles)
            def _():
                o_starts(c, n + WO_HELD)

        lax.fori_loop(quarter * (tiles // 4), (quarter + 1) * (tiles // 4), tile, None)

    def compute(t, n):
        each = PARTS // PER
        c, p = lax.div(t, PER), lax.rem(t, PER) * each + n
        here = set(range(n, PARTS, each))

        def branch(parts, on, do):
            if here & set(parts):
                pl.when((t < nsub) & on)(do)

        def first():
            for copy in (*x_copies(c), *cs_copies(c)):
                copy.wait()
            norm(0, CHUNK)

        def middle_():
            @pl.when(c + 1 < nch)
            def _():
                for copy in (*x_copies(c + 1), *cs_copies(c + 1)):
                    copy.start()

            @pl.when(c >= 2)
            def _():
                seen_copy(c - 2).wait_send()
            attention(c)
            seen_copy(c).start()

        def early():
            @pl.when(c == 0)
            def _():
                ext_copy().wait_recv()

            for i in range(WO_HELD):
                o_starts(c, i)

        branch([0], (p == 0) & (c > 0), first)
        branch(range(1, 10), (p >= 1) & (p <= 3 * nt), lambda: project(c, p - 1))
        branch([EARLY], p == EARLY, early)
        branch([10], p == 10, middle_)
        branch([12], p == 12, lambda: seen_copy(c).wait_recv())
        branch(range(12, 16), p >= 12, lambda: output(c, p - 12))

    for copy in (*x_copies(0), *cs_copies(0)):
        copy.start()
    for h in range(hl):
        vt[h, HEAD:, :] = jnp.ones((8, vt.shape[2]), bf16)

    for i, copy in enumerate(x_copies(0)):
        copy.wait()
        w_start(i)
        norm(i * (CHUNK // pieces), (i + 1) * (CHUNK // pieces))
    for h in range(pieces, HELD):
        w_start(h)
    for copy in cs_copies(0):
        copy.wait()

    @pl.when(inner)
    def _():
        pl.semaphore_wait(barrier, 4)

    @pl.when(outer)
    def _():
        pl.semaphore_wait(barrier, 3)

    ext_copy().start()

    held = _held(wb, xb, d)

    def tick(t, _):
        exchange(t)
        for i, (count, copies) in enumerate(held):
            share_of = -(-count // HOLD_TICKS)

            @pl.when((t >= nsub) & (t < nsub + HOLD_TICKS))
            def _():
                def one(j, _):
                    @pl.when(j < count)
                    def _():
                        there, here = copies(j)
                        pltpu.make_async_copy(out.at[there], here, s_hold.at[i]).start()

                lax.fori_loop((t - nsub) * share_of, (t - nsub + 1) * share_of, one, None)

    lax.fori_loop(0, PER + nsub + max(AFTER.values()), tick, None)
    drain()
    for i in range(HELD):
        pltpu.make_async_copy(wq.at[pl.ds(0, k2), pl.ds(0, TILE)], held_part(i), s_hold.at[0]).wait()
    pltpu.make_async_copy(x.at[pl.ds(0, CHUNK), :], xb, s_hold.at[1]).wait()
    for c in range(max(nch - 2, 0), nch):
        seen_copy(c).wait_send()
    ext_copy().wait_send()


def _held(wb, xb, d):
    kinds, row = [], 0

    def add(count, rows, width, where):
        nonlocal row
        across, start = d // width, row

        def piece(j):
            block, at = lax.div(j, across), lax.rem(j, across)
            there = pl.ds(pl.multiple_of(start + block * rows, 16), rows), pl.ds(pl.multiple_of(at * width, 128), width)
            return there, where(block, at)

        kinds.append((count * across, piece))
        row += count * rows

    h = wb.shape[0] * TILE // d
    add(1, h, TILE, lambda block, at: wb.at[pl.ds(pl.multiple_of(at * h, 16), h), :])
    add(xb.shape[0] // 64, 64, d, lambda block, at: xb.at[pl.ds(pl.multiple_of(block * 64, 16), 64), :])
    return kinds


def _held_rows(d):
    return HELD * (d // 2 * TILE // d) + CHUNK


def layer(x, gain, wq, wk, wv, wo, cos, sin):
    rows, d = x.shape
    hl = wq.shape[1] // HEAD
    half, qa = d // 2, d // 4
    nch = rows // CHUNK
    v, dma = pltpu.VMEM, pltpu.SemaphoreType.DMA
    hbm = pl.BlockSpec(memory_space=pl.ANY)
    wa, ia, oa, ib, ob = _split(half)
    na, nb, qa, qb = ia + oa, ib + ob, max(ia, oa), max(ib, ob)

    def buffers(n, *shapes):
        return [v((n, *s), bf16) for s in shapes]

    scratch = [
        v((WO_HELD, 2 * hl * HEAD, WO_TILE), bf16), v((hl, rows, HEAD), bf16), v((hl, HEAD + 8, rows), bf16), v((hl, CHUNK, HEAD), bf16), v((2, CHUNK, 2 * hl * HEAD), bf16), v((2, CHUNK, half), f32),
        v((hl, HEAD + 8, CHUNK), f32), v((CHUNK, TILE), f32), v((hl, CHUNK), f32), v((CHUNK, HEAD), f32), v((CHUNK, HEAD), f32),
        *buffers(4, (ROWS, qa), (ROWS, qb)),
        *buffers(SLOTS, (ROWS, wa), (ROWS, na), (ROWS, qa), (ROWS, na), (SUB, nb), (SUB, qb), (SUB, nb), (ROWS, qb)),
        *buffers(SENDS, (ROWS, wa), (ROWS, na), (ROWS, qa), (SUB, nb), (SUB, qb), (ROWS, qb)),
        dma((4,)), dma((HELD,)), dma((WO_HELD, 2)), dma((2,)), dma((2, 4)), dma((8,)), dma((RS_KINDS + AG_KINDS, SENDS)), dma((RS_KINDS, SLOTS)),
        dma((AG_KINDS, MARKS)), dma((2, 2)), dma((2,)), dma((2,)),
    ]
    kept = [v((HELD * (d // 2), TILE), bf16), v((CHUNK, d), bf16), v((IMAGES, SUB, half), bf16)]
    out, _, *held = pl.pallas_call(
        functools.partial(_kernel, d=d, hl=hl, nch=nch),
        name="layer",
        in_specs=[hbm, pl.BlockSpec(memory_space=pltpu.VMEM), hbm, hbm, hbm, hbm, hbm, hbm],
        out_specs=[hbm, hbm] + [pl.BlockSpec(memory_space=pltpu.VMEM)] * len(kept),
        out_shape=[jax.ShapeDtypeStruct((rows, d), bf16), jax.ShapeDtypeStruct((hl * HEAD, half), bf16), *kept],
        scratch_shapes=scratch,
        compiler_params=pltpu.CompilerParams(collective_id=0, has_side_effects=True, vmem_limit_bytes=LAYER_VMEM),
    )(x, gain, wq, wk, wv, wo, cos, sin)
    return handed(out, *held)


def _hand(a, wb, xb, img, out, ring, s_in, s_out, s_held, *, first, last):
    d = a.shape[1]
    half, nsub, (slots, rows) = d // 2, a.shape[0] // SUB, ring.shape[:2]
    core = lax.rem(lax.axis_index("tp"), 2)
    mine, other = (pl.ds(pl.multiple_of(n * half, 128), half) for n in (core, 1 - core))
    whole = (last - first) // rows
    total = whole + (a.shape[0] - last) // rows

    def ends(i):
        at = pl.ds(first + i * rows, rows)
        return (at, ring.at[i % slots]) if i < whole else ((at, other), ring.at[i % slots, :, pl.ds(0, half)])

    def come(i):
        there, here = ends(i)
        return pltpu.make_async_copy(a.at[there], here, s_in.at[i % slots])

    def go(i):
        there, here = ends(i)
        return pltpu.make_async_copy(here, out.at[there], s_out.at[i % slots])

    kinds = _held(wb, xb, d)
    kinds.append((IMAGES, lambda j: ((pl.ds(pl.multiple_of(last + j * SUB, 16), SUB), mine), img.at[lax.rem(nsub - IMAGES + j, IMAGES)])))

    def held(n, low, high, act):
        def one(j, _):
            there, here = kinds[n][1](j)
            act(pltpu.make_async_copy(here, out.at[there], s_held.at[n]))

        lax.fori_loop(low, high, one, None)

    ahead = slots * 5 // 8
    for i in range(min(ahead, total)):
        come(i).start()
    for i in range(total):
        for n, (count, _) in enumerate(kinds):
            held(n, count * i // total, count * (i + 1) // total, lambda copy: copy.start())
        come(i).wait()
        go(i).start()
        j = i + ahead
        if j < total:
            if j >= slots:
                go(j - slots).wait()
            come(j).start()
    for i in range(max(total - slots, 0), total):
        go(i).wait()
    for n, (count, _) in enumerate(kinds):
        held(n, 0, count, lambda copy: copy.wait())


def handed(a, wb, xb, img):
    d = a.shape[1]
    first, last = _held_rows(d), a.shape[0] - IMAGES * SUB
    slots, rows = 11, 32
    dma = pltpu.SemaphoreType.DMA
    any_, vmem = pl.BlockSpec(memory_space=pl.ANY), pl.BlockSpec(memory_space=pltpu.VMEM)
    return pl.pallas_call(
        functools.partial(_hand, first=first, last=last),
        name="hand",
        in_specs=[any_] + [vmem] * 3,
        out_specs=any_,
        out_shape=jax.ShapeDtypeStruct(a.shape, a.dtype),
        scratch_shapes=[pltpu.VMEM((slots, rows, d), bf16), dma((slots,)), dma((slots,)), dma((3,))],
        compiler_params=pltpu.CompilerParams(vmem_limit_bytes=HAND_VMEM),
    )(a, wb, xb, img)


def solution(mesh):
    def step(x, gain, wq, wk, wv, wo):
        half = HEAD // 2
        angle = np.arange(x.shape[0], dtype=np.float32)[:, None] * np.float32(THETA) ** (-np.arange(half, dtype=np.float32) / half)
        cos, sin = np.cos(angle), np.sin(angle)
        cos, sin = (jnp.asarray(np.concatenate(t, -1), f32) for t in ([cos, cos], [-sin, sin]))
        return layer(x, gain, wq, wk, wv, wo, cos, sin)

    tokens, columns = P("dp", None), P(None, "tp")
    return jax.shard_map(
        step,
        mesh=mesh,
        in_specs=(tokens, P(None), columns, columns, columns, P("tp", None)),
        out_specs=tokens,
        check_vma=False,
    )
```
